32 devices in a mesh: dp: 2 (over x), tp: 4 (over z), cp: 4 (over y, core).
Axes of the slice: x: 2, y: 2, z: 4, core: 2. Of those that a mesh axis runs over, the one named last changes fastest.
Arguments:
- hidden: bfloat16 [2, 4096, 3072], P('dp', 'cp'), parts along dimension 0
- cotangent: bfloat16 [2, 4096, 3072], P('dp', 'cp'), parts along dimension 0
- positions: int32 [8192], P(('dp', 'cp')), parts along dimension 0
- w_q: bfloat16 [3072, 3072], P(None, 'tp')
- w_k: bfloat16 [3072, 1024], P(None, 'tp')
- w_v: bfloat16 [3072, 1024], P(None, 'tp')
- w_o: bfloat16 [3072, 3072], P('tp')
- w_pre: float32 [3072], replicated
- w_post: float32 [3072], replicated
- q_norm: float32 [128], replicated
- k_norm: float32 [128], replicated
Outputs:
- output 1: bfloat16 [2, 4096, 3072], P('dp', 'cp'), parts along dimension 0
- output 2: bfloat16 [2, 4096, 3072], P('dp', 'cp'), parts along dimension 0
- output 3: float32 [6144, 3072], P('dp', 'tp'), parts along dimension 0
- output 4: float32 [6144, 1024], P('dp', 'tp'), parts along dimension 0
- output 5: float32 [6144, 1024], P('dp', 'tp'), parts along dimension 0
- output 6: float32 [6144, 3072], P(('dp', 'tp')), parts along dimension 0
- output 7: float32 [6144], P('dp'), parts along dimension 0
- output 8: float32 [6144], P('dp'), parts along dimension 0
- output 9: float32 [256], P('dp'), parts along dimension 0
- output 10: float32 [256], P('dp'), parts along dimension 0
There are 2 independent parts. The reference program is written for one: setup_inputs(seed, part) draws one part's arguments, and reference() takes and returns one part's arrays. A program takes and returns all parts, laid end to end along the dimension named above; an argument that names none is the same for every part.
All inputs are finite; a program needn't handle non-finite values.
Results may differ from the reference program's by a relative error of at most 0.02.
Values are sent between devices in bfloat16 or wider.
A program may use at most 1 GiB of HBM per device.

```python
import jax
import jax.numpy as jnp
from jax import lax

BATCH = 1
SEQ_LEN = 4096
MODEL_DIM = 3072
NUM_HEADS = 24
KV_HEADS = 8
HEAD_DIM = 128
CP_SIZE = 4
QUERY_BLOCK = 64
POS_RANGE = 131072

EPS = 1e-6
ROPE_BASE = 1000000.0
ROPE_SCALE = 8.0
NEG_BIG = -1e30


def draw_positions(key):
    gap_max = POS_RANGE // SEQ_LEN
    pos_gaps = jax.random.randint(key, (SEQ_LEN,), 1, gap_max + 1, dtype=jnp.int32)
    logical = jnp.cumsum(pos_gaps) - pos_gaps[0]
    piece_len = SEQ_LEN // (2 * CP_SIZE)
    pieces = logical.reshape(2 * CP_SIZE, piece_len)
    layout = jnp.stack([pieces[:CP_SIZE], pieces[CP_SIZE:][::-1]], axis=1)
    return layout.reshape(SEQ_LEN).astype(jnp.int32)


def setup_inputs(seed: int = 0, part: int = 0) -> dict:
    part_keys = jax.random.split(jax.random.fold_in(jax.random.key(seed), part), 3)
    weight_keys = jax.random.split(jax.random.key(seed + 1), 8)
    act_shape = (BATCH, SEQ_LEN, MODEL_DIM)
    q_cols = NUM_HEADS * HEAD_DIM
    kv_cols = KV_HEADS * HEAD_DIM
    hidden = jax.random.normal(part_keys[0], act_shape, jnp.float32).astype(jnp.bfloat16)
    cotangent = jax.random.normal(part_keys[1], act_shape, jnp.float32).astype(jnp.bfloat16)
    w_q = (jax.random.normal(weight_keys[0], (MODEL_DIM, q_cols), jnp.float32) * MODEL_DIM ** -0.5).astype(jnp.bfloat16)
    w_k = (jax.random.normal(weight_keys[1], (MODEL_DIM, kv_cols), jnp.float32) * MODEL_DIM ** -0.5).astype(jnp.bfloat16)
    w_v = (jax.random.normal(weight_keys[2], (MODEL_DIM, kv_cols), jnp.float32) * MODEL_DIM ** -0.5).astype(jnp.bfloat16)
    w_o = (jax.random.normal(weight_keys[3], (q_cols, MODEL_DIM), jnp.float32) * q_cols ** -0.5).astype(jnp.bfloat16)
    w_pre = 0.3 * jax.random.normal(weight_keys[4], (MODEL_DIM,), jnp.float32)
    w_post = 0.3 * jax.random.normal(weight_keys[5], (MODEL_DIM,), jnp.float32)
    q_norm = 0.3 * jax.random.normal(weight_keys[6], (HEAD_DIM,), jnp.float32)
    k_norm = 0.3 * jax.random.normal(weight_keys[7], (HEAD_DIM,), jnp.float32)
    return {'hidden': hidden, 'cotangent': cotangent, 'positions': draw_positions(part_keys[2]), 'w_q': w_q, 'w_k': w_k, 'w_v': w_v, 'w_o': w_o, 'w_pre': w_pre, 'w_post': w_post, 'q_norm': q_norm, 'k_norm': k_norm}


def rms_unit(values):
    return values * lax.rsqrt(jnp.mean(values * values, axis=-1, keepdims=True) + EPS)


def to_bf16(values):
    return values.astype(jnp.bfloat16).astype(jnp.float32)


def rope_apply(values, cos_t, sin_t):
    half_dim = values.shape[-1] // 2
    lower_half = values[..., :half_dim]
    upper_half = values[..., half_dim:]
    return jnp.concatenate([lower_half * cos_t - upper_half * sin_t, upper_half * cos_t + lower_half * sin_t], axis=-1)


def block_forward(x_f32, w_q, w_k, w_v, w_o, w_pre, w_post, q_norm, k_norm, positions):
    groups = NUM_HEADS // KV_HEADS
    normed = to_bf16(rms_unit(x_f32) * (1.0 + w_pre))
    q_raw = to_bf16(jnp.einsum('bsd,dh->bsh', normed, w_q)).reshape(BATCH, SEQ_LEN, NUM_HEADS, HEAD_DIM)
    k_raw = to_bf16(jnp.einsum('bsd,dh->bsh', normed, w_k)).reshape(BATCH, SEQ_LEN, KV_HEADS, HEAD_DIM)
    v_heads = to_bf16(jnp.einsum('bsd,dh->bsh', normed, w_v)).reshape(BATCH, SEQ_LEN, KV_HEADS, HEAD_DIM)
    half_dim = HEAD_DIM // 2
    inv_freq = 1.0 / (ROPE_SCALE * ROPE_BASE ** (jnp.arange(half_dim, dtype=jnp.float32) * (2.0 / HEAD_DIM)))
    angles = positions.astype(jnp.float32)[:, None] * inv_freq[None, :]
    cos_t = jnp.cos(angles)[None, :, None, :]
    sin_t = jnp.sin(angles)[None, :, None, :]
    q_fin = to_bf16(rope_apply(rms_unit(q_raw) * (1.0 + q_norm), cos_t, sin_t))
    k_fin = to_bf16(rope_apply(rms_unit(k_raw) * (1.0 + k_norm), cos_t, sin_t))
    score_scale = HEAD_DIM ** -0.5
    n_blocks = SEQ_LEN // QUERY_BLOCK
    q_blocks = jnp.moveaxis(q_fin.reshape(BATCH, n_blocks, QUERY_BLOCK, KV_HEADS, groups, HEAD_DIM), 1, 0)
    pos_blocks = positions.reshape(n_blocks, QUERY_BLOCK)

    def one_block(block_in):
        q_blk, q_pos = block_in
        scores = jnp.einsum('bqkgd,bskd->bkgqs', q_blk, k_fin) * score_scale
        allowed = positions[None, :] <= q_pos[:, None]
        attn_prob = jax.nn.softmax(jnp.where(allowed, scores, NEG_BIG), axis=-1)
        return jnp.einsum('bkgqs,bskd->bqkgd', attn_prob, v_heads)

    block_outs = lax.map(jax.checkpoint(one_block), (q_blocks, pos_blocks))
    attn_in = to_bf16(jnp.moveaxis(block_outs, 0, 1).reshape(BATCH, SEQ_LEN, NUM_HEADS * HEAD_DIM))
    attn = jnp.einsum('bsh,hd->bsd', attn_in, w_o)
    return x_f32 + rms_unit(attn) * (1.0 + w_post)


def reference(hidden, cotangent, positions, w_q, w_k, w_v, w_o, w_pre, w_post, q_norm, k_norm):
    def forward(x_f32, wq_f32, wk_f32, wv_f32, wo_f32, pre_gain, post_gain, q_gain, k_gain):
        return block_forward(x_f32, wq_f32, wk_f32, wv_f32, wo_f32, pre_gain, post_gain, q_gain, k_gain, positions)

    out_f32, pullback = jax.vjp(forward, hidden.astype(jnp.float32), w_q.astype(jnp.float32), w_k.astype(jnp.float32), w_v.astype(jnp.float32), w_o.astype(jnp.float32), w_pre, w_post, q_norm, k_norm)
    grad_list = pullback(cotangent.astype(jnp.float32))
    return (out_f32.astype(jnp.bfloat16), grad_list[0].astype(jnp.bfloat16), grad_list[1], grad_list[2], grad_list[3], grad_list[4], grad_list[5], grad_list[6], grad_list[7], grad_list[8])
```

```python
import functools

import jax
import jax.numpy as jnp
import numpy as np
from jax import lax
from jax.experimental import pallas as pl
from jax.experimental.pallas import tpu as pltpu
from jax.sharding import PartitionSpec as P

EPS = 1e-6
ROPE_BASE = 1000000.0
ROPE_SCALE = 8.0
NEG_BIG = -1e30
LOG2E = 1.4426950408889634
HD = 128
F32 = jnp.float32
BF16 = jnp.bfloat16
VMEM_MAX = 60 * 1024 * 1024
NT = (((1,), (1,)), ((), ()))
TN = (((0,), (0,)), ((), ()))


def dot(a, b, dims=(((1,), (0,)), ((), ()))):
    return lax.dot_general(a, b, dims, preferred_element_type=F32)


def params(sem, vmem=VMEM_MAX):
    return pltpu.CompilerParams(dimension_semantics=sem, vmem_limit_bytes=vmem)


def cost(flops, nbytes, trans=0):
    return pl.CostEstimate(flops=int(flops), bytes_accessed=int(nbytes), transcendentals=int(trans))


def whole(shape):
    return pl.BlockSpec(shape, lambda *_: (0,) * len(shape))


def fixed(shape):
    return pl.BlockSpec(shape, lambda *_: (0,) * len(shape), pipeline_mode=pl.Buffered(buffer_count=1))


def rope_tables(pos_loc):
    half_dim = HD // 2
    inv_freq = 1.0 / (ROPE_SCALE * ROPE_BASE ** (jnp.arange(half_dim, dtype=F32) * (2.0 / HD)))
    angles = pos_loc.astype(F32)[:, None] * inv_freq[None, :]
    cos_t, sin_t = jnp.cos(angles), jnp.sin(angles)
    return jnp.concatenate([cos_t, cos_t], axis=-1), jnp.concatenate([-sin_t, sin_t], axis=-1)


def norm_rope(raw, gain, cos_t, sin_t):
    raw = raw.astype(F32)
    unit = raw * lax.rsqrt(jnp.mean(raw * raw, axis=-1, keepdims=True) + EPS)
    scaled = unit * (1.0 + gain)
    return (scaled * cos_t + pltpu.roll(scaled, HD // 2, 1) * sin_t).astype(BF16)


def norm_rope_back(d_final, raw, gain, cos_t, sin_t):
    raw = raw.astype(F32)
    inv = lax.rsqrt(jnp.mean(raw * raw, axis=-1, keepdims=True) + EPS)
    unit = raw * inv
    d_scaled = d_final * cos_t - pltpu.roll(d_final, HD // 2, 1) * sin_t
    d_gain = jnp.sum(d_scaled * unit, axis=0, keepdims=True)
    d_unit = d_scaled * (1.0 + gain)
    d_raw = inv * (d_unit - unit * jnp.mean(d_unit * unit, axis=-1, keepdims=True))
    return d_raw.astype(BF16), d_gain


def kv_kernel(x_ref, wpre_ref, wk_ref, wv_ref, kn_ref, cos_ref, sin_ref, normed_ref, kv_ref, kraw_ref):
    x = x_ref[...].astype(F32)
    inv = lax.rsqrt(jnp.mean(x * x, axis=-1, keepdims=True) + EPS)
    normed = (x * inv * (1.0 + wpre_ref[...])).astype(BF16)
    normed_ref[...] = normed
    k_raw = dot(normed, wk_ref[...]).astype(BF16)
    kraw_ref[...] = k_raw
    width = k_raw.shape[1]
    for h in range(width // HD):
        cols = slice(h * HD, (h + 1) * HD)
        kv_ref[:, cols] = norm_rope(k_raw[:, cols], kn_ref[...], cos_ref[...], sin_ref[...])
    kv_ref[:, width:] = dot(normed, wv_ref[...]).astype(BF16)


def project_kv(x, w_pre, w_k, w_v, k_norm, cos_t, sin_t, rows=256):
    seq, dim = x.shape
    width = w_k.shape[1]
    row = lambda n: pl.BlockSpec((rows, n), lambda i: (i, 0))
    return pl.pallas_call(
        kv_kernel,
        name="project_kv",
        grid=(seq // rows,),
        in_specs=[row(dim), whole((1, dim)), fixed(w_k.shape), fixed(w_v.shape), whole((1, HD)), row(HD), row(HD)],
        out_specs=[row(dim), row(2 * width), row(width)],
        out_shape=[
            jax.ShapeDtypeStruct((seq, dim), BF16),
            jax.ShapeDtypeStruct((seq, 2 * width), BF16),
            jax.ShapeDtypeStruct((seq, width), BF16),
        ],
        compiler_params=params(("arbitrary",)),
        cost_estimate=cost(4 * seq * dim * width, 4 * seq * dim + 4 * dim * width),
    )(x, w_pre, w_k, w_v, k_norm, cos_t, sin_t)


def q_kernel(normed_ref, wq_ref, qn_ref, cos_ref, sin_ref, qfin_ref, qraw_ref):
    q_raw = dot(normed_ref[...], wq_ref[...]).astype(BF16)
    for h in range(qfin_ref.shape[0]):
        part = q_raw[:, h * HD:(h + 1) * HD]
        qraw_ref[h] = part
        qfin_ref[h] = norm_rope(part, qn_ref[...], cos_ref[...], sin_ref[...])


def project_q(normed, w_q, q_norm, cos_t, sin_t, rows=256):
    seq, dim = normed.shape
    heads = w_q.shape[1] // HD
    row = lambda n: pl.BlockSpec((rows, n), lambda i: (i, 0))
    head_rows = pl.BlockSpec((heads, rows, HD), lambda i: (0, i, 0))
    shape = jax.ShapeDtypeStruct((heads, seq, HD), BF16)
    return pl.pallas_call(
        q_kernel,
        name="project_q",
        grid=(seq // rows,),
        in_specs=[row(dim), fixed(w_q.shape), whole((1, HD)), row(HD), row(HD)],
        out_specs=[head_rows, head_rows],
        out_shape=[shape, shape],
        compiler_params=params(("arbitrary",)),
        cost_estimate=cost(2 * seq * dim * heads * HD, 2 * seq * dim + 2 * dim * heads * HD),
    )(normed, w_q, q_norm, cos_t, sin_t)


def load_kv(kv_refs, k_buf, v_buf, sems):
    kv_heads = k_buf.shape[0]
    copies = []
    for s, ref in enumerate(kv_refs):
        for h in range(kv_heads):
            for t, buf in enumerate((k_buf, v_buf)):
                src = ref.at[:, pl.ds((t * kv_heads + h) * HD, HD)]
                copies.append(pltpu.make_async_copy(src, buf.at[h, s], sems.at[s, h, t]))
    for copy in copies:
        copy.start()
    for copy in copies:
        copy.wait()


def piece_place(piece, me, n_cp):
    upper = piece >= n_cp
    owner = jnp.where(upper, 2 * n_cp - 1 - piece, piece)
    return jnp.bitwise_xor(owner, me), upper.astype(jnp.int32)


def fwd_kernel(n_cp, me_ref, q_ref, *rest):
    kv_refs = rest[:n_cp]
    o_ref, lse_ref, k_buf, v_buf, m_scr, acc_scr, sems = rest[n_cp:]
    h, half = pl.program_id(0), pl.program_id(1)
    groups, rows, _ = q_ref.shape

    @pl.when((h == 0) & (half == 0))
    def _():
        load_kv(kv_refs, k_buf, v_buf, sems)

    me = me_ref[0]
    piece = jnp.where(half == 0, me, 2 * n_cp - 1 - me)
    scale = HD ** -0.5 * LOG2E
    m_scr[...] = jnp.full(m_scr.shape, NEG_BIG, F32)
    acc_scr[...] = jnp.zeros(acc_scr.shape, F32)

    def block(j, masked):
        slot, upper = piece_place(j, me, n_cp)
        span = pl.ds(pl.multiple_of(upper * rows, rows), rows)
        k = k_buf[h, slot, span, :]
        v_ext = jnp.concatenate([v_buf[h, slot, span, :], jnp.ones((rows, HD), BF16)], axis=1)
        scores = [dot(q_ref[g], k, NT) * scale for g in range(groups)]
        for g in range(groups):
            s = scores[g]
            if masked:
                q_pos = lax.broadcasted_iota(jnp.int32, s.shape, 0)
                k_pos = lax.broadcasted_iota(jnp.int32, s.shape, 1)
                s = jnp.where(k_pos <= q_pos, s, NEG_BIG)
            m_old = m_scr[g]
            m_new = jnp.maximum(m_old, jnp.max(s, axis=1, keepdims=True))
            alpha = jnp.exp2(m_old - m_new)
            p = jnp.exp2(s - jnp.concatenate([m_new] * (rows // HD), axis=1)).astype(BF16)
            acc_scr[g] = acc_scr[g] * jnp.concatenate([alpha, alpha], axis=1) + dot(p, v_ext)
            m_scr[g] = m_new

    def full(j, carry):
        block(j, False)
        return carry

    lax.fori_loop(0, piece, full, 0)
    block(piece, True)
    for g in range(groups):
        l = acc_scr[g, :, HD:]
        o_ref[:, g * HD:(g + 1) * HD] = (acc_scr[g, :, :HD] / l).astype(BF16)
        lse_ref[0, g:g + 1, :] = jnp.transpose(m_scr[g] + jnp.log2(l))[0:1, :]


def attention_fwd(me, q_fin, kv_blocks, kv_heads):
    heads, seq, _ = q_fin.shape
    n_cp = len(kv_blocks)
    groups = heads // kv_heads
    rows = seq // 2
    grid_spec = pltpu.PrefetchScalarGridSpec(
        num_scalar_prefetch=1,
        grid=(kv_heads, 2),
        in_specs=[pl.BlockSpec((groups, rows, HD), lambda h, i, *_: (h, i, 0))] + [pl.BlockSpec(memory_space=pl.ANY)] * n_cp,
        out_specs=[
            pl.BlockSpec((rows, groups * HD), lambda h, i, *_: (i, h)),
            pl.BlockSpec((1, 8, rows), lambda h, i, *_: (h, 0, i)),
        ],
        scratch_shapes=[
            pltpu.VMEM((kv_heads, n_cp, seq, HD), BF16),
            pltpu.VMEM((kv_heads, n_cp, seq, HD), BF16),
            pltpu.VMEM((groups, rows, HD), F32),
            pltpu.VMEM((groups, rows, 2 * HD), F32),
            pltpu.SemaphoreType.DMA((n_cp, kv_heads, 2)),
        ],
    )
    pairs = heads * rows * rows * (2 * n_cp + 1)
    return pl.pallas_call(
        functools.partial(fwd_kernel, n_cp),
        name="attention_fwd",
        grid_spec=grid_spec,
        out_shape=[
            jax.ShapeDtypeStruct((seq, heads * HD), BF16),
            jax.ShapeDtypeStruct((kv_heads, 8, seq), F32),
        ],
        compiler_params=params(("arbitrary", "arbitrary")),
        cost_estimate=cost(4 * pairs * HD, 8 * seq * heads * HD, pairs),
    )(me, q_fin, *kv_blocks)


def bwd_kernel(n_cp, me_ref, q_ref, do_ref, o_ref, lse_ref, qraw_ref, cos_ref, sin_ref, qn_ref, *rest):
    kv_refs = rest[:n_cp]
    dq_ref, dkv_ref, gain_ref, k_buf, v_buf, dq_scr, sems = rest[n_cp:]
    h, half = pl.program_id(0), pl.program_id(1)
    groups, rows, _ = q_ref.shape

    @pl.when((h == 0) & (half == 0))
    def _():
        load_kv(kv_refs, k_buf, v_buf, sems)
        gain_ref[...] = jnp.zeros(gain_ref.shape, F32)

    @pl.when(half == 0)
    def _():
        dkv_ref[...] = jnp.zeros(dkv_ref.shape, F32)

    me = me_ref[0]
    piece = jnp.where(half == 0, me, 2 * n_cp - 1 - me)
    scale = HD ** -0.5
    delta = []
    for g in range(groups):
        prod = do_ref[g].astype(F32) * o_ref[:, g * HD:(g + 1) * HD].astype(F32)
        column = jnp.broadcast_to(jnp.sum(prod, axis=1, keepdims=True), (rows, HD))
        delta.append(jnp.transpose(column)[0:1, :])
    dq_scr[...] = jnp.zeros(dq_scr.shape, F32)

    def block(j, masked):
        slot, upper = piece_place(j, me, n_cp)
        span = pl.ds(pl.multiple_of(upper * rows, rows), rows)
        k = k_buf[h, slot, span, :]
        v = v_buf[h, slot, span, :]
        probs, d_scores = [], []
        for g in range(groups):
            s = dot(k, q_ref[g], NT)
            p = jnp.exp2(s * (scale * LOG2E) - lse_ref[0, g:g + 1, :])
            if masked:
                k_pos = lax.broadcasted_iota(jnp.int32, s.shape, 0)
                q_pos = lax.broadcasted_iota(jnp.int32, s.shape, 1)
                p = jnp.where(k_pos <= q_pos, p, 0.0)
            probs.append(p.astype(BF16))
            d_scores.append((p * (dot(v, do_ref[g], NT) - delta[g])).astype(BF16))
        for g in range(groups):
            dq_scr[g] += dot(d_scores[g], k, TN)
        index = (slot % 2) * (n_cp // 2) + slot // 2
        d_all = jnp.concatenate(d_scores, axis=1)
        p_all = jnp.concatenate(probs, axis=1)
        dkv_ref[index, 0, 0, span, :] += dot(d_all, q_ref[...].reshape(groups * rows, HD)) * scale
        dkv_ref[index, 1, 0, span, :] += dot(p_all, do_ref[...].reshape(groups * rows, HD))

    def full(j, carry):
        block(j, False)
        return carry

    lax.fori_loop(0, piece, full, 0)
    block(piece, True)
    for g in range(groups):
        d_raw, d_gain = norm_rope_back(dq_scr[g] * scale, qraw_ref[g], qn_ref[...], cos_ref[...], sin_ref[...])
        dq_ref[:, g * HD:(g + 1) * HD] = d_raw
        gain_ref[0:1, :] += d_gain


def attention_bwd(me, q_fin, d_out, out, lse, q_raw, cos_t, sin_t, q_norm, kv_blocks, kv_heads):
    heads, seq, _ = q_fin.shape
    n_cp = len(kv_blocks)
    groups = heads // kv_heads
    rows = seq // 2
    by_head = pl.BlockSpec((groups, rows, HD), lambda h, i, *_: (h, i, 0))
    by_row = pl.BlockSpec((rows, groups * HD), lambda h, i, *_: (i, h))
    table = pl.BlockSpec((rows, HD), lambda h, i, *_: (i, 0))
    grid_spec = pltpu.PrefetchScalarGridSpec(
        num_scalar_prefetch=1,
        grid=(kv_heads, 2),
        in_specs=[
            by_head,
            by_head,
            by_row,
            pl.BlockSpec((1, 8, rows), lambda h, i, *_: (h, 0, i)),
            by_head,
            table,
            table,
            whole((1, HD)),
        ] + [pl.BlockSpec(memory_space=pl.ANY)] * n_cp,
        out_specs=[
            by_row,
            pl.BlockSpec((n_cp, 2, 1, seq, HD), lambda h, i, *_: (0, 0, h, 0, 0)),
            whole((8, HD)),
        ],
        scratch_shapes=[
            pltpu.VMEM((kv_heads, n_cp, seq, HD), BF16),
            pltpu.VMEM((kv_heads, n_cp, seq, HD), BF16),
            pltpu.VMEM((groups, rows, HD), F32),
            pltpu.SemaphoreType.DMA((n_cp, kv_heads, 2)),
        ],
    )
    pairs = heads * rows * rows * (2 * n_cp + 1)
    return pl.pallas_call(
        functools.partial(bwd_kernel, n_cp),
        name="attention_bwd",
        grid_spec=grid_spec,
        out_shape=[
            jax.ShapeDtypeStruct((seq, heads * HD), BF16),
            jax.ShapeDtypeStruct((n_cp, 2, kv_heads, seq, HD), F32),
            jax.ShapeDtypeStruct((8, HD), F32),
        ],
        compiler_params=params(("arbitrary", "arbitrary")),
        cost_estimate=cost(10 * pairs * HD, 16 * seq * heads * HD, pairs),
    )(me, q_fin, d_out, out, lse, q_raw, cos_t, sin_t, q_norm, *kv_blocks)


def post_kernel(o_ref, wall_ref, wmine_ref, x_ref, dy_ref, wpost_ref, y_ref, dattn_ref, do_ref, dpost_ref):
    n_tp = o_ref.shape[0]
    out_all = jnp.concatenate([o_ref[t] for t in range(n_tp)], axis=1)
    attn = dot(out_all, wall_ref[...])
    inv = lax.rsqrt(jnp.mean(attn * attn, axis=-1, keepdims=True) + EPS)
    unit = attn * inv
    gain = 1.0 + wpost_ref[...]
    y_ref[...] = (x_ref[...].astype(F32) + unit * gain).astype(BF16)
    dy = dy_ref[...].astype(F32)

    @pl.when(pl.program_id(0) == 0)
    def _():
        dpost_ref[...] = jnp.zeros(dpost_ref.shape, F32)

    dpost_ref[0:1, :] += jnp.sum(dy * unit, axis=0, keepdims=True)
    d_unit = dy * gain
    d_attn = (inv * (d_unit - unit * jnp.mean(d_unit * unit, axis=-1, keepdims=True))).astype(BF16)
    dattn_ref[...] = d_attn
    d_out = dot(d_attn, wmine_ref[...], NT)
    for h in range(do_ref.shape[0]):
        do_ref[h] = d_out[:, h * HD:(h + 1) * HD].astype(BF16)


def post(out_all, w_all, w_mine, x, dy, w_post, rows=256):
    n_tp, seq, width = out_all.shape
    dim = x.shape[1]
    heads = width // HD
    row = pl.BlockSpec((rows, dim), lambda i: (i, 0))
    return pl.pallas_call(
        post_kernel,
        name="post",
        grid=(seq // rows,),
        in_specs=[
            pl.BlockSpec((n_tp, rows, width), lambda i: (0, i, 0)),
            fixed(w_all.shape),
            fixed(w_mine.shape),
            row,
            row,
            whole((1, dim)),
        ],
        out_specs=[row, row, pl.BlockSpec((heads, rows, HD), lambda i: (0, i, 0)), whole((8, dim))],
        out_shape=[
            jax.ShapeDtypeStruct((seq, dim), BF16),
            jax.ShapeDtypeStruct((seq, dim), BF16),
            jax.ShapeDtypeStruct((heads, seq, HD), BF16),
            jax.ShapeDtypeStruct((8, dim), F32),
        ],
        compiler_params=params(("arbitrary",)),
        cost_estimate=cost(2 * seq * dim * width * (n_tp + 1), 8 * seq * dim + 2 * dim * width * (n_tp + 1)),
    )(out_all, w_all, w_mine, x, dy, w_post)


def kback_kernel(own_ref, near_ref, far_ref, kraw_ref, cos_ref, sin_ref, kn_ref, out_ref, gain_ref):
    @pl.when(pl.program_id(0) == 0)
    def _():
        gain_ref[...] = jnp.zeros(gain_ref.shape, F32)

    kv_heads = own_ref.shape[2]
    for h in range(kv_heads):
        cols = slice(h * HD, (h + 1) * HD)
        d_k = own_ref[0, 0, h] + near_ref[0, 0, h] + far_ref[0, h]
        d_raw, d_gain = norm_rope_back(d_k, kraw_ref[:, cols], kn_ref[...], cos_ref[...], sin_ref[...])
        out_ref[:, cols] = d_raw
        gain_ref[0:1, :] += d_gain
        d_v = own_ref[0, 1, h] + near_ref[0, 1, h] + far_ref[1, h]
        out_ref[:, (kv_heads + h) * HD:(kv_heads + h + 1) * HD] = d_v.astype(BF16)


def key_back(dkv, near, far, k_raw, cos_t, sin_t, k_norm, rows=256):
    _, _, kv_heads, seq, _ = dkv.shape
    full = pl.BlockSpec((1, 2, kv_heads, rows, HD), lambda i: (0, 0, 0, i, 0))
    row = lambda n: pl.BlockSpec((rows, n), lambda i: (i, 0))
    return pl.pallas_call(
        kback_kernel,
        name="key_back",
        grid=(seq // rows,),
        in_specs=[
            full,
            full,
            pl.BlockSpec((2, kv_heads, rows, HD), lambda i: (0, 0, i, 0)),
            row(kv_heads * HD),
            row(HD),
            row(HD),
            whole((1, HD)),
        ],
        out_specs=[row(2 * kv_heads * HD), whole((8, HD))],
        out_shape=[
            jax.ShapeDtypeStruct((seq, 2 * kv_heads * HD), BF16),
            jax.ShapeDtypeStruct((8, HD), F32),
        ],
        compiler_params=params(("arbitrary",)),
        cost_estimate=cost(50 * seq * kv_heads * HD, 12 * seq * kv_heads * HD),
    )(dkv, near, far, k_raw, cos_t, sin_t, k_norm)


def dx_kernel(n_tp, *refs):
    g_refs = refs[:n_tp]
    w_ref, x_ref, dy_ref, wpre_ref, dx_ref, dpre_ref, acc = refs[n_tp:]
    i = pl.program_id(0)
    total = dot(g_refs[0][...], w_ref[0], NT)
    for t in range(1, n_tp):
        total += dot(g_refs[t][...], w_ref[t], NT)
    acc[i] = total

    @pl.when(i == pl.num_programs(0) - 1)
    def _():
        d_normed = jnp.concatenate([acc[t] for t in range(acc.shape[0])], axis=1)
        x = x_ref[...].astype(F32)
        inv = lax.rsqrt(jnp.mean(x * x, axis=-1, keepdims=True) + EPS)
        unit = x * inv
        dpre_ref[...] = jnp.broadcast_to(jnp.sum(d_normed * unit, axis=0, keepdims=True), dpre_ref.shape)
        d_unit = d_normed * (1.0 + wpre_ref[...])
        d_x = inv * (d_unit - unit * jnp.mean(d_unit * unit, axis=-1, keepdims=True))
        dx_ref[...] = (dy_ref[...].astype(F32) + d_x).astype(BF16)


def input_grad(grads, w_all, x, dy, w_pre, cols=512):
    n_tp = len(grads)
    rows, width = grads[0].shape
    dim = x.shape[1]
    return pl.pallas_call(
        functools.partial(dx_kernel, n_tp),
        name="input_grad",
        grid=(dim // cols,),
        in_specs=[whole((rows, width))] * n_tp + [
            pl.BlockSpec((n_tp, cols, width), lambda i: (0, i, 0)),
            whole((rows, dim)),
            whole((rows, dim)),
            whole((1, dim)),
        ],
        out_specs=[whole((rows, dim)), whole((8, dim))],
        out_shape=[jax.ShapeDtypeStruct((rows, dim), BF16), jax.ShapeDtypeStruct((8, dim), F32)],
        scratch_shapes=[pltpu.VMEM((dim // cols, rows, cols), F32)],
        compiler_params=params(("arbitrary",)),
        cost_estimate=cost(2 * n_tp * rows * width * dim, 2 * n_tp * width * dim),
    )(*grads, w_all, x, dy, w_pre)


def solution(mesh):
    n_cp, n_tp, n_dp = mesh.shape["cp"], mesh.shape["tp"], mesh.shape["dp"]
    near = [(i, i ^ 1) for i in range(n_cp)]
    across = [(i, i ^ 2) for i in range(n_cp)]

    def per_device(hidden, cotangent, pos_loc, w_q, w_k, w_v, w_o, w_pre, w_post, q_norm, k_norm):
        _, seq, dim = hidden.shape
        x, dy = hidden[0], cotangent[0]
        kv_heads = w_k.shape[1] // HD
        cp, tp, dp = lax.axis_index("cp"), lax.axis_index("tp"), lax.axis_index("dp")
        me = cp.astype(jnp.int32).reshape(1)
        everyone = ("tp", "dp", "cp")
        share = dp * n_cp + cp
        shares = n_dp * n_cp

        o_rows = w_o.shape[0] // shares
        w_o_all = lax.all_gather(lax.dynamic_slice_in_dim(w_o, share * o_rows, o_rows, 0), everyone, axis=0, tiled=True)
        w_rows = dim // shares
        parts = [lax.dynamic_slice_in_dim(w, share * w_rows, w_rows, 0) for w in (w_q, w_k, w_v)]

        cos_t, sin_t = rope_tables(pos_loc)
        qn, kn = q_norm.reshape(1, HD), k_norm.reshape(1, HD)
        wpre, wpost = w_pre.reshape(1, dim), w_post.reshape(1, dim)
        normed, kv_own, k_raw = project_kv(x, wpre, w_k, w_v, kn, cos_t, sin_t)
        kv_far = lax.ppermute(kv_own, "cp", across)
        kv_near = lax.ppermute(kv_own, "cp", near)
        kv_both = lax.ppermute(kv_far, "cp", near)
        q_fin, q_raw = project_q(normed, w_q, qn, cos_t, sin_t)
        kv_blocks = [kv_own, kv_near, kv_far, kv_both]
        out, lse = attention_fwd(me, q_fin, kv_blocks, kv_heads)

        out, w_o_all = lax.optimization_barrier((out, w_o_all))
        out_all = lax.all_gather(out, "tp", axis=0, tiled=False)
        y, d_attn, d_out, d_post = post(out_all, w_o_all, w_o, x, dy, wpost)
        fence, _ = lax.optimization_barrier((jnp.concatenate(parts, axis=1), out_all))
        w_all = lax.all_gather(fence, everyone, axis=0, tiled=True).reshape(n_tp, dim, fence.shape[1])

        def cp_sum(part):
            half = part.shape[0] // 2
            core = cp % 2
            keep = lax.dynamic_slice_in_dim(part, core * half, half, 0)
            give = lax.dynamic_slice_in_dim(part, (1 - core) * half, half, 0)
            keep = keep + lax.ppermute(give, "cp", near)
            keep = keep + lax.ppermute(keep, "cp", across)
            other = lax.ppermute(keep, "cp", near)
            first = jnp.where(core == 0, keep, other)
            second = jnp.where(core == 0, other, keep)
            return jnp.concatenate([first, second], axis=0)

        d_wo_part, d_out = lax.optimization_barrier((dot(out, d_attn, TN), d_out))
        d_wo = cp_sum(d_wo_part)

        dq, dkv, dq_gain = attention_bwd(me, q_fin, d_out, out, lse, q_raw, cos_t, sin_t, qn, kv_blocks, kv_heads)
        got = lax.ppermute(dkv[n_cp // 2:], "cp", near)
        dkv_far = lax.ppermute(dkv[1] + got[1], "cp", across)
        d_kv, dk_gain = key_back(dkv, got, dkv_far, k_raw, cos_t, sin_t, kn)

        rows = seq // n_tp
        grads = jnp.concatenate([dq, d_kv], axis=1)
        pieces = [None] * n_tp
        pieces[0] = lax.dynamic_slice_in_dim(grads, tp * rows, rows, 0)
        for s in range(1, n_tp):
            part = lax.dynamic_slice_in_dim(grads, ((tp + s) % n_tp) * rows, rows, 0)
            pieces[s] = lax.ppermute(part, "tp", [(i, (i + s) % n_tp) for i in range(n_tp)])
        stacked = jnp.stack(pieces, axis=0)
        ordered = [lax.dynamic_index_in_dim(stacked, (tp - t) % n_tp, 0, keepdims=False) for t in range(n_tp)]
        x_rows = lax.dynamic_slice_in_dim(x, tp * rows, rows, 0)
        dy_rows = lax.dynamic_slice_in_dim(dy, tp * rows, rows, 0)
        dx_rows, d_pre = input_grad(ordered, w_all, x_rows, dy_rows, wpre)
        d_hidden = lax.all_gather(dx_rows, "tp", axis=0, tiled=True)

        d_wq = cp_sum(dot(normed, dq, TN))
        d_wkv = cp_sum(dot(normed, d_kv, TN))

        small = jnp.concatenate([jnp.where(tp == 0, d_post[0], 0.0), d_pre[0], dq_gain[0], dk_gain[0]])
        small = small + lax.ppermute(small, "cp", near)
        small = small + lax.ppermute(small, "cp", across)
        small = small + lax.ppermute(small, "tp", [(i, i ^ 1) for i in range(n_tp)])
        small = small + lax.ppermute(small, "tp", [(i, i ^ 2) for i in range(n_tp)])
        d_post, d_pre = small[:dim], small[dim:2 * dim]
        d_qn, d_kn = small[2 * dim:2 * dim + HD], small[2 * dim + HD:]
        kv_cols = kv_heads * HD
        return y[None], d_hidden[None], d_wq, d_wkv[:, :kv_cols], d_wkv[:, kv_cols:], d_wo, d_pre, d_post, d_qn, d_kn

    specs_in = (P('dp', 'cp', None), P('dp', 'cp', None), P(('dp', 'cp')), P(None, 'tp'), P(None, 'tp'), P(None, 'tp'), P('tp', None), P(None), P(None), P(None), P(None))
    specs_out = (P('dp', 'cp', None), P('dp', 'cp', None), P('dp', 'tp'), P('dp', 'tp'), P('dp', 'tp'), P(('dp', 'tp'), None), P('dp'), P('dp'), P('dp'), P('dp'))
    return jax.shard_map(per_device, mesh=mesh, in_specs=specs_in, out_specs=specs_out, check_vma=False)
```

```python
import functools

import jax
import jax.numpy as jnp
from jax import lax
from jax.experimental import pallas as pl
from jax.experimental.pallas import tpu as pltpu
from jax.sharding import PartitionSpec as P


EPS = 1e-6
ROPE_BASE = 1000000.0
ROPE_SCALE = 8.0
NEG_BIG = -1e30
LOG2E = 1.4426950408889634
HD = 128
F32 = jnp.float32
BF16 = jnp.bfloat16
VMEM_MAX = 60 * 1024 * 1024
NT = (((1,), (1,)), ((), ()))
TN = (((0,), (0,)), ((), ()))


def dot(a, b, dims=(((1,), (0,)), ((), ()))):
    return lax.dot_general(a, b, dims, preferred_element_type=F32)


def params(sem, vmem=VMEM_MAX):
    return pltpu.CompilerParams(dimension_semantics=sem, vmem_limit_bytes=vmem)


def cost(flops, nbytes, trans=0):
    return pl.CostEstimate(flops=int(flops), bytes_accessed=int(nbytes), transcendentals=int(trans))


def whole(shape):
    return pl.BlockSpec(shape, lambda *_: (0,) * len(shape))


def fixed(shape):
    return pl.BlockSpec(shape, lambda *_: (0,) * len(shape), pipeline_mode=pl.Buffered(buffer_count=1))


def rope_tables(pos_loc):
    half_dim = HD // 2
    inv_freq = 1.0 / (ROPE_SCALE * ROPE_BASE ** (jnp.arange(half_dim, dtype=F32) * (2.0 / HD)))
    angles = pos_loc.astype(F32)[:, None] * inv_freq[None, :]
    cos_t, sin_t = jnp.cos(angles), jnp.sin(angles)
    return jnp.concatenate([cos_t, cos_t], axis=-1), jnp.concatenate([-sin_t, sin_t], axis=-1)


def norm_rope(raw, gain, cos_t, sin_t):
    raw = raw.astype(F32)
    unit = raw * lax.rsqrt(jnp.mean(raw * raw, axis=-1, keepdims=True) + EPS)
    scaled = unit * (1.0 + gain)
    return (scaled * cos_t + pltpu.roll(scaled, HD // 2, 1) * sin_t).astype(BF16)


def norm_rope_back(d_final, raw, gain, cos_t, sin_t):
    raw = raw.astype(F32)
    inv = lax.rsqrt(jnp.mean(raw * raw, axis=-1, keepdims=True) + EPS)
    unit = raw * inv
    d_scaled = d_final * cos_t - pltpu.roll(d_final, HD // 2, 1) * sin_t
    d_gain = jnp.sum(d_scaled * unit, axis=0, keepdims=True)
    d_unit = d_scaled * (1.0 + gain)
    d_raw = inv * (d_unit - unit * jnp.mean(d_unit * unit, axis=-1, keepdims=True))
    return d_raw.astype(BF16), d_gain


def kv_kernel(x_ref, wpre_ref, wk_ref, wv_ref, kn_ref, cos_ref, sin_ref, normed_ref, kv_ref, kraw_ref):
    x = x_ref[...].astype(F32)
    inv = lax.rsqrt(jnp.mean(x * x, axis=-1, keepdims=True) + EPS)
    normed = (x * inv * (1.0 + wpre_ref[...])).astype(BF16)
    normed_ref[...] = normed
    k_raw = dot(normed, wk_ref[...]).astype(BF16)
    kraw_ref[...] = k_raw
    width = k_raw.shape[1]
    for h in range(width // HD):
        cols = slice(h * HD, (h + 1) * HD)
        kv_ref[:, cols] = norm_rope(k_raw[:, cols], kn_ref[...], cos_ref[...], sin_ref[...])
    kv_ref[:, width:] = dot(normed, wv_ref[...]).astype(BF16)


def project_kv(x, w_pre, w_k, w_v, k_norm, cos_t, sin_t, rows=256):
    seq, dim = x.shape
    width = w_k.shape[1]
    row = lambda n: pl.BlockSpec((rows, n), lambda i: (i, 0))
    return pl.pallas_call(
        kv_kernel,
        name="project_kv",
        grid=(seq // rows,),
        in_specs=[row(dim), whole((1, dim)), fixed(w_k.shape), fixed(w_v.shape), whole((1, HD)), row(HD), row(HD)],
        out_specs=[row(dim), row(2 * width), row(width)],
        out_shape=[
            jax.ShapeDtypeStruct((seq, dim), BF16),
            jax.ShapeDtypeStruct((seq, 2 * width), BF16),
            jax.ShapeDtypeStruct((seq, width), BF16),
        ],
        compiler_params=params(("arbitrary",)),
        cost_estimate=cost(4 * seq * dim * width, 4 * seq * dim + 4 * dim * width),
    )(x, w_pre, w_k, w_v, k_norm, cos_t, sin_t)


def q_kernel(normed_ref, wq_ref, qn_ref, cos_ref, sin_ref, qfin_ref, qraw_ref):
    q_raw = dot(normed_ref[...], wq_ref[...]).astype(BF16)
    for h in range(qfin_ref.shape[0]):
        part = q_raw[:, h * HD:(h + 1) * HD]
        qraw_ref[h] = part
        qfin_ref[h] = norm_rope(part, qn_ref[...], cos_ref[...], sin_ref[...])


def project_q(normed, w_q, q_norm, cos_t, sin_t, rows=256):
    seq, dim = normed.shape
    heads = w_q.shape[1] // HD
    row = lambda n: pl.BlockSpec((rows, n), lambda i: (i, 0))
    head_rows = pl.BlockSpec((heads, rows, HD), lambda i: (0, i, 0))
    shape = jax.ShapeDtypeStruct((heads, seq, HD), BF16)
    return pl.pallas_call(
        q_kernel,
        name="project_q",
        grid=(seq // rows,),
        in_specs=[row(dim), fixed(w_q.shape), whole((1, HD)), row(HD), row(HD)],
        out_specs=[head_rows, head_rows],
        out_shape=[shape, shape],
        compiler_params=params(("arbitrary",)),
        cost_estimate=cost(2 * seq * dim * heads * HD, 2 * seq * dim + 2 * dim * heads * HD),
    )(normed, w_q, q_norm, cos_t, sin_t)


def load_kv(kv_refs, k_buf, v_buf, sems):
    kv_heads = k_buf.shape[0]
    copies = []
    for s, ref in enumerate(kv_refs):
        for h in range(kv_heads):
            for t, buf in enumerate((k_buf, v_buf)):
                src = ref.at[:, pl.ds((t * kv_heads + h) * HD, HD)]
                copies.append(pltpu.make_async_copy(src, buf.at[h, s], sems.at[s, h, t]))
    for copy in copies:
        copy.start()
    for copy in copies:
        copy.wait()


def piece_place(piece, me, n_cp):
    upper = piece >= n_cp
    owner = jnp.where(upper, 2 * n_cp - 1 - piece, piece)
    return jnp.bitwise_xor(owner, me), upper.astype(jnp.int32)


def fwd_kernel(n_cp, me_ref, q_ref, *rest):
    kv_refs = rest[:n_cp]
    o_ref, lse_ref, k_buf, v_buf, m_scr, acc_scr, sems = rest[n_cp:]
    h, half = pl.program_id(0), pl.program_id(1)
    groups, rows, _ = q_ref.shape

    @pl.when((h == 0) & (half == 0))
    def _():
        load_kv(kv_refs, k_buf, v_buf, sems)

    me = me_ref[0]
    piece = jnp.where(half == 0, me, 2 * n_cp - 1 - me)
    scale = HD ** -0.5 * LOG2E
    m_scr[...] = jnp.full(m_scr.shape, NEG_BIG, F32)
    acc_scr[...] = jnp.zeros(acc_scr.shape, F32)

    def block(j, masked):
        slot, upper = piece_place(j, me, n_cp)
        span = pl.ds(pl.multiple_of(upper * rows, rows), rows)
        k = k_buf[h, slot, span, :]
        v_ext = jnp.concatenate([v_buf[h, slot, span, :], jnp.ones((rows, HD), BF16)], axis=1)
        scores = [dot(q_ref[g], k, NT) * scale for g in range(groups)]
        for g in range(groups):
            s = scores[g]
            if masked:
                q_pos = lax.broadcasted_iota(jnp.int32, s.shape, 0)
                k_pos = lax.broadcasted_iota(jnp.int32, s.shape, 1)
                s = jnp.where(k_pos <= q_pos, s, NEG_BIG)
            m_old = m_scr[g]
            m_new = jnp.maximum(m_old, jnp.max(s, axis=1, keepdims=True))
            alpha = jnp.exp2(m_old - m_new)
            p = jnp.exp2(s - jnp.concatenate([m_new] * (rows // HD), axis=1)).astype(BF16)
            acc_scr[g] = acc_scr[g] * jnp.concatenate([alpha, alpha], axis=1) + dot(p, v_ext)
            m_scr[g] = m_new

    def full(j, carry):
        block(j, False)
        return carry

    lax.fori_loop(0, piece, full, 0)
    block(piece, True)
    for g in range(groups):
        l = acc_scr[g, :, HD:]
        o_ref[:, g * HD:(g + 1) * HD] = (acc_scr[g, :, :HD] / l).astype(BF16)
        lse_ref[0, g:g + 1, :] = jnp.transpose(m_scr[g] + jnp.log2(l))[0:1, :]


def attention_fwd(me, q_fin, kv_blocks, kv_heads):
    heads, seq, _ = q_fin.shape
    n_cp = len(kv_blocks)
    groups = heads // kv_heads
    rows = seq // 2
    grid_spec = pltpu.PrefetchScalarGridSpec(
        num_scalar_prefetch=1,
        grid=(kv_heads, 2),
        in_specs=[pl.BlockSpec((groups, rows, HD), lambda h, i, *_: (h, i, 0))] + [pl.BlockSpec(memory_space=pl.ANY)] * n_cp,
        out_specs=[
            pl.BlockSpec((rows, groups * HD), lambda h, i, *_: (i, h)),
            pl.BlockSpec((1, 8, rows), lambda h, i, *_: (h, 0, i)),
        ],
        scratch_shapes=[
            pltpu.VMEM((kv_heads, n_cp, seq, HD), BF16),
            pltpu.VMEM((kv_heads, n_cp, seq, HD), BF16),
            pltpu.VMEM((groups, rows, HD), F32),
            pltpu.VMEM((groups, rows, 2 * HD), F32),
            pltpu.SemaphoreType.DMA((n_cp, kv_heads, 2)),
        ],
    )
    pairs = heads * rows * rows * (2 * n_cp + 1)
    return pl.pallas_call(
        functools.partial(fwd_kernel, n_cp),
        name="attention_fwd",
        grid_spec=grid_spec,
        out_shape=[
            jax.ShapeDtypeStruct((seq, heads * HD), BF16),
            jax.ShapeDtypeStruct((kv_heads, 8, seq), F32),
        ],
        compiler_params=params(("arbitrary", "arbitrary")),
        cost_estimate=cost(4 * pairs * HD, 8 * seq * heads * HD, pairs),
    )(me, q_fin, *kv_blocks)


def bwd_kernel(n_cp, me_ref, q_ref, do_ref, o_ref, lse_ref, qraw_ref, cos_ref, sin_ref, qn_ref, *rest):
    kv_refs = rest[:n_cp]
    dq_ref, keep_ref, send_ref, gain_ref, k_buf, v_buf, dq_scr, dkv_scr, sems = rest[n_cp:]
    h, half = pl.program_id(0), pl.program_id(1)
    groups, rows, _ = q_ref.shape

    @pl.when((h == 0) & (half == 0))
    def _():
        load_kv(kv_refs, k_buf, v_buf, sems)
        gain_ref[...] = jnp.zeros(gain_ref.shape, F32)

    @pl.when(half == 0)
    def _():
        dkv_scr[...] = jnp.zeros(dkv_scr.shape, F32)

    me = me_ref[0]
    piece = jnp.where(half == 0, me, 2 * n_cp - 1 - me)
    scale = HD ** -0.5
    delta = []
    for g in range(groups):
        prod = do_ref[g].astype(F32) * o_ref[:, g * HD:(g + 1) * HD].astype(F32)
        column = jnp.broadcast_to(jnp.sum(prod, axis=1, keepdims=True), (rows, HD))
        delta.append(jnp.transpose(column)[0:1, :])
    dq_scr[...] = jnp.zeros(dq_scr.shape, F32)

    def block(j, masked):
        slot, upper = piece_place(j, me, n_cp)
        span = pl.ds(pl.multiple_of(upper * rows, rows), rows)
        k = k_buf[h, slot, span, :]
        v = v_buf[h, slot, span, :]
        probs, d_scores = [], []
        for g in range(groups):
            s = dot(k, q_ref[g], NT)
            p = jnp.exp2(s * (scale * LOG2E) - lse_ref[0, g:g + 1, :])
            if masked:
                k_pos = lax.broadcasted_iota(jnp.int32, s.shape, 0)
                q_pos = lax.broadcasted_iota(jnp.int32, s.shape, 1)
                p = jnp.where(k_pos <= q_pos, p, 0.0)
            probs.append(p.astype(BF16))
            d_scores.append((p * (dot(v, do_ref[g], NT) - delta[g])).astype(BF16))
        for g in range(groups):
            dq_scr[g] += dot(d_scores[g], k, TN)
        index = (slot % 2) * (n_cp // 2) + slot // 2
        d_all = jnp.concatenate(d_scores, axis=1)
        p_all = jnp.concatenate(probs, axis=1)
        dkv_scr[index, 0, span, :] += dot(d_all, q_ref[...].reshape(groups * rows, HD)) * scale
        dkv_scr[index, 1, span, :] += dot(p_all, do_ref[...].reshape(groups * rows, HD))

    def full(j, carry):
        block(j, False)
        return carry

    lax.fori_loop(0, piece, full, 0)
    block(piece, True)
    for g in range(groups):
        d_raw, d_gain = norm_rope_back(dq_scr[g] * scale, qraw_ref[g], qn_ref[...], cos_ref[...], sin_ref[...])
        dq_ref[:, g * HD:(g + 1) * HD] = d_raw
        gain_ref[0:1, :] += d_gain

    @pl.when(half == 1)
    def _():
        for i in range(n_cp // 2):
            keep_ref[i, :, 0] = dkv_scr[i]
            send_ref[i, :, 0] = dkv_scr[n_cp // 2 + i]


def attention_bwd(me, q_fin, d_out, out, lse, q_raw, cos_t, sin_t, q_norm, kv_blocks, kv_heads):
    heads, seq, _ = q_fin.shape
    n_cp = len(kv_blocks)
    groups = heads // kv_heads
    rows = seq // 2
    by_head = pl.BlockSpec((groups, rows, HD), lambda h, i, *_: (h, i, 0))
    by_row = pl.BlockSpec((rows, groups * HD), lambda h, i, *_: (i, h))
    table = pl.BlockSpec((rows, HD), lambda h, i, *_: (i, 0))
    by_owner = pl.BlockSpec((n_cp // 2, 2, 1, seq, HD), lambda h, i, *_: (0, 0, h, 0, 0))
    kv_grads = jax.ShapeDtypeStruct((n_cp // 2, 2, kv_heads, seq, HD), F32)
    grid_spec = pltpu.PrefetchScalarGridSpec(
        num_scalar_prefetch=1,
        grid=(kv_heads, 2),
        in_specs=[
            by_head,
            by_head,
            by_row,
            pl.BlockSpec((1, 8, rows), lambda h, i, *_: (h, 0, i)),
            by_head,
            table,
            table,
            whole((1, HD)),
        ] + [pl.BlockSpec(memory_space=pl.ANY)] * n_cp,
        out_specs=[
            by_row,
            by_owner,
            by_owner,
            whole((8, HD)),
        ],
        scratch_shapes=[
            pltpu.VMEM((kv_heads, n_cp, seq, HD), BF16),
            pltpu.VMEM((kv_heads, n_cp, seq, HD), BF16),
            pltpu.VMEM((groups, rows, HD), F32),
            pltpu.VMEM((n_cp, 2, seq, HD), F32),
            pltpu.SemaphoreType.DMA((n_cp, kv_heads, 2)),
        ],
    )
    pairs = heads * rows * rows * (2 * n_cp + 1)
    return pl.pallas_call(
        functools.partial(bwd_kernel, n_cp),
        name="attention_bwd",
        grid_spec=grid_spec,
        out_shape=[
            jax.ShapeDtypeStruct((seq, heads * HD), BF16),
            kv_grads,
            kv_grads,
            jax.ShapeDtypeStruct((8, HD), F32),
        ],
        compiler_params=params(("arbitrary", "arbitrary")),
        cost_estimate=cost(10 * pairs * HD, 16 * seq * heads * HD, pairs),
    )(me, q_fin, d_out, out, lse, q_raw, cos_t, sin_t, q_norm, *kv_blocks)


def post_kernel(n_w, share_ref, o_ref, *rest):
    w_refs = rest[:n_w]
    wmine_ref, x_ref, dy_ref, wpost_ref, y_ref, dattn_ref, do_ref, dpost_ref, attn_scr = rest[n_w:]
    n_tp = o_ref.shape[0]
    out_all = jnp.concatenate([o_ref[t] for t in range(n_tp)], axis=1)
    for s in range(n_w):
        attn_scr[jnp.bitwise_xor(share_ref[0], s)] = dot(out_all, w_refs[s][...])
    attn = jnp.concatenate([attn_scr[s] for s in range(n_w)], axis=1)
    inv = lax.rsqrt(jnp.mean(attn * attn, axis=-1, keepdims=True) + EPS)
    unit = attn * inv
    gain = 1.0 + wpost_ref[...]
    y_ref[...] = (x_ref[...].astype(F32) + unit * gain).astype(BF16)
    dy = dy_ref[...].astype(F32)

    @pl.when(pl.program_id(0) == 0)
    def _():
        dpost_ref[...] = jnp.zeros(dpost_ref.shape, F32)

    dpost_ref[0:1, :] += jnp.sum(dy * unit, axis=0, keepdims=True)
    d_unit = dy * gain
    d_attn = (inv * (d_unit - unit * jnp.mean(d_unit * unit, axis=-1, keepdims=True))).astype(BF16)
    dattn_ref[...] = d_attn
    d_out = dot(d_attn, wmine_ref[...], NT)
    for h in range(do_ref.shape[0]):
        do_ref[h] = d_out[:, h * HD:(h + 1) * HD].astype(BF16)


def post(share, out_all, w_all, w_mine, x, dy, w_post, rows=256):
    n_tp, seq, width = out_all.shape
    dim = x.shape[1]
    heads = width // HD
    n_w = len(w_all)
    row = pl.BlockSpec((rows, dim), lambda i, *_: (i, 0))
    grid_spec = pltpu.PrefetchScalarGridSpec(
        num_scalar_prefetch=1,
        grid=(seq // rows,),
        in_specs=[pl.BlockSpec((n_tp, rows, width), lambda i, *_: (0, i, 0))]
        + [fixed(w.shape) for w in w_all]
        + [fixed(w_mine.shape), row, row, whole((1, dim))],
        out_specs=[row, row, pl.BlockSpec((heads, rows, HD), lambda i, *_: (0, i, 0)), whole((8, dim))],
        scratch_shapes=[pltpu.VMEM((n_w, rows, dim // n_w), F32)],
    )
    return pl.pallas_call(
        functools.partial(post_kernel, n_w),
        name="post",
        grid_spec=grid_spec,
        out_shape=[
            jax.ShapeDtypeStruct((seq, dim), BF16),
            jax.ShapeDtypeStruct((seq, dim), BF16),
            jax.ShapeDtypeStruct((heads, seq, HD), BF16),
            jax.ShapeDtypeStruct((8, dim), F32),
        ],
        compiler_params=params(("arbitrary",)),
        cost_estimate=cost(2 * seq * dim * width * (n_tp + 1), 8 * seq * dim + 2 * dim * width * (n_tp + 1)),
    )(share, out_all, *w_all, w_mine, x, dy, w_post)


def kback_kernel(own_ref, near_ref, far_ref, kraw_ref, cos_ref, sin_ref, kn_ref, out_ref, gain_ref):
    @pl.when(pl.program_id(0) == 0)
    def _():
        gain_ref[...] = jnp.zeros(gain_ref.shape, F32)

    kv_heads = own_ref.shape[2]
    for h in range(kv_heads):
        cols = slice(h * HD, (h + 1) * HD)
        d_k = own_ref[0, 0, h] + near_ref[0, 0, h] + far_ref[0, h]
        d_raw, d_gain = norm_rope_back(d_k, kraw_ref[:, cols], kn_ref[...], cos_ref[...], sin_ref[...])
        out_ref[:, cols] = d_raw
        gain_ref[0:1, :] += d_gain
        d_v = own_ref[0, 1, h] + near_ref[0, 1, h] + far_ref[1, h]
        out_ref[:, (kv_heads + h) * HD:(kv_heads + h + 1) * HD] = d_v.astype(BF16)


def key_back(dkv, near, far, k_raw, cos_t, sin_t, k_norm, rows=256):
    _, _, kv_heads, seq, _ = dkv.shape
    full = pl.BlockSpec((1, 2, kv_heads, rows, HD), lambda i: (0, 0, 0, i, 0))
    row = lambda n: pl.BlockSpec((rows, n), lambda i: (i, 0))
    return pl.pallas_call(
        kback_kernel,
        name="key_back",
        grid=(seq // rows,),
        in_specs=[
            full,
            full,
            pl.BlockSpec((2, kv_heads, rows, HD), lambda i: (0, 0, i, 0)),
            row(kv_heads * HD),
            row(HD),
            row(HD),
            whole((1, HD)),
        ],
        out_specs=[row(2 * kv_heads * HD), whole((8, HD))],
        out_shape=[
            jax.ShapeDtypeStruct((seq, 2 * kv_heads * HD), BF16),
            jax.ShapeDtypeStruct((8, HD), F32),
        ],
        compiler_params=params(("arbitrary",)),
        cost_estimate=cost(50 * seq * kv_heads * HD, 12 * seq * kv_heads * HD),
    )(dkv, near, far, k_raw, cos_t, sin_t, k_norm)


def dx_kernel(n_tp, tp_ref, *refs):
    q_refs, kv_refs = refs[:n_tp], refs[n_tp:2 * n_tp]
    w_ref, x_ref, dy_ref, wpre_ref, dx_ref, dpre_ref, acc = refs[2 * n_tp:]
    i = pl.program_id(0)
    split = q_refs[0].shape[1]
    total = None
    for s in range(n_tp):
        t = lax.rem(tp_ref[0] + n_tp - s, n_tp)
        part = dot(q_refs[s][...], w_ref[t, :, :split], NT) + dot(kv_refs[s][...], w_ref[t, :, split:], NT)
        total = part if total is None else total + part
    acc[i] = total

    @pl.when(i == pl.num_programs(0) - 1)
    def _():
        d_normed = jnp.concatenate([acc[t] for t in range(acc.shape[0])], axis=1)
        x = x_ref[...].astype(F32)
        inv = lax.rsqrt(jnp.mean(x * x, axis=-1, keepdims=True) + EPS)
        unit = x * inv
        dpre_ref[...] = jnp.broadcast_to(jnp.sum(d_normed * unit, axis=0, keepdims=True), dpre_ref.shape)
        d_unit = d_normed * (1.0 + wpre_ref[...])
        d_x = inv * (d_unit - unit * jnp.mean(d_unit * unit, axis=-1, keepdims=True))
        dx_ref[...] = (dy_ref[...].astype(F32) + d_x).astype(BF16)


def input_grad(tp, q_grads, kv_grads, w_all, x, dy, w_pre, cols=512):
    n_tp = len(q_grads)
    rows, q_width = q_grads[0].shape
    kv_width = kv_grads[0].shape[1]
    dim = x.shape[1]
    here = pl.BlockSpec((rows, dim), lambda i, t: (t[0], 0))
    grid_spec = pltpu.PrefetchScalarGridSpec(
        num_scalar_prefetch=1,
        grid=(dim // cols,),
        in_specs=[whole((rows, q_width))] * n_tp
        + [whole((rows, kv_width))] * n_tp
        + [pl.BlockSpec((n_tp, cols, q_width + kv_width), lambda i, *_: (0, i, 0)), here, here, whole((1, dim))],
        out_specs=[whole((rows, dim)), whole((8, dim))],
        scratch_shapes=[pltpu.VMEM((dim // cols, rows, cols), F32)],
    )
    return pl.pallas_call(
        functools.partial(dx_kernel, n_tp),
        name="input_grad",
        grid_spec=grid_spec,
        out_shape=[jax.ShapeDtypeStruct((rows, dim), BF16), jax.ShapeDtypeStruct((8, dim), F32)],
        compiler_params=params(("arbitrary",)),
        cost_estimate=cost(2 * n_tp * rows * (q_width + kv_width) * dim, 2 * n_tp * (q_width + kv_width) * dim),
    )(tp, *q_grads, *kv_grads, w_all, x, dy, w_pre)


def dw_kernel(n_cp, me_ref, *refs):
    n_refs, q_refs, kv_refs = refs[:n_cp], refs[n_cp:2 * n_cp], refs[2 * n_cp:3 * n_cp]
    dwq_ref, dwk_ref, dwv_ref, n_buf, g_buf, n_sem, g_sem = refs[3 * n_cp:]
    i = pl.program_id(0)
    cols = n_buf.shape[3]
    seq, q_width = q_refs[0].shape
    kv_width = kv_refs[0].shape[1]
    me = me_ref[0]

    def fetch(step, par):
        span = pl.ds(pl.multiple_of(step * cols, cols), cols)
        return [
            pltpu.make_async_copy(n_refs[s].at[:, span], n_buf.at[par, jnp.bitwise_xor(me, s)], n_sem.at[par, s])
            for s in range(n_cp)
        ]

    @pl.when(i == 0)
    def _():
        copies = fetch(0, 0)
        for s in range(n_cp):
            owner = jnp.bitwise_xor(me, s)
            copies.append(pltpu.make_async_copy(q_refs[s], g_buf.at[owner, :, pl.ds(0, q_width)], g_sem.at[s, 0]))
            copies.append(pltpu.make_async_copy(kv_refs[s], g_buf.at[owner, :, pl.ds(q_width, kv_width)], g_sem.at[s, 1]))
        for copy in copies:
            copy.start()
        for copy in copies[n_cp:]:
            copy.wait()

    @pl.when(i + 1 < pl.num_programs(0))
    def _():
        for copy in fetch(i + 1, (i + 1) % 2):
            copy.start()

    for copy in fetch(i, i % 2):
        copy.wait()
    lhs = n_buf[i % 2].reshape(n_cp * seq, cols)
    grad = dot(lhs, g_buf[...].reshape(n_cp * seq, q_width + kv_width), TN)
    dwq_ref[...] = grad[:, :q_width]
    dwk_ref[...] = grad[:, q_width:q_width + kv_width // 2]
    dwv_ref[...] = grad[:, q_width + kv_width // 2:]


def weight_grads(me, normed, q_grads, kv_grads, cols=256):
    n_cp = len(normed)
    seq, dim = normed[0].shape
    q_width, kv_width = q_grads[0].shape[1], kv_grads[0].shape[1]
    anywhere = pl.BlockSpec(memory_space=pl.ANY)
    tile = lambda n: pl.BlockSpec((cols, n), lambda i, *_: (i, 0))
    grid_spec = pltpu.PrefetchScalarGridSpec(
        num_scalar_prefetch=1,
        grid=(dim // cols,),
        in_specs=[anywhere] * (3 * n_cp),
        out_specs=[tile(q_width), tile(kv_width // 2), tile(kv_width // 2)],
        scratch_shapes=[
            pltpu.VMEM((2, n_cp, seq, cols), BF16),
            pltpu.VMEM((n_cp, seq, q_width + kv_width), BF16),
            pltpu.SemaphoreType.DMA((2, n_cp)),
            pltpu.SemaphoreType.DMA((n_cp, 2)),
        ],
    )
    return pl.pallas_call(
        functools.partial(dw_kernel, n_cp),
        name="weight_grads",
        grid_spec=grid_spec,
        out_shape=[
            jax.ShapeDtypeStruct((dim, q_width), F32),
            jax.ShapeDtypeStruct((dim, kv_width // 2), F32),
            jax.ShapeDtypeStruct((dim, kv_width // 2), F32),
        ],
        compiler_params=params(("arbitrary",)),
        cost_estimate=cost(2 * n_cp * seq * dim * (q_width + kv_width), 2 * n_cp * seq * (dim + q_width + kv_width)),
    )(me, *normed, *q_grads, *kv_grads)


def join_kernel(core_ref, keep_ref, other_ref, out_ref):
    half = pl.program_id(0) // (pl.num_programs(0) // 2)

    @pl.when(half == core_ref[0])
    def _():
        out_ref[...] = keep_ref[...]

    @pl.when(half != core_ref[0])
    def _():
        out_ref[...] = other_ref[...]


def join_halves(core, keep, other, rows=128):
    half, width = keep.shape
    n = half // rows
    grid_spec = pltpu.PrefetchScalarGridSpec(
        num_scalar_prefetch=1,
        grid=(2 * n,),
        in_specs=[
            pl.BlockSpec((rows, width), lambda i, c: (jnp.clip(i - c[0] * n, 0, n - 1), 0)),
            pl.BlockSpec((rows, width), lambda i, c: (jnp.clip(i - (1 - c[0]) * n, 0, n - 1), 0)),
        ],
        out_specs=pl.BlockSpec((rows, width), lambda i, c: (i, 0)),
    )
    return pl.pallas_call(
        join_kernel,
        name="join_halves",
        grid_spec=grid_spec,
        out_shape=jax.ShapeDtypeStruct((2 * half, width), F32),
        compiler_params=params(("arbitrary",)),
        cost_estimate=cost(half * width, 16 * half * width),
    )(core, keep, other)


def solution(mesh):
    n_cp, n_tp, n_dp = mesh.shape["cp"], mesh.shape["tp"], mesh.shape["dp"]
    near = [(i, i ^ 1) for i in range(n_cp)]
    across = [(i, i ^ 2) for i in range(n_cp)]
    beside = [(i, i ^ 1) for i in range(n_dp)]

    def from_cp(value):
        far = lax.ppermute(value, "cp", across)
        return [value, lax.ppermute(value, "cp", near), far, lax.ppermute(far, "cp", near)]

    def per_device(hidden, cotangent, pos_loc, w_q, w_k, w_v, w_o, w_pre, w_post, q_norm, k_norm):
        _, seq, dim = hidden.shape
        x, dy = hidden[0], cotangent[0]
        kv_heads = w_k.shape[1] // HD
        cp, tp, dp = (lax.axis_index(a).astype(jnp.int32) for a in ("cp", "tp", "dp"))
        core = cp % 2
        me, one_tp, one_core = cp.reshape(1), tp.reshape(1), core.reshape(1)

        share = dp * 2 + core
        cols = dim // (2 * n_dp)
        mine = lax.all_gather(lax.dynamic_slice_in_dim(w_o, share * cols, cols, 1), "tp", axis=0, tiled=True)
        w_o_all = [mine, lax.ppermute(mine, "cp", near)]
        if n_dp == 2:
            w_o_all.append(lax.ppermute(mine, "dp", beside))
            w_o_all.append(lax.ppermute(w_o_all[2], "cp", near))

        cos_t, sin_t = rope_tables(pos_loc)
        qn, kn = q_norm.reshape(1, HD), k_norm.reshape(1, HD)
        wpre, wpost = w_pre.reshape(1, dim), w_post.reshape(1, dim)
        normed, kv_own, k_raw = project_kv(x, wpre, w_k, w_v, kn, cos_t, sin_t)
        kv_blocks = from_cp(kv_own)
        q_fin, q_raw = project_q(normed, w_q, qn, cos_t, sin_t)
        normed_out, _ = lax.optimization_barrier((normed, kv_blocks[2]))
        normed_all = from_cp(normed_out)
        out, lse = attention_fwd(me, q_fin, kv_blocks, kv_heads)

        out_sent, _ = lax.optimization_barrier((out, mine))
        out_all = lax.all_gather(out_sent, "tp", axis=0, tiled=False)
        y, d_attn, d_out, d_post = post(share.reshape(1), out_all, w_o_all, w_o, x, dy, wpost)

        eighth = dp * n_cp + cp
        w_rows = dim // (n_dp * n_cp)
        parts = [lax.dynamic_slice_in_dim(w, eighth * w_rows, w_rows, 0) for w in (w_q, w_k, w_v)]
        fence, _ = lax.optimization_barrier((jnp.concatenate(parts, axis=1), out_all))
        w_all = lax.all_gather(fence, ("tp", "dp", "cp"), axis=0, tiled=True).reshape(n_tp, dim, fence.shape[1])

        half = w_o.shape[0] // 2
        give = dot(lax.dynamic_slice_in_dim(out, (1 - core) * half, half, 1), d_attn, TN)
        got = lax.ppermute(give, "cp", near)
        keep = dot(lax.dynamic_slice_in_dim(out, core * half, half, 1), d_attn, TN) + got
        keep, d_out = lax.optimization_barrier((keep, d_out))
        keep = keep + lax.ppermute(keep, "cp", across)
        other = lax.ppermute(keep, "cp", near)
        d_wo = join_halves(one_core, keep, other)

        dq, dkv, dkv_send, dq_gain = attention_bwd(
            me, q_fin, d_out, out, lse, q_raw, cos_t, sin_t, qn, kv_blocks, kv_heads
        )
        got = lax.ppermute(dkv_send, "cp", near)
        dkv_far = lax.ppermute(dkv[1] + got[1], "cp", across)
        d_kv, dk_gain = key_back(dkv, got, dkv_far, k_raw, cos_t, sin_t, kn)

        rows = seq // n_tp

        def exchange_rows(value):
            pieces = [lax.dynamic_slice_in_dim(value, tp * rows, rows, 0)]
            for s in range(1, n_tp):
                part = lax.dynamic_slice_in_dim(value, ((tp + s) % n_tp) * rows, rows, 0)
                pieces.append(lax.ppermute(part, "tp", [(i, (i + s) % n_tp) for i in range(n_tp)]))
            return pieces

        dq_rows = exchange_rows(dq)
        dq_all = from_cp(dq)
        dkv_rows = exchange_rows(d_kv)
        dx_rows, d_pre = input_grad(one_tp, dq_rows, dkv_rows, w_all, x, dy, wpre)
        d_hidden = lax.all_gather(dx_rows, "tp", axis=0, tiled=True)

        dkv_all = from_cp(d_kv)
        d_wq, d_wk, d_wv = weight_grads(me, normed_all, dq_all, dkv_all)

        small = jnp.concatenate([jnp.where(tp == 0, d_post[0], 0.0), d_pre[0], dq_gain[0], dk_gain[0]])
        small = small + lax.ppermute(small, "cp", near)
        small = small + lax.ppermute(small, "cp", across)
        small = small + lax.ppermute(small, "tp", [(i, i ^ 1) for i in range(n_tp)])
        small = small + lax.ppermute(small, "tp", [(i, i ^ 2) for i in range(n_tp)])
        d_post, d_pre = small[:dim], small[dim:2 * dim]
        d_qn, d_kn = small[2 * dim:2 * dim + HD], small[2 * dim + HD:]
        return y[None], d_hidden[None], d_wq, d_wk, d_wv, d_wo, d_pre, d_post, d_qn, d_kn

    specs_in = (P('dp', 'cp', None), P('dp', 'cp', None), P(('dp', 'cp')), P(None, 'tp'), P(None, 'tp'), P(None, 'tp'), P('tp', None), P(None), P(None), P(None), P(None))
    specs_out = (P('dp', 'cp', None), P('dp', 'cp', None), P('dp', 'tp'), P('dp', 'tp'), P('dp', 'tp'), P(('dp', 'tp'), None), P('dp'), P('dp'), P('dp'), P('dp'))
    return jax.shard_map(per_device, mesh=mesh, in_specs=specs_in, out_specs=specs_out, check_vma=False)
```

```python
import functools

import jax
import jax.numpy as jnp
from jax import lax
from jax.experimental import pallas as pl
from jax.experimental.pallas import tpu as pltpu
from jax.sharding import PartitionSpec as P


EPS = 1e-6
ROPE_BASE = 1000000.0
ROPE_SCALE = 8.0
NEG_BIG = -1e30
LOG2E = 1.4426950408889634
HD = 128
F32 = jnp.float32
BF16 = jnp.bfloat16
VMEM_MAX = 60 * 1024 * 1024
VMEM_TOP = 67043328
NT = (((1,), (1,)), ((), ()))
TN = (((0,), (0,)), ((), ()))


def dot(a, b, dims=(((1,), (0,)), ((), ()))):
    return lax.dot_general(a, b, dims, preferred_element_type=F32)


def params(dims, vmem=VMEM_MAX):
    return pltpu.CompilerParams(dimension_semantics=("arbitrary",) * dims, vmem_limit_bytes=vmem)


def cost(flops, nbytes, trans=0):
    return pl.CostEstimate(flops=int(flops), bytes_accessed=int(nbytes), transcendentals=int(trans))


def whole(shape):
    return pl.BlockSpec(shape, lambda *_: (0,) * len(shape))


def fixed(shape):
    return pl.BlockSpec(shape, lambda *_: (0,) * len(shape), pipeline_mode=pl.Buffered(buffer_count=1))


def rope_tables(pos_loc):
    half_dim = HD // 2
    inv_freq = 1.0 / (ROPE_SCALE * ROPE_BASE ** (jnp.arange(half_dim, dtype=F32) * (2.0 / HD)))
    angles = pos_loc.astype(F32)[:, None] * inv_freq[None, :]
    cos_t, sin_t = jnp.cos(angles), jnp.sin(angles)
    return jnp.concatenate([cos_t, cos_t], axis=-1), jnp.concatenate([-sin_t, sin_t], axis=-1)


def norm_rope(raw, gain, cos_t, sin_t):
    raw = raw.astype(F32)
    unit = raw * lax.rsqrt(jnp.mean(raw * raw, axis=-1, keepdims=True) + EPS)
    scaled = unit * (1.0 + gain)
    return (scaled * cos_t + pltpu.roll(scaled, HD // 2, 1) * sin_t).astype(BF16)


def norm_rope_back(d_final, raw, gain, cos_t, sin_t):
    raw = raw.astype(F32)
    inv = lax.rsqrt(jnp.mean(raw * raw, axis=-1, keepdims=True) + EPS)
    unit = raw * inv
    d_scaled = d_final * cos_t - pltpu.roll(d_final, HD // 2, 1) * sin_t
    d_gain = jnp.sum(d_scaled * unit, axis=0, keepdims=True)
    d_unit = d_scaled * (1.0 + gain)
    d_raw = inv * (d_unit - unit * jnp.mean(d_unit * unit, axis=-1, keepdims=True))
    return d_raw.astype(BF16), d_gain


def kv_kernel(x_ref, wpre_ref, wk_ref, wv_ref, kn_ref, cos_ref, sin_ref, normed_ref, kv_ref, kraw_ref):
    x = x_ref[...].astype(F32)
    inv = lax.rsqrt(jnp.mean(x * x, axis=-1, keepdims=True) + EPS)
    normed = (x * inv * (1.0 + wpre_ref[...])).astype(BF16)
    normed_ref[...] = normed
    k_raw = dot(normed, wk_ref[...]).astype(BF16)
    kraw_ref[...] = k_raw
    width = k_raw.shape[1]
    for h in range(width // HD):
        cols = slice(h * HD, (h + 1) * HD)
        kv_ref[:, cols] = norm_rope(k_raw[:, cols], kn_ref[...], cos_ref[...], sin_ref[...])
    kv_ref[:, width:] = dot(normed, wv_ref[...]).astype(BF16)


def project_kv(x, w_pre, w_k, w_v, k_norm, cos_t, sin_t, rows=256):
    seq, dim = x.shape
    width = w_k.shape[1]
    row = lambda n: pl.BlockSpec((rows, n), lambda i: (i, 0))
    return pl.pallas_call(
        kv_kernel,
        name="pkv",
        grid=(seq // rows,),
        in_specs=[row(dim), whole((1, dim)), fixed(w_k.shape), fixed(w_v.shape), whole((1, HD)), row(HD), row(HD)],
        out_specs=[row(dim), row(2 * width), row(width)],
        out_shape=[
            jax.ShapeDtypeStruct((seq, dim), BF16),
            jax.ShapeDtypeStruct((seq, 2 * width), BF16),
            jax.ShapeDtypeStruct((seq, width), BF16),
        ],
        compiler_params=params(1),
        cost_estimate=cost(4 * seq * dim * width, 4 * seq * dim + 4 * dim * width),
    )(x, w_pre, w_k, w_v, k_norm, cos_t, sin_t)


def q_kernel(normed_ref, wq_ref, qn_ref, cos_ref, sin_ref, qfin_ref, qraw_ref):
    q_raw = dot(normed_ref[...], wq_ref[...]).astype(BF16)
    for h in range(qfin_ref.shape[0]):
        part = q_raw[:, h * HD:(h + 1) * HD]
        qraw_ref[h] = part
        qfin_ref[h] = norm_rope(part, qn_ref[...], cos_ref[...], sin_ref[...])


def project_q(normed, w_q, q_norm, cos_t, sin_t, rows=256):
    seq, dim = normed.shape
    heads = w_q.shape[1] // HD
    row = lambda n: pl.BlockSpec((rows, n), lambda i: (i, 0))
    head_rows = pl.BlockSpec((heads, rows, HD), lambda i: (0, i, 0))
    shape = jax.ShapeDtypeStruct((heads, seq, HD), BF16)
    return pl.pallas_call(
        q_kernel,
        name="pq",
        grid=(seq // rows,),
        in_specs=[row(dim), fixed(w_q.shape), whole((1, HD)), row(HD), row(HD)],
        out_specs=[head_rows, head_rows],
        out_shape=[shape, shape],
        compiler_params=params(1),
        cost_estimate=cost(2 * seq * dim * heads * HD, 2 * seq * dim + 2 * dim * heads * HD),
    )(normed, w_q, q_norm, cos_t, sin_t)


def load_kv(kv_refs, k_buf, v_buf, sems, heads):
    kv_heads = kv_refs[0].shape[1] // (2 * HD)
    copies = []
    for s, ref in enumerate(kv_refs):
        for i, h in enumerate(heads):
            for t, buf in enumerate((k_buf, v_buf)):
                src = ref.at[:, pl.ds((t * kv_heads + h) * HD, HD)]
                copies.append(pltpu.make_async_copy(src, buf.at[i, s], sems.at[s, i, t]))
    for copy in copies:
        copy.start()
    for copy in copies:
        copy.wait()


def piece_place(piece, me, n_cp):
    upper = piece >= n_cp
    owner = jnp.where(upper, 2 * n_cp - 1 - piece, piece)
    return jnp.bitwise_xor(owner, me), upper.astype(jnp.int32)


def fwd_kernel(n_cp, me_ref, q_ref, *rest):
    kv_refs = rest[:n_cp]
    o_ref, lse_ref, k_buf, v_buf, m_scr, acc_scr, sems = rest[n_cp:]
    h, half = pl.program_id(0), pl.program_id(1)
    groups, rows, _ = q_ref.shape

    @pl.when((h == 0) & (half == 0))
    def _():
        load_kv(kv_refs, k_buf, v_buf, sems, range(k_buf.shape[0]))

    me = me_ref[0]
    piece = jnp.where(half == 0, me, 2 * n_cp - 1 - me)
    scale = HD ** -0.5 * LOG2E
    m_scr[...] = jnp.full(m_scr.shape, NEG_BIG, F32)
    acc_scr[...] = jnp.zeros(acc_scr.shape, F32)

    def block(j, masked):
        slot, upper = piece_place(j, me, n_cp)
        span = pl.ds(pl.multiple_of(upper * rows, rows), rows)
        k = k_buf[h, slot, span, :]
        v_ext = jnp.concatenate([v_buf[h, slot, span, :], jnp.ones((rows, HD), BF16)], axis=1)
        scores = [dot(q_ref[g], k, NT) * scale for g in range(groups)]
        for g in range(groups):
            s = scores[g]
            if masked:
                q_pos = lax.broadcasted_iota(jnp.int32, s.shape, 0)
                k_pos = lax.broadcasted_iota(jnp.int32, s.shape, 1)
                s = jnp.where(k_pos <= q_pos, s, NEG_BIG)
            m_old = m_scr[g]
            m_new = jnp.maximum(m_old, jnp.max(s, axis=1, keepdims=True))
            alpha = jnp.exp2(m_old - m_new)
            p = jnp.exp2(s - jnp.concatenate([m_new] * (rows // HD), axis=1)).astype(BF16)
            acc_scr[g] = acc_scr[g] * jnp.concatenate([alpha, alpha], axis=1) + dot(p, v_ext)
            m_scr[g] = m_new

    def full(j, carry):
        block(j, False)
        return carry

    lax.fori_loop(0, piece, full, 0)
    block(piece, True)
    for g in range(groups):
        l = acc_scr[g, :, HD:]
        o_ref[:, g * HD:(g + 1) * HD] = (acc_scr[g, :, :HD] / l).astype(BF16)
        lse_ref[0, g:g + 1, :] = jnp.transpose(m_scr[g] + jnp.log2(l))[0:1, :]


def attention_fwd(me, q_fin, kv_blocks, kv_heads):
    heads, seq, _ = q_fin.shape
    n_cp = len(kv_blocks)
    groups = heads // kv_heads
    rows = seq // 2
    grid_spec = pltpu.PrefetchScalarGridSpec(
        num_scalar_prefetch=1,
        grid=(kv_heads, 2),
        in_specs=[pl.BlockSpec((groups, rows, HD), lambda h, i, *_: (h, i, 0))] + [pl.BlockSpec(memory_space=pl.ANY)] * n_cp,
        out_specs=[
            pl.BlockSpec((rows, groups * HD), lambda h, i, *_: (i, h)),
            pl.BlockSpec((1, 8, rows), lambda h, i, *_: (h, 0, i)),
        ],
        scratch_shapes=[
            pltpu.VMEM((kv_heads, n_cp, seq, HD), BF16),
            pltpu.VMEM((kv_heads, n_cp, seq, HD), BF16),
            pltpu.VMEM((groups, rows, HD), F32),
            pltpu.VMEM((groups, rows, 2 * HD), F32),
            pltpu.SemaphoreType.DMA((n_cp, kv_heads, 2)),
        ],
    )
    pairs = heads * rows * rows * (2 * n_cp + 1)
    return pl.pallas_call(
        functools.partial(fwd_kernel, n_cp),
        name="fwd",
        grid_spec=grid_spec,
        out_shape=[
            jax.ShapeDtypeStruct((seq, heads * HD), BF16),
            jax.ShapeDtypeStruct((kv_heads, 8, seq), F32),
        ],
        compiler_params=params(2),
        cost_estimate=cost(4 * pairs * HD, 8 * seq * heads * HD, pairs),
    )(me, q_fin, *kv_blocks)


def bwd_kernel(n_cp, head, me_ref, q_ref, do_ref, o_ref, lse_ref, qraw_ref, cos_ref, sin_ref, qn_ref, *rest):
    kv_refs = rest[:n_cp]
    dq_ref, keep_ref, send_ref, gain_ref, k_buf, v_buf, dq_scr, dkv_scr, sems = rest[-9:]
    half = pl.program_id(0)
    groups, rows, _ = q_ref.shape

    @pl.when(half == 0)
    def _():
        load_kv(kv_refs, k_buf, v_buf, sems, (head,))
        gain_ref[...] = jnp.zeros(gain_ref.shape, F32)
        dkv_scr[...] = jnp.zeros(dkv_scr.shape, F32)

    me = me_ref[0]
    piece = jnp.where(half == 0, me, 2 * n_cp - 1 - me)
    scale = HD ** -0.5
    delta = []
    for g in range(groups):
        prod = do_ref[g].astype(F32) * o_ref[:, g * HD:(g + 1) * HD].astype(F32)
        column = jnp.broadcast_to(jnp.sum(prod, axis=1, keepdims=True), (rows, HD))
        delta.append(jnp.transpose(column)[0:1, :])
    dq_scr[...] = jnp.zeros(dq_scr.shape, F32)

    def block(j, masked):
        slot, upper = piece_place(j, me, n_cp)
        span = pl.ds(pl.multiple_of(upper * rows, rows), rows)
        k = k_buf[0, slot, span, :]
        v = v_buf[0, slot, span, :]
        probs, d_scores = [], []
        for g in range(groups):
            s = dot(k, q_ref[g], NT)
            p = jnp.exp2(s * (scale * LOG2E) - lse_ref[0, g:g + 1, :])
            if masked:
                k_pos = lax.broadcasted_iota(jnp.int32, s.shape, 0)
                q_pos = lax.broadcasted_iota(jnp.int32, s.shape, 1)
                p = jnp.where(k_pos <= q_pos, p, 0.0)
            probs.append(p.astype(BF16))
            d_scores.append((p * (dot(v, do_ref[g], NT) - delta[g])).astype(BF16))
        for g in range(groups):
            dq_scr[g] += dot(d_scores[g], k, TN)
        index = (slot % 2) * (n_cp // 2) + slot // 2
        d_all = jnp.concatenate(d_scores, axis=1)
        p_all = jnp.concatenate(probs, axis=1)
        dkv_scr[index, 0, span, :] += dot(d_all, q_ref[...].reshape(groups * rows, HD)) * scale
        dkv_scr[index, 1, span, :] += dot(p_all, do_ref[...].reshape(groups * rows, HD))

    def full(j, carry):
        block(j, False)
        return carry

    lax.fori_loop(0, piece, full, 0)
    block(piece, True)
    for g in range(groups):
        d_raw, d_gain = norm_rope_back(dq_scr[g] * scale, qraw_ref[g], qn_ref[...], cos_ref[...], sin_ref[...])
        dq_ref[:, g * HD:(g + 1) * HD] = d_raw
        gain_ref[0:1, :] += d_gain

    @pl.when(half == 1)
    def _():
        for i in range(n_cp // 2):
            keep_ref[i] = dkv_scr[i]
            send_ref[i] = dkv_scr[n_cp // 2 + i]


def attention_bwd(head, me, q_fin, d_out, out, lse, q_raw, cos_t, sin_t, q_norm, kv_blocks, kv_heads, dq=None):
    heads, seq, _ = q_fin.shape
    n_cp = len(kv_blocks)
    groups = heads // kv_heads
    rows = seq // 2
    by_head = pl.BlockSpec((groups, rows, HD), lambda i, *_: (head, i, 0))
    by_row = pl.BlockSpec((rows, groups * HD), lambda i, *_: (i, head))
    table = pl.BlockSpec((rows, HD), lambda i, *_: (i, 0))
    anywhere = pl.BlockSpec(memory_space=pl.ANY)
    kv_grads = jax.ShapeDtypeStruct((n_cp // 2, 2, seq, HD), F32)
    extra = () if dq is None else (dq,)
    grid_spec = pltpu.PrefetchScalarGridSpec(
        num_scalar_prefetch=1,
        grid=(2,),
        in_specs=[
            by_head,
            by_head,
            by_row,
            pl.BlockSpec((1, 8, rows), lambda i, *_: (head, 0, i)),
            by_head,
            table,
            table,
            whole((1, HD)),
        ]
        + [anywhere] * (n_cp + len(extra)),
        out_specs=[by_row, whole(kv_grads.shape), whole(kv_grads.shape), whole((8, HD))],
        scratch_shapes=[
            pltpu.VMEM((1, n_cp, seq, HD), BF16),
            pltpu.VMEM((1, n_cp, seq, HD), BF16),
            pltpu.VMEM((groups, rows, HD), F32),
            pltpu.VMEM((n_cp, 2, seq, HD), F32),
            pltpu.SemaphoreType.DMA((n_cp, 1, 2)),
        ],
    )
    pairs = groups * rows * rows * (2 * n_cp + 1)
    return pl.pallas_call(
        functools.partial(bwd_kernel, n_cp, head),
        grid_spec=grid_spec,
        out_shape=[
            jax.ShapeDtypeStruct((seq, heads * HD), BF16),
            kv_grads,
            kv_grads,
            jax.ShapeDtypeStruct((8, HD), F32),
        ],
        input_output_aliases={9 + n_cp: 0} if extra else {},
        compiler_params=params(1),
        cost_estimate=cost(10 * pairs * HD, 16 * seq * groups * HD, pairs),
    )(me, q_fin, d_out, out, lse, q_raw, cos_t, sin_t, q_norm, *kv_blocks, *extra)


def post_kernel(n_w, n_tiles, at_ref, o_ref, *rest):
    w_refs = rest[:n_w]
    mine_ref, wmine_ref, x_ref, dy_ref, wpost_ref, y_ref, do_ref, give_ref, keep_ref, dpost_ref = rest[n_w:n_w + 10]
    o_buf, w_buf, attn_scr, o_sem, w_sem = rest[n_w + 10:]
    i = pl.program_id(0)
    n_tp, _, width = o_ref.shape
    rows = x_ref.shape[0]

    def weight_copy(s, par):
        return pltpu.make_async_copy(w_refs[s], w_buf.at[par], w_sem.at[par])

    @pl.when(i == 0)
    def _():
        copies = [
            pltpu.make_async_copy(o_ref.at[t], o_buf.at[:, pl.ds(t * width, width)], o_sem.at[t]) for t in range(n_tp)
        ]
        for copy in copies:
            copy.start()
        weight_copy(0, 0).start()
        for copy in copies:
            copy.wait()

    for s in range(1, n_w):

        @pl.when(i == s - 1)
        def _():
            weight_copy(s, s % 2).start()

    @pl.when(i < n_w)
    def _():
        par = lax.rem(i, 2)
        weight_copy(0, par).wait()
        attn_scr[jnp.bitwise_xor(at_ref[0], i)] = dot(o_buf[...], w_buf[par])

    @pl.when(i == n_tiles)
    def _():
        dpost_ref[...] = jnp.zeros(dpost_ref.shape, F32)
        give_ref[...] = jnp.zeros(give_ref.shape, F32)
        keep_ref[...] = jnp.zeros(keep_ref.shape, F32)

    @pl.when(i >= n_tiles)
    def _():
        span = pl.ds(pl.multiple_of((i - n_tiles) * rows, rows), rows)
        attn = jnp.concatenate([attn_scr[s, span, :] for s in range(n_w)], axis=1)
        inv = lax.rsqrt(jnp.mean(attn * attn, axis=-1, keepdims=True) + EPS)
        unit = attn * inv
        gain = 1.0 + wpost_ref[...]
        y_ref[...] = (x_ref[...].astype(F32) + unit * gain).astype(BF16)
        dy = dy_ref[...].astype(F32)
        dpost_ref[0:1, :] += jnp.sum(dy * unit, axis=0, keepdims=True)
        d_unit = dy * gain
        d_attn = (inv * (d_unit - unit * jnp.mean(d_unit * unit, axis=-1, keepdims=True))).astype(BF16)
        d_out = dot(d_attn, wmine_ref[...], NT)
        for h in range(do_ref.shape[0]):
            do_ref[h] = d_out[:, h * HD:(h + 1) * HD].astype(BF16)
        half = give_ref.shape[0]
        core = at_ref[1]
        give_ref[...] += dot(mine_ref[:, pl.ds(pl.multiple_of((1 - core) * half, HD), half)], d_attn, TN)
        keep_ref[...] += dot(mine_ref[:, pl.ds(pl.multiple_of(core * half, HD), half)], d_attn, TN)


def post(at, out_all, w_all, out, w_mine, x, dy, w_post, rows=256):
    n_tp, seq, width = out_all.shape
    dim = x.shape[1]
    heads = width // HD
    n_w = len(w_all)
    block = lambda i: jnp.maximum(i - n_w, 0)
    row = lambda n: pl.BlockSpec((rows, n), lambda i, *_: (block(i), 0))
    half = jax.ShapeDtypeStruct((width // 2, dim), F32)
    grid_spec = pltpu.PrefetchScalarGridSpec(
        num_scalar_prefetch=1,
        grid=(n_w + seq // rows,),
        in_specs=[pl.BlockSpec(memory_space=pl.ANY)] * (1 + n_w)
        + [row(width), fixed(w_mine.shape), row(dim), row(dim), whole((1, dim))],
        out_specs=[
            row(dim),
            pl.BlockSpec((heads, rows, HD), lambda i, *_: (0, block(i), 0)),
            fixed(half.shape),
            fixed(half.shape),
            whole((8, dim)),
        ],
        scratch_shapes=[
            pltpu.VMEM((seq, n_tp * width), BF16),
            pltpu.VMEM((2, n_tp * width, dim // n_w), BF16),
            pltpu.VMEM((n_w, seq, dim // n_w), F32),
            pltpu.SemaphoreType.DMA((n_tp,)),
            pltpu.SemaphoreType.DMA((2,)),
        ],
    )
    return pl.pallas_call(
        functools.partial(post_kernel, n_w, n_w),
        name="post",
        grid_spec=grid_spec,
        out_shape=[
            jax.ShapeDtypeStruct((seq, dim), BF16),
            jax.ShapeDtypeStruct((heads, seq, HD), BF16),
            half,
            half,
            jax.ShapeDtypeStruct((8, dim), F32),
        ],
        compiler_params=params(1, VMEM_TOP),
        cost_estimate=cost(2 * seq * dim * width * (n_tp + 2), 8 * seq * dim + 2 * dim * width * (n_tp + 1)),
    )(at, out_all, *w_all, out, w_mine, x, dy, w_post)


def kback_kernel(kv_heads, *refs):
    parts = refs[:3 * kv_heads]
    kraw_ref, cos_ref, sin_ref, kn_ref, out_ref, gain_ref = refs[3 * kv_heads:]

    @pl.when(pl.program_id(0) == 0)
    def _():
        gain_ref[...] = jnp.zeros(gain_ref.shape, F32)

    for h in range(kv_heads):
        own_ref, near_ref, far_ref = parts[3 * h:3 * h + 3]
        cols = slice(h * HD, (h + 1) * HD)
        d_k = own_ref[0, 0] + near_ref[0, 0] + far_ref[0]
        d_raw, d_gain = norm_rope_back(d_k, kraw_ref[:, cols], kn_ref[...], cos_ref[...], sin_ref[...])
        out_ref[:, cols] = d_raw
        gain_ref[0:1, :] += d_gain
        d_v = own_ref[0, 1] + near_ref[0, 1] + far_ref[1]
        out_ref[:, (kv_heads + h) * HD:(kv_heads + h + 1) * HD] = d_v.astype(BF16)


def key_back(parts, k_raw, cos_t, sin_t, k_norm, rows=256):
    kv_heads = len(parts) // 3
    seq = k_raw.shape[0]
    two = pl.BlockSpec((1, 2, rows, HD), lambda i: (0, 0, i, 0))
    one = pl.BlockSpec((2, rows, HD), lambda i: (0, i, 0))
    row = lambda n: pl.BlockSpec((rows, n), lambda i: (i, 0))
    return pl.pallas_call(
        functools.partial(kback_kernel, kv_heads),
        name="kback",
        grid=(seq // rows,),
        in_specs=[two, two, one] * kv_heads + [row(kv_heads * HD), row(HD), row(HD), whole((1, HD))],
        out_specs=[row(2 * kv_heads * HD), whole((8, HD))],
        out_shape=[
            jax.ShapeDtypeStruct((seq, 2 * kv_heads * HD), BF16),
            jax.ShapeDtypeStruct((8, HD), F32),
        ],
        compiler_params=params(1),
        cost_estimate=cost(50 * seq * kv_heads * HD, 12 * seq * kv_heads * HD),
    )(*parts, k_raw, cos_t, sin_t, k_norm)


def dx_kernel(n_tp, tp_ref, *refs):
    q_refs, kv_refs = refs[:n_tp], refs[n_tp:2 * n_tp]
    w_ref, x_ref, dy_ref, wpre_ref, dx_ref, dpre_ref, acc = refs[2 * n_tp:]
    i = pl.program_id(0)
    split = q_refs[0].shape[1]
    total = None
    for s in range(n_tp):
        t = lax.rem(tp_ref[0] + n_tp - s, n_tp)
        part = dot(q_refs[s][...], w_ref[t, :, :split], NT) + dot(kv_refs[s][...], w_ref[t, :, split:], NT)
        total = part if total is None else total + part
    acc[i] = total

    @pl.when(i == pl.num_programs(0) - 1)
    def _():
        d_normed = jnp.concatenate([acc[t] for t in range(acc.shape[0])], axis=1)
        x = x_ref[...].astype(F32)
        inv = lax.rsqrt(jnp.mean(x * x, axis=-1, keepdims=True) + EPS)
        unit = x * inv
        dpre_ref[...] = jnp.broadcast_to(jnp.sum(d_normed * unit, axis=0, keepdims=True), dpre_ref.shape)
        d_unit = d_normed * (1.0 + wpre_ref[...])
        d_x = inv * (d_unit - unit * jnp.mean(d_unit * unit, axis=-1, keepdims=True))
        dx_ref[...] = (dy_ref[...].astype(F32) + d_x).astype(BF16)


def input_grad(tp, q_grads, kv_grads, w_all, x, dy, w_pre, cols=512):
    n_tp = len(q_grads)
    rows, q_width = q_grads[0].shape
    kv_width = kv_grads[0].shape[1]
    dim = x.shape[1]
    here = pl.BlockSpec((rows, dim), lambda i, t: (t[0], 0))
    grid_spec = pltpu.PrefetchScalarGridSpec(
        num_scalar_prefetch=1,
        grid=(dim // cols,),
        in_specs=[whole((rows, q_width))] * n_tp
        + [whole((rows, kv_width))] * n_tp
        + [pl.BlockSpec((n_tp, cols, q_width + kv_width), lambda i, *_: (0, i, 0)), here, here, whole((1, dim))],
        out_specs=[whole((rows, dim)), whole((8, dim))],
        scratch_shapes=[pltpu.VMEM((dim // cols, rows, cols), F32)],
    )
    return pl.pallas_call(
        functools.partial(dx_kernel, n_tp),
        name="dx",
        grid_spec=grid_spec,
        out_shape=[jax.ShapeDtypeStruct((rows, dim), BF16), jax.ShapeDtypeStruct((8, dim), F32)],
        compiler_params=params(1),
        cost_estimate=cost(2 * n_tp * rows * (q_width + kv_width) * dim, 2 * n_tp * (q_width + kv_width) * dim),
    )(tp, *q_grads, *kv_grads, w_all, x, dy, w_pre)


def dw_kernel(n_cp, me_ref, *refs):
    n_refs, q_refs, kv_refs = refs[:n_cp], refs[n_cp:2 * n_cp], refs[2 * n_cp:3 * n_cp]
    dwq_ref, dwk_ref, dwv_ref, n_buf, g_buf, n_sem, g_sem = refs[3 * n_cp:]
    i = pl.program_id(0)
    cols = n_buf.shape[3]
    seq, q_width = q_refs[0].shape
    kv_width = kv_refs[0].shape[1]
    me = me_ref[0]

    def fetch(step, par):
        span = pl.ds(pl.multiple_of(step * cols, cols), cols)
        return [
            pltpu.make_async_copy(n_refs[s].at[:, span], n_buf.at[par, jnp.bitwise_xor(me, s)], n_sem.at[par, s])
            for s in range(n_cp)
        ]

    @pl.when(i == 0)
    def _():
        copies = fetch(0, 0)
        for s in range(n_cp):
            owner = jnp.bitwise_xor(me, s)
            copies.append(pltpu.make_async_copy(q_refs[s], g_buf.at[owner, :, pl.ds(0, q_width)], g_sem.at[s, 0]))
            copies.append(pltpu.make_async_copy(kv_refs[s], g_buf.at[owner, :, pl.ds(q_width, kv_width)], g_sem.at[s, 1]))
        for copy in copies:
            copy.start()
        for copy in copies[n_cp:]:
            copy.wait()

    @pl.when(i + 1 < pl.num_programs(0))
    def _():
        for copy in fetch(i + 1, (i + 1) % 2):
            copy.start()

    for copy in fetch(i, i % 2):
        copy.wait()
    lhs = n_buf[i % 2].reshape(n_cp * seq, cols)
    grad = dot(lhs, g_buf[...].reshape(n_cp * seq, q_width + kv_width), TN)
    dwq_ref[...] = grad[:, :q_width]
    dwk_ref[...] = grad[:, q_width:q_width + kv_width // 2]
    dwv_ref[...] = grad[:, q_width + kv_width // 2:]


def weight_grads(me, normed, q_grads, kv_grads, cols=256):
    n_cp = len(normed)
    seq, dim = normed[0].shape
    q_width, kv_width = q_grads[0].shape[1], kv_grads[0].shape[1]
    anywhere = pl.BlockSpec(memory_space=pl.ANY)
    tile = lambda n: pl.BlockSpec((cols, n), lambda i, *_: (i, 0))
    grid_spec = pltpu.PrefetchScalarGridSpec(
        num_scalar_prefetch=1,
        grid=(dim // cols,),
        in_specs=[anywhere] * (3 * n_cp),
        out_specs=[tile(q_width), tile(kv_width // 2), tile(kv_width // 2)],
        scratch_shapes=[
            pltpu.VMEM((2, n_cp, seq, cols), BF16),
            pltpu.VMEM((n_cp, seq, q_width + kv_width), BF16),
            pltpu.SemaphoreType.DMA((2, n_cp)),
            pltpu.SemaphoreType.DMA((n_cp, 2)),
        ],
    )
    return pl.pallas_call(
        functools.partial(dw_kernel, n_cp),
        name="dw",
        grid_spec=grid_spec,
        out_shape=[
            jax.ShapeDtypeStruct((dim, q_width), F32),
            jax.ShapeDtypeStruct((dim, kv_width // 2), F32),
            jax.ShapeDtypeStruct((dim, kv_width // 2), F32),
        ],
        compiler_params=params(1),
        cost_estimate=cost(2 * n_cp * seq * dim * (q_width + kv_width), 2 * n_cp * seq * (dim + q_width + kv_width)),
    )(me, *normed, *q_grads, *kv_grads)


def join_kernel(n, core_ref, *refs):
    out_ref = refs[-1]
    i = pl.program_id(0)
    for j in range(n):
        for t, ref in enumerate((refs[j], refs[n + j])):

            @pl.when((lax.rem(i, n) == j) & (jnp.bitwise_xor(i // n, core_ref[0]) == t))
            def _():
                out_ref[...] = ref[...]


def join_halves(core, keep, other):
    n = len(keep)
    rows, width = keep[0].shape
    grid_spec = pltpu.PrefetchScalarGridSpec(
        num_scalar_prefetch=1,
        grid=(2 * n,),
        in_specs=[fixed((rows, width))] * (2 * n),
        out_specs=pl.BlockSpec((rows, width), lambda i, c: (i, 0)),
    )
    return pl.pallas_call(
        functools.partial(join_kernel, n),
        name="join",
        grid_spec=grid_spec,
        out_shape=jax.ShapeDtypeStruct((2 * n * rows, width), F32),
        compiler_params=params(1),
        cost_estimate=cost(n * rows * width, 16 * n * rows * width),
    )(core, *keep, *other)


def solution(mesh):
    n_cp, n_tp, n_dp = mesh.shape["cp"], mesh.shape["tp"], mesh.shape["dp"]
    near = [(i, i ^ 1) for i in range(n_cp)]
    across = [(i, i ^ 2) for i in range(n_cp)]
    beside = [(i, i ^ 1) for i in range(n_dp)]

    def from_cp(value):
        far = lax.ppermute(value, "cp", across)
        return [value, lax.ppermute(value, "cp", near), far, lax.ppermute(far, "cp", near)]

    def per_device(hidden, cotangent, pos_loc, w_q, w_k, w_v, w_o, w_pre, w_post, q_norm, k_norm):
        _, seq, dim = hidden.shape
        x, dy = hidden[0], cotangent[0]
        kv_heads = w_k.shape[1] // HD
        cp, tp, dp = (lax.axis_index(a).astype(jnp.int32) for a in ("cp", "tp", "dp"))
        core = cp % 2
        me, one_tp, one_core = cp.reshape(1), tp.reshape(1), core.reshape(1)

        share = dp * n_cp + cp
        shares = n_dp * n_cp
        cols = dim // shares
        mine = lax.all_gather(lax.dynamic_slice_in_dim(w_o, share * cols, cols, 1), "tp", axis=0, tiled=True)
        w_o_all = from_cp(mine)
        if n_dp == 2:
            own, far = lax.ppermute(mine, "dp", beside), lax.ppermute(w_o_all[2], "dp", beside)
            w_o_all += [own, lax.ppermute(own, "cp", near), far, lax.ppermute(far, "cp", near)]

        cos_t, sin_t = rope_tables(pos_loc)
        qn, kn = q_norm.reshape(1, HD), k_norm.reshape(1, HD)
        wpre, wpost = w_pre.reshape(1, dim), w_post.reshape(1, dim)
        normed, kv_own, k_raw = project_kv(x, wpre, w_k, w_v, kn, cos_t, sin_t)
        kv_blocks = from_cp(kv_own)
        q_fin, q_raw = project_q(normed, w_q, qn, cos_t, sin_t)
        normed_all = from_cp(normed)
        out, lse = attention_fwd(me, q_fin, kv_blocks, kv_heads)

        out_sent, _ = lax.optimization_barrier((out, mine))
        out_all = lax.all_gather(out_sent, "tp", axis=0, tiled=False)
        at = jnp.stack([share, core])
        y, d_out, give, keep, d_post = post(at, out_all, w_o_all, out, w_o, x, dy, wpost)

        w_rows = dim // shares
        parts = [lax.dynamic_slice_in_dim(w, share * w_rows, w_rows, 0) for w in (w_q, w_k, w_v)]
        fence, _ = lax.optimization_barrier((jnp.concatenate(parts, axis=1), out_all))
        w_all = lax.all_gather(fence, ("tp", "dp", "cp"), axis=0, tiled=True).reshape(n_tp, dim, fence.shape[1])

        got = lax.ppermute(give, "cp", near)
        keep = keep + got
        part = keep.shape[0] // 2
        kept, other = [], []
        for j in range(2):
            mine_part = keep[j * part:(j + 1) * part]
            mine_part = mine_part + lax.ppermute(mine_part, "cp", across)
            kept.append(mine_part)
            other.append(lax.ppermute(mine_part, "cp", near))
        d_wo = join_halves(one_core, kept, other)

        dq, dq_gain, dkv_parts = None, [], []
        for h in range(kv_heads):
            dq, dkv, dkv_send, gain = attention_bwd(
                h, me, q_fin, d_out, out, lse, q_raw, cos_t, sin_t, qn, kv_blocks, kv_heads, dq
            )
            dq_gain.append(gain[0])
            got = lax.ppermute(dkv_send, "cp", near)
            dkv_parts += [dkv, got, lax.ppermute(dkv[1] + got[1], "cp", across)]
        d_kv, dk_gain = key_back(dkv_parts, k_raw, cos_t, sin_t, kn)

        rows = seq // n_tp

        def exchange_rows(value):
            pieces = [lax.dynamic_slice_in_dim(value, tp * rows, rows, 0)]
            for s in range(1, n_tp):
                part = lax.dynamic_slice_in_dim(value, ((tp + s) % n_tp) * rows, rows, 0)
                pieces.append(lax.ppermute(part, "tp", [(i, (i + s) % n_tp) for i in range(n_tp)]))
            return pieces

        dq_rows = exchange_rows(dq)
        dq_all = from_cp(dq)
        dkv_rows = exchange_rows(d_kv)
        dx_rows, d_pre = input_grad(one_tp, dq_rows, dkv_rows, w_all, x, dy, wpre)
        d_hidden = lax.all_gather(dx_rows, "tp", axis=0, tiled=True)

        dkv_all = from_cp(d_kv)
        d_wq, d_wk, d_wv = weight_grads(me, normed_all, dq_all, dkv_all)

        small = jnp.concatenate([jnp.where(tp == 0, d_post[0], 0.0), d_pre[0], sum(dq_gain), dk_gain[0]])
        small = small + lax.ppermute(small, "cp", near)
        small = small + lax.ppermute(small, "cp", across)
        small = small + lax.ppermute(small, "tp", [(i, i ^ 1) for i in range(n_tp)])
        small = small + lax.ppermute(small, "tp", [(i, i ^ 2) for i in range(n_tp)])
        d_post, d_pre = small[:dim], small[dim:2 * dim]
        d_qn, d_kn = small[2 * dim:2 * dim + HD], small[2 * dim + HD:]
        return y[None], d_hidden[None], d_wq, d_wk, d_wv, d_wo, d_pre, d_post, d_qn, d_kn

    specs_in = (P('dp', 'cp', None), P('dp', 'cp', None), P(('dp', 'cp')), P(None, 'tp'), P(None, 'tp'), P(None, 'tp'), P('tp', None), P(None), P(None), P(None), P(None))
    specs_out = (P('dp', 'cp', None), P('dp', 'cp', None), P('dp', 'tp'), P('dp', 'tp'), P('dp', 'tp'), P(('dp', 'tp'), None), P('dp'), P('dp'), P('dp'), P('dp'))
    return jax.shard_map(per_device, mesh=mesh, in_specs=specs_in, out_specs=specs_out, check_vma=False)
```

```python
import functools

import jax
import jax.numpy as jnp
from jax import lax
from jax.experimental import pallas as pl
from jax.experimental.pallas import tpu as pltpu
from jax.sharding import PartitionSpec as P


EPS = 1e-6
ROPE_BASE = 1000000.0
ROPE_SCALE = 8.0
NEG_BIG = -1e30
LOG2E = 1.4426950408889634
HD = 128
F32 = jnp.float32
BF16 = jnp.bfloat16
VMEM_MAX = 60 * 1024 * 1024
VMEM_TOP = 67043328
NT = (((1,), (1,)), ((), ()))
TN = (((0,), (0,)), ((), ()))


def dot(a, b, dims=(((1,), (0,)), ((), ()))):
    return lax.dot_general(a, b, dims, preferred_element_type=F32)


def params(dims, vmem=VMEM_MAX):
    return pltpu.CompilerParams(dimension_semantics=("arbitrary",) * dims, vmem_limit_bytes=vmem)


def cost(flops, nbytes, trans=0):
    return pl.CostEstimate(flops=int(flops), bytes_accessed=int(nbytes), transcendentals=int(trans))


def whole(shape):
    return pl.BlockSpec(shape, lambda *_: (0,) * len(shape))


def fixed(shape):
    return pl.BlockSpec(shape, lambda *_: (0,) * len(shape), pipeline_mode=pl.Buffered(buffer_count=1))


def rope_tables(pos_loc):
    half_dim = HD // 2
    inv_freq = 1.0 / (ROPE_SCALE * ROPE_BASE ** (jnp.arange(half_dim, dtype=F32) * (2.0 / HD)))
    angles = pos_loc.astype(F32)[:, None] * inv_freq[None, :]
    cos_t, sin_t = jnp.cos(angles), jnp.sin(angles)
    return jnp.concatenate([cos_t, cos_t], axis=-1), jnp.concatenate([-sin_t, sin_t], axis=-1)


def norm_rope(raw, gain, cos_t, sin_t):
    raw = raw.astype(F32)
    unit = raw * lax.rsqrt(jnp.mean(raw * raw, axis=-1, keepdims=True) + EPS)
    scaled = unit * (1.0 + gain)
    return (scaled * cos_t + pltpu.roll(scaled, HD // 2, 1) * sin_t).astype(BF16)


def norm_rope_back(d_final, raw, gain, cos_t, sin_t):
    raw = raw.astype(F32)
    inv = lax.rsqrt(jnp.mean(raw * raw, axis=-1, keepdims=True) + EPS)
    unit = raw * inv
    d_scaled = d_final * cos_t - pltpu.roll(d_final, HD // 2, 1) * sin_t
    d_gain = jnp.sum(d_scaled * unit, axis=0, keepdims=True)
    d_unit = d_scaled * (1.0 + gain)
    d_raw = inv * (d_unit - unit * jnp.mean(d_unit * unit, axis=-1, keepdims=True))
    return d_raw.astype(BF16), d_gain


def kv_kernel(x_ref, wpre_ref, wk_ref, wv_ref, kn_ref, cos_ref, sin_ref, normed_ref, kv_ref, kraw_ref):
    x = x_ref[...].astype(F32)
    inv = lax.rsqrt(jnp.mean(x * x, axis=-1, keepdims=True) + EPS)
    normed = (x * inv * (1.0 + wpre_ref[...])).astype(BF16)
    normed_ref[...] = normed
    k_raw = dot(normed, wk_ref[...]).astype(BF16)
    kraw_ref[...] = k_raw
    width = k_raw.shape[1]
    for h in range(width // HD):
        cols = slice(h * HD, (h + 1) * HD)
        kv_ref[:, cols] = norm_rope(k_raw[:, cols], kn_ref[...], cos_ref[...], sin_ref[...])
    kv_ref[:, width:] = dot(normed, wv_ref[...]).astype(BF16)


def project_kv(x, w_pre, w_k, w_v, k_norm, cos_t, sin_t, rows=256):
    seq, dim = x.shape
    width = w_k.shape[1]
    row = lambda n: pl.BlockSpec((rows, n), lambda i: (i, 0))
    return pl.pallas_call(
        kv_kernel,
        name="pkv",
        grid=(seq // rows,),
        in_specs=[row(dim), whole((1, dim)), fixed(w_k.shape), fixed(w_v.shape), whole((1, HD)), row(HD), row(HD)],
        out_specs=[row(dim), row(2 * width), row(width)],
        out_shape=[
            jax.ShapeDtypeStruct((seq, dim), BF16),
            jax.ShapeDtypeStruct((seq, 2 * width), BF16),
            jax.ShapeDtypeStruct((seq, width), BF16),
        ],
        compiler_params=params(1),
        cost_estimate=cost(4 * seq * dim * width, 4 * seq * dim + 4 * dim * width),
    )(x, w_pre, w_k, w_v, k_norm, cos_t, sin_t)


def q_kernel(normed_ref, wq_ref, qn_ref, cos_ref, sin_ref, qfin_ref, qraw_ref):
    q_raw = dot(normed_ref[...], wq_ref[...]).astype(BF16)
    for h in range(qfin_ref.shape[0]):
        part = q_raw[:, h * HD:(h + 1) * HD]
        qraw_ref[h] = part
        qfin_ref[h] = norm_rope(part, qn_ref[...], cos_ref[...], sin_ref[...])


def project_q(normed, w_q, q_norm, cos_t, sin_t, rows=256):
    seq, dim = normed.shape
    heads = w_q.shape[1] // HD
    row = lambda n: pl.BlockSpec((rows, n), lambda i: (i, 0))
    head_rows = pl.BlockSpec((heads, rows, HD), lambda i: (0, i, 0))
    shape = jax.ShapeDtypeStruct((heads, seq, HD), BF16)
    return pl.pallas_call(
        q_kernel,
        name="pq",
        grid=(seq // rows,),
        in_specs=[row(dim), fixed(w_q.shape), whole((1, HD)), row(HD), row(HD)],
        out_specs=[head_rows, head_rows],
        out_shape=[shape, shape],
        compiler_params=params(1),
        cost_estimate=cost(2 * seq * dim * heads * HD, 2 * seq * dim + 2 * dim * heads * HD),
    )(normed, w_q, q_norm, cos_t, sin_t)


def load_kv(kv_refs, k_buf, v_buf, sems, heads):
    kv_heads = kv_refs[0].shape[1] // (2 * HD)
    copies = []
    for s, ref in enumerate(kv_refs):
        for i, h in enumerate(heads):
            for t, buf in enumerate((k_buf, v_buf)):
                src = ref.at[:, pl.ds((t * kv_heads + h) * HD, HD)]
                copies.append(pltpu.make_async_copy(src, buf.at[i, s], sems.at[s, i, t]))
    for copy in copies:
        copy.start()
    for copy in copies:
        copy.wait()


def piece_place(piece, me, n_cp):
    upper = piece >= n_cp
    owner = jnp.where(upper, 2 * n_cp - 1 - piece, piece)
    return jnp.bitwise_xor(owner, me), upper.astype(jnp.int32)


def fwd_kernel(n_cp, me_ref, q_ref, *rest):
    kv_refs = rest[:n_cp]
    o_ref, lse_ref, k_buf, v_buf, m_scr, acc_scr, sems = rest[n_cp:]
    h, half = pl.program_id(0), pl.program_id(1)
    groups, rows, _ = q_ref.shape

    @pl.when((h == 0) & (half == 0))
    def _():
        load_kv(kv_refs, k_buf, v_buf, sems, range(k_buf.shape[0]))

    me = me_ref[0]
    piece = jnp.where(half == 0, me, 2 * n_cp - 1 - me)
    scale = HD ** -0.5 * LOG2E
    m_scr[...] = jnp.full(m_scr.shape, NEG_BIG, F32)
    acc_scr[...] = jnp.zeros(acc_scr.shape, F32)

    def block(j, masked):
        slot, upper = piece_place(j, me, n_cp)
        span = pl.ds(pl.multiple_of(upper * rows, rows), rows)
        k = k_buf[h, slot, span, :]
        v_ext = jnp.concatenate([v_buf[h, slot, span, :], jnp.ones((rows, HD), BF16)], axis=1)
        scores = [dot(q_ref[g], k, NT) * scale for g in range(groups)]
        for g in range(groups):
            s = scores[g]
            if masked:
                q_pos = lax.broadcasted_iota(jnp.int32, s.shape, 0)
                k_pos = lax.broadcasted_iota(jnp.int32, s.shape, 1)
                s = jnp.where(k_pos <= q_pos, s, NEG_BIG)
            m_old = m_scr[g]
            m_new = jnp.maximum(m_old, jnp.max(s, axis=1, keepdims=True))
            alpha = jnp.exp2(m_old - m_new)
            p = jnp.exp2(s - jnp.concatenate([m_new] * (rows // HD), axis=1)).astype(BF16)
            acc_scr[g] = acc_scr[g] * jnp.concatenate([alpha, alpha], axis=1) + dot(p, v_ext)
            m_scr[g] = m_new

    def full(j, carry):
        block(j, False)
        return carry

    lax.fori_loop(0, piece, full, 0)
    block(piece, True)
    for g in range(groups):
        l = acc_scr[g, :, HD:]
        o_ref[:, g * HD:(g + 1) * HD] = (acc_scr[g, :, :HD] / l).astype(BF16)
        lse_ref[0, g:g + 1, :] = jnp.transpose(m_scr[g] + jnp.log2(l))[0:1, :]


def attention_fwd(me, q_fin, kv_blocks, kv_heads):
    heads, seq, _ = q_fin.shape
    n_cp = len(kv_blocks)
    groups = heads // kv_heads
    rows = seq // 2
    grid_spec = pltpu.PrefetchScalarGridSpec(
        num_scalar_prefetch=1,
        grid=(kv_heads, 2),
        in_specs=[pl.BlockSpec((groups, rows, HD), lambda h, i, *_: (h, i, 0))] + [pl.BlockSpec(memory_space=pl.ANY)] * n_cp,
        out_specs=[
            pl.BlockSpec((rows, groups * HD), lambda h, i, *_: (i, h)),
            pl.BlockSpec((1, 8, rows), lambda h, i, *_: (h, 0, i)),
        ],
        scratch_shapes=[
            pltpu.VMEM((kv_heads, n_cp, seq, HD), BF16),
            pltpu.VMEM((kv_heads, n_cp, seq, HD), BF16),
            pltpu.VMEM((groups, rows, HD), F32),
            pltpu.VMEM((groups, rows, 2 * HD), F32),
            pltpu.SemaphoreType.DMA((n_cp, kv_heads, 2)),
        ],
    )
    pairs = heads * rows * rows * (2 * n_cp + 1)
    return pl.pallas_call(
        functools.partial(fwd_kernel, n_cp),
        name="fwd",
        grid_spec=grid_spec,
        out_shape=[
            jax.ShapeDtypeStruct((seq, heads * HD), BF16),
            jax.ShapeDtypeStruct((kv_heads, 8, seq), F32),
        ],
        compiler_params=params(2),
        cost_estimate=cost(4 * pairs * HD, 8 * seq * heads * HD, pairs),
    )(me, q_fin, *kv_blocks)


def bwd_kernel(n_cp, head, me_ref, q_ref, do_ref, o_ref, lse_ref, qraw_ref, cos_ref, sin_ref, qn_ref, *rest):
    kv_refs = rest[:n_cp]
    dq_ref, keep_ref, send_ref, gain_ref, k_buf, v_buf, dq_scr, dkv_scr, sems = rest[-9:]
    half = pl.program_id(0)
    groups, rows, _ = q_ref.shape

    @pl.when(half == 0)
    def _():
        load_kv(kv_refs, k_buf, v_buf, sems, (head,))
        gain_ref[...] = jnp.zeros(gain_ref.shape, F32)
        dkv_scr[...] = jnp.zeros(dkv_scr.shape, F32)

    me = me_ref[0]
    piece = jnp.where(half == 0, me, 2 * n_cp - 1 - me)
    scale = HD ** -0.5
    delta = []
    for g in range(groups):
        prod = do_ref[g].astype(F32) * o_ref[:, g * HD:(g + 1) * HD].astype(F32)
        column = jnp.broadcast_to(jnp.sum(prod, axis=1, keepdims=True), (rows, HD))
        delta.append(jnp.transpose(column)[0:1, :])
    dq_scr[...] = jnp.zeros(dq_scr.shape, F32)

    def block(j, masked):
        slot, upper = piece_place(j, me, n_cp)
        span = pl.ds(pl.multiple_of(upper * rows, rows), rows)
        k = k_buf[0, slot, span, :]
        v = v_buf[0, slot, span, :]
        probs, d_scores = [], []
        for g in range(groups):
            s = dot(k, q_ref[g], NT)
            p = jnp.exp2(s * (scale * LOG2E) - lse_ref[0, g:g + 1, :])
            if masked:
                k_pos = lax.broadcasted_iota(jnp.int32, s.shape, 0)
                q_pos = lax.broadcasted_iota(jnp.int32, s.shape, 1)
                p = jnp.where(k_pos <= q_pos, p, 0.0)
            probs.append(p.astype(BF16))
            d_scores.append((p * (dot(v, do_ref[g], NT) - delta[g])).astype(BF16))
        for g in range(groups):
            dq_scr[g] += dot(d_scores[g], k, TN)
        index = (slot % 2) * (n_cp // 2) + slot // 2
        d_all = jnp.concatenate(d_scores, axis=1)
        p_all = jnp.concatenate(probs, axis=1)
        dkv_scr[index, 0, span, :] += dot(d_all, q_ref[...].reshape(groups * rows, HD)) * scale
        dkv_scr[index, 1, span, :] += dot(p_all, do_ref[...].reshape(groups * rows, HD))

    def full(j, carry):
        block(j, False)
        return carry

    lax.fori_loop(0, piece, full, 0)
    block(piece, True)
    for g in range(groups):
        d_raw, d_gain = norm_rope_back(dq_scr[g] * scale, qraw_ref[g], qn_ref[...], cos_ref[...], sin_ref[...])
        dq_ref[:, g * HD:(g + 1) * HD] = d_raw
        gain_ref[0:1, :] += d_gain

    @pl.when(half == 1)
    def _():
        for i in range(n_cp // 2):
            keep_ref[i] = dkv_scr[i]
            send_ref[i] = dkv_scr[n_cp // 2 + i]


def attention_bwd(head, me, q_fin, d_out, out, lse, q_raw, cos_t, sin_t, q_norm, kv_blocks, kv_heads, dq=None):
    heads, seq, _ = q_fin.shape
    n_cp = len(kv_blocks)
    groups = heads // kv_heads
    rows = seq // 2
    by_head = pl.BlockSpec((groups, rows, HD), lambda i, *_: (head, i, 0))
    by_row = pl.BlockSpec((rows, groups * HD), lambda i, *_: (i, head))
    table = pl.BlockSpec((rows, HD), lambda i, *_: (i, 0))
    anywhere = pl.BlockSpec(memory_space=pl.ANY)
    kv_grads = jax.ShapeDtypeStruct((n_cp // 2, 2, seq, HD), F32)
    extra = () if dq is None else (dq,)
    grid_spec = pltpu.PrefetchScalarGridSpec(
        num_scalar_prefetch=1,
        grid=(2,),
        in_specs=[
            by_head,
            by_head,
            by_row,
            pl.BlockSpec((1, 8, rows), lambda i, *_: (head, 0, i)),
            by_head,
            table,
            table,
            whole((1, HD)),
        ]
        + [anywhere] * (n_cp + len(extra)),
        out_specs=[by_row, whole(kv_grads.shape), whole(kv_grads.shape), whole((8, HD))],
        scratch_shapes=[
            pltpu.VMEM((1, n_cp, seq, HD), BF16),
            pltpu.VMEM((1, n_cp, seq, HD), BF16),
            pltpu.VMEM((groups, rows, HD), F32),
            pltpu.VMEM((n_cp, 2, seq, HD), F32),
            pltpu.SemaphoreType.DMA((n_cp, 1, 2)),
        ],
    )
    pairs = groups * rows * rows * (2 * n_cp + 1)
    return pl.pallas_call(
        functools.partial(bwd_kernel, n_cp, head),
        grid_spec=grid_spec,
        out_shape=[
            jax.ShapeDtypeStruct((seq, heads * HD), BF16),
            kv_grads,
            kv_grads,
            jax.ShapeDtypeStruct((8, HD), F32),
        ],
        input_output_aliases={9 + n_cp: 0} if extra else {},
        compiler_params=params(1),
        cost_estimate=cost(10 * pairs * HD, 16 * seq * groups * HD, pairs),
    )(me, q_fin, d_out, out, lse, q_raw, cos_t, sin_t, q_norm, *kv_blocks, *extra)


def post_kernel(n_w, n_tiles, at_ref, o_ref, *rest):
    w_refs = rest[:n_w]
    mine_ref, wmine_ref, x_ref, dy_ref, wpost_ref, y_ref, do_ref, give_ref, keep_ref, dpost_ref = rest[n_w:n_w + 10]
    o_buf, w_buf, attn_scr, o_sem, w_sem = rest[n_w + 10:]
    i = pl.program_id(0)
    n_tp, _, width = o_ref.shape
    rows = x_ref.shape[0]

    def weight_copy(s, par):
        return pltpu.make_async_copy(w_refs[s], w_buf.at[par], w_sem.at[par])

    @pl.when(i == 0)
    def _():
        copies = [
            pltpu.make_async_copy(o_ref.at[t], o_buf.at[:, pl.ds(t * width, width)], o_sem.at[t]) for t in range(n_tp)
        ]
        for copy in copies:
            copy.start()
        weight_copy(0, 0).start()
        for copy in copies:
            copy.wait()

    for s in range(1, n_w):

        @pl.when(i == s - 1)
        def _():
            weight_copy(s, s % 2).start()

    @pl.when(i < n_w)
    def _():
        par = lax.rem(i, 2)
        weight_copy(0, par).wait()
        attn_scr[jnp.bitwise_xor(at_ref[0], i)] = dot(o_buf[...], w_buf[par])

    @pl.when(i == n_tiles)
    def _():
        dpost_ref[...] = jnp.zeros(dpost_ref.shape, F32)
        give_ref[...] = jnp.zeros(give_ref.shape, F32)
        keep_ref[...] = jnp.zeros(keep_ref.shape, F32)

    @pl.when(i >= n_tiles)
    def _():
        span = pl.ds(pl.multiple_of((i - n_tiles) * rows, rows), rows)
        attn = jnp.concatenate([attn_scr[s, span, :] for s in range(n_w)], axis=1)
        inv = lax.rsqrt(jnp.mean(attn * attn, axis=-1, keepdims=True) + EPS)
        unit = attn * inv
        gain = 1.0 + wpost_ref[...]
        y_ref[...] = (x_ref[...].astype(F32) + unit * gain).astype(BF16)
        dy = dy_ref[...].astype(F32)
        dpost_ref[0:1, :] += jnp.sum(dy * unit, axis=0, keepdims=True)
        d_unit = dy * gain
        d_attn = (inv * (d_unit - unit * jnp.mean(d_unit * unit, axis=-1, keepdims=True))).astype(BF16)
        d_out = dot(d_attn, wmine_ref[...], NT)
        for h in range(do_ref.shape[0]):
            do_ref[h] = d_out[:, h * HD:(h + 1) * HD].astype(BF16)
        half = give_ref.shape[0]
        core = at_ref[1]
        give_ref[...] += dot(mine_ref[:, pl.ds(pl.multiple_of((1 - core) * half, HD), half)], d_attn, TN)
        keep_ref[...] += dot(mine_ref[:, pl.ds(pl.multiple_of(core * half, HD), half)], d_attn, TN)


def post(at, out_all, w_all, out, w_mine, x, dy, w_post, rows=256):
    n_tp, seq, width = out_all.shape
    dim = x.shape[1]
    heads = width // HD
    n_w = len(w_all)
    block = lambda i: jnp.maximum(i - n_w, 0)
    row = lambda n: pl.BlockSpec((rows, n), lambda i, *_: (block(i), 0))
    half = jax.ShapeDtypeStruct((width // 2, dim), F32)
    grid_spec = pltpu.PrefetchScalarGridSpec(
        num_scalar_prefetch=1,
        grid=(n_w + seq // rows,),
        in_specs=[pl.BlockSpec(memory_space=pl.ANY)] * (1 + n_w)
        + [row(width), fixed(w_mine.shape), row(dim), row(dim), whole((1, dim))],
        out_specs=[
            row(dim),
            pl.BlockSpec((heads, rows, HD), lambda i, *_: (0, block(i), 0)),
            fixed(half.shape),
            fixed(half.shape),
            whole((8, dim)),
        ],
        scratch_shapes=[
            pltpu.VMEM((seq, n_tp * width), BF16),
            pltpu.VMEM((2, n_tp * width, dim // n_w), BF16),
            pltpu.VMEM((n_w, seq, dim // n_w), F32),
            pltpu.SemaphoreType.DMA((n_tp,)),
            pltpu.SemaphoreType.DMA((2,)),
        ],
    )
    return pl.pallas_call(
        functools.partial(post_kernel, n_w, n_w),
        name="post",
        grid_spec=grid_spec,
        out_shape=[
            jax.ShapeDtypeStruct((seq, dim), BF16),
            jax.ShapeDtypeStruct((heads, seq, HD), BF16),
            half,
            half,
            jax.ShapeDtypeStruct((8, dim), F32),
        ],
        compiler_params=params(1, VMEM_TOP),
        cost_estimate=cost(2 * seq * dim * width * (n_tp + 2), 8 * seq * dim + 2 * dim * width * (n_tp + 1)),
    )(at, out_all, *w_all, out, w_mine, x, dy, w_post)


def kback_kernel(kv_heads, *refs):
    parts = refs[:3 * kv_heads]
    kraw_ref, cos_ref, sin_ref, kn_ref, out_ref, gain_ref = refs[3 * kv_heads:]

    @pl.when(pl.program_id(0) == 0)
    def _():
        gain_ref[...] = jnp.zeros(gain_ref.shape, F32)

    for h in range(kv_heads):
        own_ref, near_ref, far_ref = parts[3 * h:3 * h + 3]
        cols = slice(h * HD, (h + 1) * HD)
        d_k = own_ref[0, 0] + near_ref[0, 0] + far_ref[0]
        d_raw, d_gain = norm_rope_back(d_k, kraw_ref[:, cols], kn_ref[...], cos_ref[...], sin_ref[...])
        out_ref[:, cols] = d_raw
        gain_ref[0:1, :] += d_gain
        d_v = own_ref[0, 1] + near_ref[0, 1] + far_ref[1]
        out_ref[:, (kv_heads + h) * HD:(kv_heads + h + 1) * HD] = d_v.astype(BF16)


def key_back(parts, k_raw, cos_t, sin_t, k_norm, rows=256):
    kv_heads = len(parts) // 3
    seq = k_raw.shape[0]
    two = pl.BlockSpec((1, 2, rows, HD), lambda i: (0, 0, i, 0))
    one = pl.BlockSpec((2, rows, HD), lambda i: (0, i, 0))
    row = lambda n: pl.BlockSpec((rows, n), lambda i: (i, 0))
    return pl.pallas_call(
        functools.partial(kback_kernel, kv_heads),
        name="kback",
        grid=(seq // rows,),
        in_specs=[two, two, one] * kv_heads + [row(kv_heads * HD), row(HD), row(HD), whole((1, HD))],
        out_specs=[row(2 * kv_heads * HD), whole((8, HD))],
        out_shape=[
            jax.ShapeDtypeStruct((seq, 2 * kv_heads * HD), BF16),
            jax.ShapeDtypeStruct((8, HD), F32),
        ],
        compiler_params=params(1),
        cost_estimate=cost(50 * seq * kv_heads * HD, 12 * seq * kv_heads * HD),
    )(*parts, k_raw, cos_t, sin_t, k_norm)


def dx_kernel(n_tp, tp_ref, *refs):
    q_refs, kv_refs = refs[:n_tp], refs[n_tp:2 * n_tp]
    w_ref, x_ref, dy_ref, wpre_ref, dx_ref, dpre_ref, acc = refs[2 * n_tp:]
    i = pl.program_id(0)
    split = q_refs[0].shape[1]
    total = None
    for s in range(n_tp):
        t = lax.rem(tp_ref[0] + n_tp - s, n_tp)
        part = dot(q_refs[s][...], w_ref[t, :, :split], NT) + dot(kv_refs[s][...], w_ref[t, :, split:], NT)
        total = part if total is None else total + part
    acc[i] = total

    @pl.when(i == pl.num_programs(0) - 1)
    def _():
        d_normed = jnp.concatenate([acc[t] for t in range(acc.shape[0])], axis=1)
        x = x_ref[...].astype(F32)
        inv = lax.rsqrt(jnp.mean(x * x, axis=-1, keepdims=True) + EPS)
        unit = x * inv
        dpre_ref[...] = jnp.broadcast_to(jnp.sum(d_normed * unit, axis=0, keepdims=True), dpre_ref.shape)
        d_unit = d_normed * (1.0 + wpre_ref[...])
        d_x = inv * (d_unit - unit * jnp.mean(d_unit * unit, axis=-1, keepdims=True))
        dx_ref[...] = (dy_ref[...].astype(F32) + d_x).astype(BF16)


def input_grad(tp, q_grads, kv_grads, w_all, x, dy, w_pre, cols=512):
    n_tp = len(q_grads)
    rows, q_width = q_grads[0].shape
    kv_width = kv_grads[0].shape[1]
    dim = x.shape[1]
    here = pl.BlockSpec((rows, dim), lambda i, t: (t[0], 0))
    grid_spec = pltpu.PrefetchScalarGridSpec(
        num_scalar_prefetch=1,
        grid=(dim // cols,),
        in_specs=[whole((rows, q_width))] * n_tp
        + [whole((rows, kv_width))] * n_tp
        + [pl.BlockSpec((n_tp, cols, q_width + kv_width), lambda i, *_: (0, i, 0)), here, here, whole((1, dim))],
        out_specs=[whole((rows, dim)), whole((8, dim))],
        scratch_shapes=[pltpu.VMEM((dim // cols, rows, cols), F32)],
    )
    return pl.pallas_call(
        functools.partial(dx_kernel, n_tp),
        name="dx",
        grid_spec=grid_spec,
        out_shape=[jax.ShapeDtypeStruct((rows, dim), BF16), jax.ShapeDtypeStruct((8, dim), F32)],
        compiler_params=params(1),
        cost_estimate=cost(2 * n_tp * rows * (q_width + kv_width) * dim, 2 * n_tp * (q_width + kv_width) * dim),
    )(tp, *q_grads, *kv_grads, w_all, x, dy, w_pre)


def dw_kernel(n_cp, me_ref, *refs):
    q_refs, kv_refs, n_refs = refs[:n_cp], refs[n_cp:2 * n_cp], refs[2 * n_cp:-7]
    dwq_ref, dwk_ref, dwv_ref, n_buf, g_buf, n_sem, g_sem = refs[-7:]
    i = pl.program_id(0)
    cols = n_buf.shape[3]
    seq, q_width = q_refs[0].shape
    kv_width = kv_refs[0].shape[1]
    me = me_ref[0]

    def fetch(step, par):
        span = pl.ds(pl.multiple_of(step * cols, cols), cols)
        copies, start = [], 0
        for j, ref in enumerate(n_refs):
            s, rows = j % n_cp, ref.shape[0]
            start = (start if s else sum(r.shape[0] for r in n_refs[:j:n_cp]))
            to = n_buf.at[par, jnp.bitwise_xor(me, s), pl.ds(start, rows)]
            copies.append(pltpu.make_async_copy(ref.at[:, span], to, n_sem.at[par, j]))
        return copies

    @pl.when(i == 0)
    def _():
        copies = fetch(0, 0)
        for s in range(n_cp):
            owner = jnp.bitwise_xor(me, s)
            copies.append(pltpu.make_async_copy(q_refs[s], g_buf.at[owner, :, pl.ds(0, q_width)], g_sem.at[s, 0]))
            copies.append(pltpu.make_async_copy(kv_refs[s], g_buf.at[owner, :, pl.ds(q_width, kv_width)], g_sem.at[s, 1]))
        for copy in copies:
            copy.start()
        for copy in copies[len(n_refs):]:
            copy.wait()

    @pl.when(i + 1 < pl.num_programs(0))
    def _():
        for copy in fetch(i + 1, (i + 1) % 2):
            copy.start()

    for copy in fetch(i, i % 2):
        copy.wait()
    lhs = n_buf[i % 2].reshape(n_cp * seq, cols)
    grad = dot(lhs, g_buf[...].reshape(n_cp * seq, q_width + kv_width), TN)
    dwq_ref[...] = grad[:, :q_width]
    dwk_ref[...] = grad[:, q_width:q_width + kv_width // 2]
    dwv_ref[...] = grad[:, q_width + kv_width // 2:]


def weight_grads(me, normed, q_grads, kv_grads, cols=256):
    n_cp = len(q_grads)
    seq, q_width = q_grads[0].shape
    dim, kv_width = normed[0].shape[1], kv_grads[0].shape[1]
    anywhere = pl.BlockSpec(memory_space=pl.ANY)
    tile = lambda n: pl.BlockSpec((cols, n), lambda i, *_: (i, 0))
    grid_spec = pltpu.PrefetchScalarGridSpec(
        num_scalar_prefetch=1,
        grid=(dim // cols,),
        in_specs=[anywhere] * (2 * n_cp + len(normed)),
        out_specs=[tile(q_width), tile(kv_width // 2), tile(kv_width // 2)],
        scratch_shapes=[
            pltpu.VMEM((2, n_cp, seq, cols), BF16),
            pltpu.VMEM((n_cp, seq, q_width + kv_width), BF16),
            pltpu.SemaphoreType.DMA((2, len(normed))),
            pltpu.SemaphoreType.DMA((n_cp, 2)),
        ],
    )
    return pl.pallas_call(
        functools.partial(dw_kernel, n_cp),
        name="dw",
        grid_spec=grid_spec,
        out_shape=[
            jax.ShapeDtypeStruct((dim, q_width), F32),
            jax.ShapeDtypeStruct((dim, kv_width // 2), F32),
            jax.ShapeDtypeStruct((dim, kv_width // 2), F32),
        ],
        compiler_params=params(1),
        cost_estimate=cost(2 * n_cp * seq * dim * (q_width + kv_width), 2 * n_cp * seq * (dim + q_width + kv_width)),
    )(me, *q_grads, *kv_grads, *normed)


def join_kernel(n, core_ref, *refs):
    out_ref = refs[-1]
    i = pl.program_id(0)
    for j in range(n):
        for t, ref in enumerate((refs[j], refs[n + j])):

            @pl.when((lax.rem(i, n) == j) & (jnp.bitwise_xor(i // n, core_ref[0]) == t))
            def _():
                out_ref[...] = ref[...]


def join_halves(core, keep, other):
    n = len(keep)
    rows, width = keep[0].shape
    grid_spec = pltpu.PrefetchScalarGridSpec(
        num_scalar_prefetch=1,
        grid=(2 * n,),
        in_specs=[fixed((rows, width))] * (2 * n),
        out_specs=pl.BlockSpec((rows, width), lambda i, c: (i, 0)),
    )
    return pl.pallas_call(
        functools.partial(join_kernel, n),
        name="join",
        grid_spec=grid_spec,
        out_shape=jax.ShapeDtypeStruct((2 * n * rows, width), F32),
        compiler_params=params(1),
        cost_estimate=cost(n * rows * width, 16 * n * rows * width),
    )(core, *keep, *other)


def solution(mesh):
    n_cp, n_tp, n_dp = mesh.shape["cp"], mesh.shape["tp"], mesh.shape["dp"]
    near = [(i, i ^ 1) for i in range(n_cp)]
    across = [(i, i ^ 2) for i in range(n_cp)]
    beside = [(i, i ^ 1) for i in range(n_dp)]

    def from_cp(value):
        far = lax.ppermute(value, "cp", across)
        return [value, lax.ppermute(value, "cp", near), far, lax.ppermute(far, "cp", near)]

    def per_device(hidden, cotangent, pos_loc, w_q, w_k, w_v, w_o, w_pre, w_post, q_norm, k_norm):
        _, seq, dim = hidden.shape
        x, dy = hidden[0], cotangent[0]
        kv_heads = w_k.shape[1] // HD
        cp, tp, dp = (lax.axis_index(a).astype(jnp.int32) for a in ("cp", "tp", "dp"))
        core = cp % 2
        me, one_tp, one_core = cp.reshape(1), tp.reshape(1), core.reshape(1)

        share = dp * n_cp + cp
        shares = n_dp * n_cp
        cols = dim // shares
        mine = lax.all_gather(lax.dynamic_slice_in_dim(w_o, share * cols, cols, 1), "tp", axis=0, tiled=True)
        w_o_all = from_cp(mine)
        if n_dp == 2:
            own, far = lax.ppermute(mine, "dp", beside), lax.ppermute(w_o_all[2], "dp", beside)
            w_o_all += [own, lax.ppermute(own, "cp", near), far, lax.ppermute(far, "cp", near)]

        cos_t, sin_t = rope_tables(pos_loc)
        qn, kn = q_norm.reshape(1, HD), k_norm.reshape(1, HD)
        wpre, wpost = w_pre.reshape(1, dim), w_post.reshape(1, dim)
        normed, kv_own, k_raw = project_kv(x, wpre, w_k, w_v, kn, cos_t, sin_t)
        kv_blocks = from_cp(kv_own)
        q_fin, q_raw = project_q(normed, w_q, qn, cos_t, sin_t)
        early = seq // 4
        normed_all = from_cp(normed[:early]) + from_cp(normed[early:])
        out, lse = attention_fwd(me, q_fin, kv_blocks, kv_heads)

        out_sent, _ = lax.optimization_barrier((out, mine))
        out_all = lax.all_gather(out_sent, "tp", axis=0, tiled=False)
        at = jnp.stack([share, core])
        y, d_out, give, keep, d_post = post(at, out_all, w_o_all, out, w_o, x, dy, wpost)

        w_rows = dim // shares
        parts = [lax.dynamic_slice_in_dim(w, share * w_rows, w_rows, 0) for w in (w_q, w_k, w_v)]
        parts = jnp.concatenate(parts, axis=1)
        fence, _ = lax.optimization_barrier((parts, out_all))
        w_all = lax.all_gather(fence, ("tp", "dp", "cp"), axis=0, tiled=True).reshape(n_tp, dim, fence.shape[1])

        got = lax.ppermute(give, "cp", near)
        keep = keep + got
        part = keep.shape[0] // 2
        kept, other = [], []
        for j in range(2):
            mine_part = keep[j * part:(j + 1) * part]
            mine_part = mine_part + lax.ppermute(mine_part, "cp", across)
            kept.append(mine_part)
            other.append(lax.ppermute(mine_part, "cp", near))
        d_wo = join_halves(one_core, kept, other)

        dq, dq_gain, dkv_parts = None, [], []
        for h in range(kv_heads):
            dq, dkv, dkv_send, gain = attention_bwd(
                h, me, q_fin, d_out, out, lse, q_raw, cos_t, sin_t, qn, kv_blocks, kv_heads, dq
            )
            dq_gain.append(gain[0])
            got = lax.ppermute(dkv_send, "cp", near)
            dkv_parts += [dkv, got, lax.ppermute(dkv[1] + got[1], "cp", across)]
        d_kv, dk_gain = key_back(dkv_parts, k_raw, cos_t, sin_t, kn)

        rows = seq // n_tp

        def exchange_rows(value):
            pieces = [lax.dynamic_slice_in_dim(value, tp * rows, rows, 0)]
            for s in range(1, n_tp):
                part = lax.dynamic_slice_in_dim(value, ((tp + s) % n_tp) * rows, rows, 0)
                pieces.append(lax.ppermute(part, "tp", [(i, (i + s) % n_tp) for i in range(n_tp)]))
            return pieces

        dq_rows = exchange_rows(dq)
        dq_all = from_cp(dq)
        dkv_rows = exchange_rows(d_kv)
        dx_rows, d_pre = input_grad(one_tp, dq_rows, dkv_rows, w_all, x, dy, wpre)
        d_hidden = lax.all_gather(dx_rows, "tp", axis=0, tiled=True)

        dkv_all = from_cp(d_kv)
        d_wq, d_wk, d_wv = weight_grads(me, normed_all, dq_all, dkv_all)

        small = jnp.concatenate([jnp.where(tp == 0, d_post[0], 0.0), d_pre[0], sum(dq_gain), dk_gain[0]])
        small = small + lax.ppermute(small, "cp", near)
        small = small + lax.ppermute(small, "cp", across)
        small = small + lax.ppermute(small, "tp", [(i, i ^ 1) for i in range(n_tp)])
        small = small + lax.ppermute(small, "tp", [(i, i ^ 2) for i in range(n_tp)])
        d_post, d_pre = small[:dim], small[dim:2 * dim]
        d_qn, d_kn = small[2 * dim:2 * dim + HD], small[2 * dim + HD:]
        return y[None], d_hidden[None], d_wq, d_wk, d_wv, d_wo, d_pre, d_post, d_qn, d_kn

    specs_in = (P('dp', 'cp', None), P('dp', 'cp', None), P(('dp', 'cp')), P(None, 'tp'), P(None, 'tp'), P(None, 'tp'), P('tp', None), P(None), P(None), P(None), P(None))
    specs_out = (P('dp', 'cp', None), P('dp', 'cp', None), P('dp', 'tp'), P('dp', 'tp'), P('dp', 'tp'), P(('dp', 'tp'), None), P('dp'), P('dp'), P('dp'), P('dp'))
    return jax.shard_map(per_device, mesh=mesh, in_specs=specs_in, out_specs=specs_out, check_vma=False)
```

```python
import functools

import jax
import jax.numpy as jnp
from jax import lax
from jax.experimental import pallas as pl
from jax.experimental.pallas import tpu as pltpu
from jax.sharding import PartitionSpec as P


EPS = 1e-6
ROPE_BASE = 1000000.0
ROPE_SCALE = 8.0
NEG_BIG = -1e30
LOG2E = 1.4426950408889634
HD = 128
F32 = jnp.float32
BF16 = jnp.bfloat16
VMEM_MAX = 60 * 1024 * 1024
VMEM_TOP = 67043328
NT = (((1,), (1,)), ((), ()))
TN = (((0,), (0,)), ((), ()))


def dot(a, b, dims=(((1,), (0,)), ((), ()))):
    return lax.dot_general(a, b, dims, preferred_element_type=F32)


def params(dims, vmem=VMEM_MAX):
    return pltpu.CompilerParams(dimension_semantics=("arbitrary",) * dims, vmem_limit_bytes=vmem)


def cost(flops, nbytes, trans=0):
    return pl.CostEstimate(flops=int(flops), bytes_accessed=int(nbytes), transcendentals=int(trans))


def whole(shape):
    return pl.BlockSpec(shape, lambda *_: (0,) * len(shape))


def fixed(shape):
    return pl.BlockSpec(shape, lambda *_: (0,) * len(shape), pipeline_mode=pl.Buffered(buffer_count=1))


def rope_tables(pos_loc):
    half_dim = HD // 2
    inv_freq = 1.0 / (ROPE_SCALE * ROPE_BASE ** (jnp.arange(half_dim, dtype=F32) * (2.0 / HD)))
    angles = pos_loc.astype(F32)[:, None] * inv_freq[None, :]
    cos_t, sin_t = jnp.cos(angles), jnp.sin(angles)
    return jnp.concatenate([cos_t, cos_t], axis=-1), jnp.concatenate([-sin_t, sin_t], axis=-1)


def norm_rope(raw, gain, cos_t, sin_t):
    raw = raw.astype(F32)
    unit = raw * lax.rsqrt(jnp.mean(raw * raw, axis=-1, keepdims=True) + EPS)
    scaled = unit * (1.0 + gain)
    return (scaled * cos_t + pltpu.roll(scaled, HD // 2, 1) * sin_t).astype(BF16)


def norm_rope_back(d_final, raw, gain, cos_t, sin_t):
    raw = raw.astype(F32)
    inv = lax.rsqrt(jnp.mean(raw * raw, axis=-1, keepdims=True) + EPS)
    unit = raw * inv
    d_scaled = d_final * cos_t - pltpu.roll(d_final, HD // 2, 1) * sin_t
    d_gain = jnp.sum(d_scaled * unit, axis=0, keepdims=True)
    d_unit = d_scaled * (1.0 + gain)
    d_raw = inv * (d_unit - unit * jnp.mean(d_unit * unit, axis=-1, keepdims=True))
    return d_raw.astype(BF16), d_gain


def kv_kernel(x_ref, wpre_ref, wk_ref, wv_ref, kn_ref, cos_ref, sin_ref, first_ref, later_ref, kv_ref, kraw_ref):
    x = x_ref[...].astype(F32)
    inv = lax.rsqrt(jnp.mean(x * x, axis=-1, keepdims=True) + EPS)
    normed = (x * inv * (1.0 + wpre_ref[...])).astype(BF16)
    first = pl.program_id(0) == 0

    @pl.when(first)
    def _():
        first_ref[...] = normed

    @pl.when(jnp.logical_not(first))
    def _():
        later_ref[...] = normed

    k_raw = dot(normed, wk_ref[...]).astype(BF16)
    kraw_ref[...] = k_raw
    width = k_raw.shape[1]
    for h in range(width // HD):
        cols = slice(h * HD, (h + 1) * HD)
        kv_ref[:, cols] = norm_rope(k_raw[:, cols], kn_ref[...], cos_ref[...], sin_ref[...])
    kv_ref[:, width:] = dot(normed, wv_ref[...]).astype(BF16)


def parts_spec(rows, dim):
    return [pl.BlockSpec((rows, dim), lambda i: (0, 0)), pl.BlockSpec((rows, dim), lambda i: (jnp.maximum(i - 1, 0), 0))]


def project_kv(x, w_pre, w_k, w_v, k_norm, cos_t, sin_t, rows):
    seq, dim = x.shape
    width = w_k.shape[1]
    row = lambda n: pl.BlockSpec((rows, n), lambda i: (i, 0))
    return pl.pallas_call(
        kv_kernel,
        name="pkv",
        grid=(seq // rows,),
        in_specs=[row(dim), whole((1, dim)), fixed(w_k.shape), fixed(w_v.shape), whole((1, HD)), row(HD), row(HD)],
        out_specs=parts_spec(rows, dim) + [row(2 * width), row(width)],
        out_shape=[
            jax.ShapeDtypeStruct((rows, dim), BF16),
            jax.ShapeDtypeStruct((seq - rows, dim), BF16),
            jax.ShapeDtypeStruct((seq, 2 * width), BF16),
            jax.ShapeDtypeStruct((seq, width), BF16),
        ],
        compiler_params=params(1),
        cost_estimate=cost(4 * seq * dim * width, 4 * seq * dim + 4 * dim * width),
    )(x, w_pre, w_k, w_v, k_norm, cos_t, sin_t)


def q_kernel(first_ref, later_ref, wq_ref, qn_ref, cos_ref, sin_ref, qfin_ref, qraw_ref):
    normed = jnp.where(pl.program_id(0) == 0, first_ref[...], later_ref[...])
    q_raw = dot(normed, wq_ref[...]).astype(BF16)
    for h in range(qfin_ref.shape[0]):
        part = q_raw[:, h * HD:(h + 1) * HD]
        qraw_ref[h] = part
        qfin_ref[h] = norm_rope(part, qn_ref[...], cos_ref[...], sin_ref[...])


def project_q(first, later, w_q, q_norm, cos_t, sin_t):
    rows, dim = first.shape
    seq = rows + later.shape[0]
    heads = w_q.shape[1] // HD
    row = lambda n: pl.BlockSpec((rows, n), lambda i: (i, 0))
    head_rows = pl.BlockSpec((heads, rows, HD), lambda i: (0, i, 0))
    shape = jax.ShapeDtypeStruct((heads, seq, HD), BF16)
    return pl.pallas_call(
        q_kernel,
        name="pq",
        grid=(seq // rows,),
        in_specs=parts_spec(rows, dim) + [fixed(w_q.shape), whole((1, HD)), row(HD), row(HD)],
        out_specs=[head_rows, head_rows],
        out_shape=[shape, shape],
        compiler_params=params(1),
        cost_estimate=cost(2 * seq * dim * heads * HD, 2 * seq * dim + 2 * dim * heads * HD),
    )(first, later, w_q, q_norm, cos_t, sin_t)


def load_kv(kv_refs, k_buf, v_buf, sems, heads):
    kv_heads = kv_refs[0].shape[1] // (2 * HD)
    copies = []
    for s, ref in enumerate(kv_refs):
        for i, h in enumerate(heads):
            for t, buf in enumerate((k_buf, v_buf)):
                src = ref.at[:, pl.ds((t * kv_heads + h) * HD, HD)]
                copies.append(pltpu.make_async_copy(src, buf.at[i, s], sems.at[s, i, t]))
    for copy in copies:
        copy.start()
    for copy in copies:
        copy.wait()


def piece_place(piece, me, n_cp):
    upper = piece >= n_cp
    owner = jnp.where(upper, 2 * n_cp - 1 - piece, piece)
    return jnp.bitwise_xor(owner, me), upper.astype(jnp.int32)


def fwd_kernel(n_cp, me_ref, q_ref, *rest):
    kv_refs = rest[:n_cp]
    o_ref, lse_ref, k_buf, v_buf, m_scr, acc_scr, sems = rest[n_cp:]
    h, half = pl.program_id(0), pl.program_id(1)
    groups, rows, _ = q_ref.shape

    @pl.when((h == 0) & (half == 0))
    def _():
        load_kv(kv_refs, k_buf, v_buf, sems, range(k_buf.shape[0]))

    me = me_ref[0]
    piece = jnp.where(half == 0, me, 2 * n_cp - 1 - me)
    scale = HD ** -0.5 * LOG2E
    m_scr[...] = jnp.full(m_scr.shape, NEG_BIG, F32)
    acc_scr[...] = jnp.zeros(acc_scr.shape, F32)

    def block(j, masked):
        slot, upper = piece_place(j, me, n_cp)
        span = pl.ds(pl.multiple_of(upper * rows, rows), rows)
        k = k_buf[h, slot, span, :]
        v_ext = jnp.concatenate([v_buf[h, slot, span, :], jnp.ones((rows, HD), BF16)], axis=1)
        scores = [dot(q_ref[g], k, NT) * scale for g in range(groups)]
        for g in range(groups):
            s = scores[g]
            if masked:
                q_pos = lax.broadcasted_iota(jnp.int32, s.shape, 0)
                k_pos = lax.broadcasted_iota(jnp.int32, s.shape, 1)
                s = jnp.where(k_pos <= q_pos, s, NEG_BIG)
            m_old = m_scr[g]
            m_new = jnp.maximum(m_old, jnp.max(s, axis=1, keepdims=True))
            alpha = jnp.exp2(m_old - m_new)
            p = jnp.exp2(s - jnp.concatenate([m_new] * (rows // HD), axis=1)).astype(BF16)
            acc_scr[g] = acc_scr[g] * jnp.concatenate([alpha, alpha], axis=1) + dot(p, v_ext)
            m_scr[g] = m_new

    def full(j, carry):
        block(j, False)
        return carry

    lax.fori_loop(0, piece, full, 0)
    block(piece, True)
    for g in range(groups):
        l = acc_scr[g, :, HD:]
        o_ref[:, g * HD:(g + 1) * HD] = (acc_scr[g, :, :HD] / l).astype(BF16)
        lse_ref[0, g:g + 1, :] = jnp.transpose(m_scr[g] + jnp.log2(l))[0:1, :]


def attention_fwd(me, q_fin, kv_blocks, kv_heads):
    heads, seq, _ = q_fin.shape
    n_cp = len(kv_blocks)
    groups = heads // kv_heads
    rows = seq // 2
    grid_spec = pltpu.PrefetchScalarGridSpec(
        num_scalar_prefetch=1,
        grid=(kv_heads, 2),
        in_specs=[pl.BlockSpec((groups, rows, HD), lambda h, i, *_: (h, i, 0))] + [pl.BlockSpec(memory_space=pl.ANY)] * n_cp,
        out_specs=[
            pl.BlockSpec((rows, groups * HD), lambda h, i, *_: (i, h)),
            pl.BlockSpec((1, 8, rows), lambda h, i, *_: (h, 0, i)),
        ],
        scratch_shapes=[
            pltpu.VMEM((kv_heads, n_cp, seq, HD), BF16),
            pltpu.VMEM((kv_heads, n_cp, seq, HD), BF16),
            pltpu.VMEM((groups, rows, HD), F32),
            pltpu.VMEM((groups, rows, 2 * HD), F32),
            pltpu.SemaphoreType.DMA((n_cp, kv_heads, 2)),
        ],
    )
    pairs = heads * rows * rows * (2 * n_cp + 1)
    return pl.pallas_call(
        functools.partial(fwd_kernel, n_cp),
        name="fwd",
        grid_spec=grid_spec,
        out_shape=[
            jax.ShapeDtypeStruct((seq, heads * HD), BF16),
            jax.ShapeDtypeStruct((kv_heads, 8, seq), F32),
        ],
        compiler_params=params(2),
        cost_estimate=cost(4 * pairs * HD, 8 * seq * heads * HD, pairs),
    )(me, q_fin, *kv_blocks)


def bwd_kernel(n_cp, head, me_ref, q_ref, do_ref, o_ref, lse_ref, qraw_ref, cos_ref, sin_ref, qn_ref, *rest):
    kv_refs = rest[:n_cp]
    dq_ref, keep_ref, send_ref, gain_ref, k_buf, v_buf, dq_scr, dkv_scr, sems = rest[-9:]
    half = pl.program_id(0)
    groups, rows, _ = q_ref.shape

    @pl.when(half == 0)
    def _():
        load_kv(kv_refs, k_buf, v_buf, sems, (head,))
        gain_ref[...] = jnp.zeros(gain_ref.shape, F32)
        dkv_scr[...] = jnp.zeros(dkv_scr.shape, F32)

    me = me_ref[0]
    piece = jnp.where(half == 0, me, 2 * n_cp - 1 - me)
    scale = HD ** -0.5
    delta = []
    for g in range(groups):
        prod = do_ref[g].astype(F32) * o_ref[:, g * HD:(g + 1) * HD].astype(F32)
        column = jnp.broadcast_to(jnp.sum(prod, axis=1, keepdims=True), (rows, HD))
        delta.append(jnp.transpose(column)[0:1, :])
    dq_scr[...] = jnp.zeros(dq_scr.shape, F32)

    def block(j, masked):
        slot, upper = piece_place(j, me, n_cp)
        span = pl.ds(pl.multiple_of(upper * rows, rows), rows)
        k = k_buf[0, slot, span, :]
        v = v_buf[0, slot, span, :]
        probs, d_scores = [], []
        for g in range(groups):
            s = dot(k, q_ref[g], NT)
            p = jnp.exp2(s * (scale * LOG2E) - lse_ref[0, g:g + 1, :])
            if masked:
                k_pos = lax.broadcasted_iota(jnp.int32, s.shape, 0)
                q_pos = lax.broadcasted_iota(jnp.int32, s.shape, 1)
                p = jnp.where(k_pos <= q_pos, p, 0.0)
            probs.append(p.astype(BF16))
            d_scores.append((p * (dot(v, do_ref[g], NT) - delta[g])).astype(BF16))
        for g in range(groups):
            dq_scr[g] += dot(d_scores[g], k, TN)
        index = (slot % 2) * (n_cp // 2) + slot // 2
        d_all = jnp.concatenate(d_scores, axis=1)
        p_all = jnp.concatenate(probs, axis=1)
        dkv_scr[index, 0, span, :] += dot(d_all, q_ref[...].reshape(groups * rows, HD)) * scale
        dkv_scr[index, 1, span, :] += dot(p_all, do_ref[...].reshape(groups * rows, HD))

    def full(j, carry):
        block(j, False)
        return carry

    lax.fori_loop(0, piece, full, 0)
    block(piece, True)
    for g in range(groups):
        d_raw, d_gain = norm_rope_back(dq_scr[g] * scale, qraw_ref[g], qn_ref[...], cos_ref[...], sin_ref[...])
        dq_ref[:, g * HD:(g + 1) * HD] = d_raw
        gain_ref[0:1, :] += d_gain

    @pl.when(half == 1)
    def _():
        for i in range(n_cp // 2):
            keep_ref[i] = dkv_scr[i]
            send_ref[i] = dkv_scr[n_cp // 2 + i]


def attention_bwd(head, me, q_fin, d_out, out, lse, q_raw, cos_t, sin_t, q_norm, kv_blocks, kv_heads, dq=None):
    heads, seq, _ = q_fin.shape
    n_cp = len(kv_blocks)
    groups = heads // kv_heads
    rows = seq // 2
    by_head = pl.BlockSpec((groups, rows, HD), lambda i, *_: (head, i, 0))
    by_row = pl.BlockSpec((rows, groups * HD), lambda i, *_: (i, head))
    table = pl.BlockSpec((rows, HD), lambda i, *_: (i, 0))
    anywhere = pl.BlockSpec(memory_space=pl.ANY)
    kv_grads = jax.ShapeDtypeStruct((n_cp // 2, 2, seq, HD), F32)
    extra = () if dq is None else (dq,)
    grid_spec = pltpu.PrefetchScalarGridSpec(
        num_scalar_prefetch=1,
        grid=(2,),
        in_specs=[
            by_head,
            by_head,
            by_row,
            pl.BlockSpec((1, 8, rows), lambda i, *_: (head, 0, i)),
            by_head,
            table,
            table,
            whole((1, HD)),
        ]
        + [anywhere] * (n_cp + len(extra)),
        out_specs=[by_row, whole(kv_grads.shape), whole(kv_grads.shape), whole((8, HD))],
        scratch_shapes=[
            pltpu.VMEM((1, n_cp, seq, HD), BF16),
            pltpu.VMEM((1, n_cp, seq, HD), BF16),
            pltpu.VMEM((groups, rows, HD), F32),
            pltpu.VMEM((n_cp, 2, seq, HD), F32),
            pltpu.SemaphoreType.DMA((n_cp, 1, 2)),
        ],
    )
    pairs = groups * rows * rows * (2 * n_cp + 1)
    return pl.pallas_call(
        functools.partial(bwd_kernel, n_cp, head),
        grid_spec=grid_spec,
        out_shape=[
            jax.ShapeDtypeStruct((seq, heads * HD), BF16),
            kv_grads,
            kv_grads,
            jax.ShapeDtypeStruct((8, HD), F32),
        ],
        input_output_aliases={9 + n_cp: 0} if extra else {},
        compiler_params=params(1),
        cost_estimate=cost(10 * pairs * HD, 16 * seq * groups * HD, pairs),
    )(me, q_fin, d_out, out, lse, q_raw, cos_t, sin_t, q_norm, *kv_blocks, *extra)


def post_kernel(n_w, n_tiles, at_ref, o_ref, *rest):
    w_refs = rest[:n_w]
    mine_ref, wmine_ref, x_ref, dy_ref, wpost_ref, y_ref, do_ref, give_ref, keep_ref, dpost_ref = rest[n_w:n_w + 10]
    o_buf, w_buf, attn_scr, o_sem, w_sem = rest[n_w + 10:]
    i = pl.program_id(0)
    n_tp, _, width = o_ref.shape
    rows = x_ref.shape[0]

    def weight_copy(s, par):
        return pltpu.make_async_copy(w_refs[s], w_buf.at[par], w_sem.at[par])

    @pl.when(i == 0)
    def _():
        copies = [
            pltpu.make_async_copy(o_ref.at[t], o_buf.at[:, pl.ds(t * width, width)], o_sem.at[t]) for t in range(n_tp)
        ]
        for copy in copies:
            copy.start()
        weight_copy(0, 0).start()
        for copy in copies:
            copy.wait()

    for s in range(1, n_w):

        @pl.when(i == s - 1)
        def _():
            weight_copy(s, s % 2).start()

    @pl.when(i < n_w)
    def _():
        par = lax.rem(i, 2)
        weight_copy(0, par).wait()
        attn_scr[jnp.bitwise_xor(at_ref[0], i)] = dot(o_buf[...], w_buf[par])

    @pl.when(i == n_tiles)
    def _():
        dpost_ref[...] = jnp.zeros(dpost_ref.shape, F32)
        give_ref[...] = jnp.zeros(give_ref.shape, F32)
        keep_ref[...] = jnp.zeros(keep_ref.shape, F32)

    @pl.when(i >= n_tiles)
    def _():
        span = pl.ds(pl.multiple_of((i - n_tiles) * rows, rows), rows)
        attn = jnp.concatenate([attn_scr[s, span, :] for s in range(n_w)], axis=1)
        inv = lax.rsqrt(jnp.mean(attn * attn, axis=-1, keepdims=True) + EPS)
        unit = attn * inv
        gain = 1.0 + wpost_ref[...]
        y_ref[...] = (x_ref[...].astype(F32) + unit * gain).astype(BF16)
        dy = dy_ref[...].astype(F32)
        dpost_ref[0:1, :] += jnp.sum(dy * unit, axis=0, keepdims=True)
        d_unit = dy * gain
        d_attn = (inv * (d_unit - unit * jnp.mean(d_unit * unit, axis=-1, keepdims=True))).astype(BF16)
        d_out = dot(d_attn, wmine_ref[...], NT)
        for h in range(do_ref.shape[0]):
            do_ref[h] = d_out[:, h * HD:(h + 1) * HD].astype(BF16)
        half = give_ref.shape[0]
        core = at_ref[1]
        give_ref[...] += dot(mine_ref[:, pl.ds(pl.multiple_of((1 - core) * half, HD), half)], d_attn, TN)
        keep_ref[...] += dot(mine_ref[:, pl.ds(pl.multiple_of(core * half, HD), half)], d_attn, TN)


def post(at, out_all, w_all, out, w_mine, x, dy, w_post, rows=256):
    n_tp, seq, width = out_all.shape
    dim = x.shape[1]
    heads = width // HD
    n_w = len(w_all)
    block = lambda i: jnp.maximum(i - n_w, 0)
    row = lambda n: pl.BlockSpec((rows, n), lambda i, *_: (block(i), 0))
    half = jax.ShapeDtypeStruct((width // 2, dim), F32)
    grid_spec = pltpu.PrefetchScalarGridSpec(
        num_scalar_prefetch=1,
        grid=(n_w + seq // rows,),
        in_specs=[pl.BlockSpec(memory_space=pl.ANY)] * (1 + n_w)
        + [row(width), fixed(w_mine.shape), row(dim), row(dim), whole((1, dim))],
        out_specs=[
            row(dim),
            pl.BlockSpec((heads, rows, HD), lambda i, *_: (0, block(i), 0)),
            fixed(half.shape),
            fixed(half.shape),
            whole((8, dim)),
        ],
        scratch_shapes=[
            pltpu.VMEM((seq, n_tp * width), BF16),
            pltpu.VMEM((2, n_tp * width, dim // n_w), BF16),
            pltpu.VMEM((n_w, seq, dim // n_w), F32),
            pltpu.SemaphoreType.DMA((n_tp,)),
            pltpu.SemaphoreType.DMA((2,)),
        ],
    )
    return pl.pallas_call(
        functools.partial(post_kernel, n_w, n_w),
        name="post",
        grid_spec=grid_spec,
        out_shape=[
            jax.ShapeDtypeStruct((seq, dim), BF16),
            jax.ShapeDtypeStruct((heads, seq, HD), BF16),
            half,
            half,
            jax.ShapeDtypeStruct((8, dim), F32),
        ],
        compiler_params=params(1, VMEM_TOP),
        cost_estimate=cost(2 * seq * dim * width * (n_tp + 2), 8 * seq * dim + 2 * dim * width * (n_tp + 1)),
    )(at, out_all, *w_all, out, w_mine, x, dy, w_post)


def kback_kernel(kv_heads, *refs):
    parts = refs[:3 * kv_heads]
    kraw_ref, cos_ref, sin_ref, kn_ref, out_ref, gain_ref = refs[3 * kv_heads:]

    @pl.when(pl.program_id(0) == 0)
    def _():
        gain_ref[...] = jnp.zeros(gain_ref.shape, F32)

    for h in range(kv_heads):
        own_ref, near_ref, far_ref = parts[3 * h:3 * h + 3]
        cols = slice(h * HD, (h + 1) * HD)
        d_k = own_ref[0, 0] + near_ref[0, 0] + far_ref[0]
        d_raw, d_gain = norm_rope_back(d_k, kraw_ref[:, cols], kn_ref[...], cos_ref[...], sin_ref[...])
        out_ref[:, cols] = d_raw
        gain_ref[0:1, :] += d_gain
        d_v = own_ref[0, 1] + near_ref[0, 1] + far_ref[1]
        out_ref[:, (kv_heads + h) * HD:(kv_heads + h + 1) * HD] = d_v.astype(BF16)


def key_back(parts, k_raw, cos_t, sin_t, k_norm, rows=256):
    kv_heads = len(parts) // 3
    seq = k_raw.shape[0]
    two = pl.BlockSpec((1, 2, rows, HD), lambda i: (0, 0, i, 0))
    one = pl.BlockSpec((2, rows, HD), lambda i: (0, i, 0))
    row = lambda n: pl.BlockSpec((rows, n), lambda i: (i, 0))
    return pl.pallas_call(
        functools.partial(kback_kernel, kv_heads),
        name="kback",
        grid=(seq // rows,),
        in_specs=[two, two, one] * kv_heads + [row(kv_heads * HD), row(HD), row(HD), whole((1, HD))],
        out_specs=[row(2 * kv_heads * HD), whole((8, HD))],
        out_shape=[
            jax.ShapeDtypeStruct((seq, 2 * kv_heads * HD), BF16),
            jax.ShapeDtypeStruct((8, HD), F32),
        ],
        compiler_params=params(1),
        cost_estimate=cost(50 * seq * kv_heads * HD, 12 * seq * kv_heads * HD),
    )(*parts, k_raw, cos_t, sin_t, k_norm)


def dx_kernel(n_tp, tp_ref, *refs):
    q_refs, kv_refs = refs[:n_tp], refs[n_tp:2 * n_tp]
    w_ref, x_ref, dy_ref, wpre_ref, dx_ref, dpre_ref, acc = refs[2 * n_tp:]
    i = pl.program_id(0)
    split = q_refs[0].shape[1]
    total = None
    for s in range(n_tp):
        t = lax.rem(tp_ref[0] + n_tp - s, n_tp)
        part = dot(q_refs[s][...], w_ref[t, :, :split], NT) + dot(kv_refs[s][...], w_ref[t, :, split:], NT)
        total = part if total is None else total + part
    acc[i] = total

    @pl.when(i == pl.num_programs(0) - 1)
    def _():
        d_normed = jnp.concatenate([acc[t] for t in range(acc.shape[0])], axis=1)
        x = x_ref[...].astype(F32)
        inv = lax.rsqrt(jnp.mean(x * x, axis=-1, keepdims=True) + EPS)
        unit = x * inv
        dpre_ref[...] = jnp.broadcast_to(jnp.sum(d_normed * unit, axis=0, keepdims=True), dpre_ref.shape)
        d_unit = d_normed * (1.0 + wpre_ref[...])
        d_x = inv * (d_unit - unit * jnp.mean(d_unit * unit, axis=-1, keepdims=True))
        dx_ref[...] = (dy_ref[...].astype(F32) + d_x).astype(BF16)


def input_grad(tp, q_grads, kv_grads, w_all, x, dy, w_pre, cols=512):
    n_tp = len(q_grads)
    rows, q_width = q_grads[0].shape
    kv_width = kv_grads[0].shape[1]
    dim = x.shape[1]
    here = pl.BlockSpec((rows, dim), lambda i, t: (t[0], 0))
    grid_spec = pltpu.PrefetchScalarGridSpec(
        num_scalar_prefetch=1,
        grid=(dim // cols,),
        in_specs=[whole((rows, q_width))] * n_tp
        + [whole((rows, kv_width))] * n_tp
        + [pl.BlockSpec((n_tp, cols, q_width + kv_width), lambda i, *_: (0, i, 0)), here, here, whole((1, dim))],
        out_specs=[whole((rows, dim)), whole((8, dim))],
        scratch_shapes=[pltpu.VMEM((dim // cols, rows, cols), F32)],
    )
    return pl.pallas_call(
        functools.partial(dx_kernel, n_tp),
        name="dx",
        grid_spec=grid_spec,
        out_shape=[jax.ShapeDtypeStruct((rows, dim), BF16), jax.ShapeDtypeStruct((8, dim), F32)],
        compiler_params=params(1),
        cost_estimate=cost(2 * n_tp * rows * (q_width + kv_width) * dim, 2 * n_tp * (q_width + kv_width) * dim),
    )(tp, *q_grads, *kv_grads, w_all, x, dy, w_pre)


def dw_kernel(n_cp, me_ref, *refs):
    q_refs, kv_refs, n_refs = refs[:n_cp], refs[n_cp:2 * n_cp], refs[2 * n_cp:-7]
    dwq_ref, dwk_ref, dwv_ref, n_buf, g_buf, n_sem, g_sem = refs[-7:]
    i = pl.program_id(0)
    cols = n_buf.shape[3]
    seq, q_width = q_refs[0].shape
    kv_width = kv_refs[0].shape[1]
    me = me_ref[0]

    def fetch(step, par):
        span = pl.ds(pl.multiple_of(step * cols, cols), cols)
        copies, start = [], 0
        for j, ref in enumerate(n_refs):
            s, rows = j % n_cp, ref.shape[0]
            start = (start if s else sum(r.shape[0] for r in n_refs[:j:n_cp]))
            to = n_buf.at[par, jnp.bitwise_xor(me, s), pl.ds(start, rows)]
            copies.append(pltpu.make_async_copy(ref.at[:, span], to, n_sem.at[par, j]))
        return copies

    @pl.when(i == 0)
    def _():
        copies = fetch(0, 0)
        for s in range(n_cp):
            owner = jnp.bitwise_xor(me, s)
            copies.append(pltpu.make_async_copy(q_refs[s], g_buf.at[owner, :, pl.ds(0, q_width)], g_sem.at[s, 0]))
            copies.append(pltpu.make_async_copy(kv_refs[s], g_buf.at[owner, :, pl.ds(q_width, kv_width)], g_sem.at[s, 1]))
        for copy in copies:
            copy.start()
        for copy in copies[len(n_refs):]:
            copy.wait()

    @pl.when(i + 1 < pl.num_programs(0))
    def _():
        for copy in fetch(i + 1, (i + 1) % 2):
            copy.start()

    for copy in fetch(i, i % 2):
        copy.wait()
    lhs = n_buf[i % 2].reshape(n_cp * seq, cols)
    grad = dot(lhs, g_buf[...].reshape(n_cp * seq, q_width + kv_width), TN)
    dwq_ref[...] = grad[:, :q_width]
    dwk_ref[...] = grad[:, q_width:q_width + kv_width // 2]
    dwv_ref[...] = grad[:, q_width + kv_width // 2:]


def weight_grads(me, normed, q_grads, kv_grads, cols=256):
    n_cp = len(q_grads)
    seq, q_width = q_grads[0].shape
    dim, kv_width = normed[0].shape[1], kv_grads[0].shape[1]
    anywhere = pl.BlockSpec(memory_space=pl.ANY)
    tile = lambda n: pl.BlockSpec((cols, n), lambda i, *_: (i, 0))
    grid_spec = pltpu.PrefetchScalarGridSpec(
        num_scalar_prefetch=1,
        grid=(dim // cols,),
        in_specs=[anywhere] * (2 * n_cp + len(normed)),
        out_specs=[tile(q_width), tile(kv_width // 2), tile(kv_width // 2)],
        scratch_shapes=[
            pltpu.VMEM((2, n_cp, seq, cols), BF16),
            pltpu.VMEM((n_cp, seq, q_width + kv_width), BF16),
            pltpu.SemaphoreType.DMA((2, len(normed))),
            pltpu.SemaphoreType.DMA((n_cp, 2)),
        ],
    )
    return pl.pallas_call(
        functools.partial(dw_kernel, n_cp),
        name="dw",
        grid_spec=grid_spec,
        out_shape=[
            jax.ShapeDtypeStruct((dim, q_width), F32),
            jax.ShapeDtypeStruct((dim, kv_width // 2), F32),
            jax.ShapeDtypeStruct((dim, kv_width // 2), F32),
        ],
        compiler_params=params(1),
        cost_estimate=cost(2 * n_cp * seq * dim * (q_width + kv_width), 2 * n_cp * seq * (dim + q_width + kv_width)),
    )(me, *q_grads, *kv_grads, *normed)


def join_kernel(core_ref, keep_ref, other_ref, *rest):
    half = pl.program_id(0)

    @pl.when(half == core_ref[0])
    def _():
        rest[-1][...] = keep_ref[...]

    @pl.when(half != core_ref[0])
    def _():
        rest[-1][...] = other_ref[...]


def join_halves(core, keep, other, start, half, total=None):
    block, width = HD, keep.shape[1]
    n = keep.shape[0] // block
    extra = () if total is None else (total,)
    part = pl.BlockSpec((block, width), lambda i, j, c: (j, 0))
    grid_spec = pltpu.PrefetchScalarGridSpec(
        num_scalar_prefetch=1,
        grid=(2, n),
        in_specs=[part, part] + [pl.BlockSpec(memory_space=pl.ANY)] * len(extra),
        out_specs=pl.BlockSpec((block, width), lambda i, j, c: (i * (half // block) + start // block + j, 0)),
    )
    return pl.pallas_call(
        join_kernel,
        name="join",
        grid_spec=grid_spec,
        out_shape=jax.ShapeDtypeStruct((2 * half, width), F32),
        input_output_aliases={3: 0} if extra else {},
        compiler_params=params(2),
        cost_estimate=cost(n * block * width, 16 * n * block * width),
    )(core, keep, other, *extra)


def solution(mesh):
    n_cp, n_tp, n_dp = mesh.shape["cp"], mesh.shape["tp"], mesh.shape["dp"]
    near = [(i, i ^ 1) for i in range(n_cp)]
    across = [(i, i ^ 2) for i in range(n_cp)]
    beside = [(i, i ^ 1) for i in range(n_dp)]

    def from_cp(value):
        far = lax.ppermute(value, "cp", across)
        return [value, lax.ppermute(value, "cp", near), far, lax.ppermute(far, "cp", near)]

    def per_device(hidden, cotangent, pos_loc, w_q, w_k, w_v, w_o, w_pre, w_post, q_norm, k_norm):
        _, seq, dim = hidden.shape
        x, dy = hidden[0], cotangent[0]
        kv_heads = w_k.shape[1] // HD
        cp, tp, dp = (lax.axis_index(a).astype(jnp.int32) for a in ("cp", "tp", "dp"))
        core = cp % 2
        me, one_tp, one_core = cp.reshape(1), tp.reshape(1), core.reshape(1)

        share = dp * n_cp + cp
        shares = n_dp * n_cp
        cols = dim // shares
        mine = lax.all_gather(lax.dynamic_slice_in_dim(w_o, share * cols, cols, 1), "tp", axis=0, tiled=True)
        w_o_all = from_cp(mine)
        if n_dp == 2:
            own, far = lax.ppermute(mine, "dp", beside), lax.ppermute(w_o_all[2], "dp", beside)
            w_o_all += [own, lax.ppermute(own, "cp", near), far, lax.ppermute(far, "cp", near)]

        cos_t, sin_t = rope_tables(pos_loc)
        qn, kn = q_norm.reshape(1, HD), k_norm.reshape(1, HD)
        wpre, wpost = w_pre.reshape(1, dim), w_post.reshape(1, dim)
        first, later, kv_own, k_raw = project_kv(x, wpre, w_k, w_v, kn, cos_t, sin_t, seq // 4)
        kv_blocks = from_cp(kv_own)
        q_fin, q_raw = project_q(first, later, w_q, qn, cos_t, sin_t)
        normed_all = from_cp(first) + from_cp(later)
        out, lse = attention_fwd(me, q_fin, kv_blocks, kv_heads)

        out_sent, _ = lax.optimization_barrier((out, mine))
        out_all = lax.all_gather(out_sent, "tp", axis=0, tiled=False)
        at = jnp.stack([share, core])
        y, d_out, give, keep, d_post = post(at, out_all, w_o_all, out, w_o, x, dy, wpost)

        w_rows = dim // shares
        parts = [lax.dynamic_slice_in_dim(w, share * w_rows, w_rows, 0) for w in (w_q, w_k, w_v)]
        parts = jnp.concatenate(parts, axis=1)
        fence, _ = lax.optimization_barrier((parts, out_all))
        w_all = lax.all_gather(fence, ("tp", "dp", "cp"), axis=0, tiled=True).reshape(n_tp, dim, fence.shape[1])

        got = lax.ppermute(give, "cp", near)
        half = keep.shape[0]
        d_wo = None
        for start, stop in ((0, half - HD), (half - HD, half)):
            mine_part = keep[start:stop] + got[start:stop]
            mine_part = mine_part + lax.ppermute(mine_part, "cp", across)
            other = lax.ppermute(mine_part, "cp", near)
            d_wo = join_halves(one_core, mine_part, other, start, half, d_wo)

        dq, dq_gain, dkv_parts = None, [], []
        for h in range(kv_heads):
            dq, dkv, dkv_send, gain = attention_bwd(
                h, me, q_fin, d_out, out, lse, q_raw, cos_t, sin_t, qn, kv_blocks, kv_heads, dq
            )
            dq_gain.append(gain[0])
            got = lax.ppermute(dkv_send, "cp", near)
            dkv_parts += [dkv, got, lax.ppermute(dkv[1] + got[1], "cp", across)]
        d_kv, dk_gain = key_back(dkv_parts, k_raw, cos_t, sin_t, kn)

        rows = seq // n_tp

        def exchange_rows(value):
            pieces = [lax.dynamic_slice_in_dim(value, tp * rows, rows, 0)]
            for s in range(1, n_tp):
                part = lax.dynamic_slice_in_dim(value, ((tp + s) % n_tp) * rows, rows, 0)
                pieces.append(lax.ppermute(part, "tp", [(i, (i + s) % n_tp) for i in range(n_tp)]))
            return pieces

        dq_rows = exchange_rows(dq)
        dq_all = from_cp(dq)
        dkv_rows = exchange_rows(d_kv)
        dx_rows, d_pre = input_grad(one_tp, dq_rows, dkv_rows, w_all, x, dy, wpre)
        d_hidden = lax.all_gather(dx_rows, "tp", axis=0, tiled=True)

        dkv_all = from_cp(d_kv)
        d_wq, d_wk, d_wv = weight_grads(me, normed_all, dq_all, dkv_all)

        small = jnp.concatenate([jnp.where(tp == 0, d_post[0], 0.0), d_pre[0], sum(dq_gain), dk_gain[0]])
        small = small + lax.ppermute(small, "cp", near)
        small = small + lax.ppermute(small, "cp", across)
        small = small + lax.ppermute(small, "tp", [(i, i ^ 1) for i in range(n_tp)])
        small = small + lax.ppermute(small, "tp", [(i, i ^ 2) for i in range(n_tp)])
        d_post, d_pre = small[:dim], small[dim:2 * dim]
        d_qn, d_kn = small[2 * dim:2 * dim + HD], small[2 * dim + HD:]
        return y[None], d_hidden[None], d_wq, d_wk, d_wv, d_wo, d_pre, d_post, d_qn, d_kn

    specs_in = (P('dp', 'cp', None), P('dp', 'cp', None), P(('dp', 'cp')), P(None, 'tp'), P(None, 'tp'), P(None, 'tp'), P('tp', None), P(None), P(None), P(None), P(None))
    specs_out = (P('dp', 'cp', None), P('dp', 'cp', None), P('dp', 'tp'), P('dp', 'tp'), P('dp', 'tp'), P(('dp', 'tp'), None), P('dp'), P('dp'), P('dp'), P('dp'))
    return jax.shard_map(per_device, mesh=mesh, in_specs=specs_in, out_specs=specs_out, check_vma=False)
```

```python
import functools

import jax
import jax.numpy as jnp
from jax import lax
from jax.experimental import pallas as pl
from jax.experimental.pallas import tpu as pltpu
from jax.sharding import PartitionSpec as P


EPS = 1e-6
ROPE_BASE = 1000000.0
ROPE_SCALE = 8.0
NEG_BIG = -1e30
LOG2E = 1.4426950408889634
HD = 128
F32 = jnp.float32
BF16 = jnp.bfloat16
VMEM_MAX = 60 * 1024 * 1024
VMEM_TOP = 67043328
NT = (((1,), (1,)), ((), ()))
TN = (((0,), (0,)), ((), ()))


def dot(a, b, dims=(((1,), (0,)), ((), ()))):
    return lax.dot_general(a, b, dims, preferred_element_type=F32)


def params(dims, vmem=VMEM_MAX):
    return pltpu.CompilerParams(dimension_semantics=("arbitrary",) * dims, vmem_limit_bytes=vmem)


def cost(flops, nbytes, trans=0):
    return pl.CostEstimate(flops=int(flops), bytes_accessed=int(nbytes), transcendentals=int(trans))


def whole(shape):
    return pl.BlockSpec(shape, lambda *_: (0,) * len(shape))


def fixed(shape):
    return pl.BlockSpec(shape, lambda *_: (0,) * len(shape), pipeline_mode=pl.Buffered(buffer_count=1))


def rope_tables(pos_loc):
    half_dim = HD // 2
    inv_freq = 1.0 / (ROPE_SCALE * ROPE_BASE ** (jnp.arange(half_dim, dtype=F32) * (2.0 / HD)))
    angles = pos_loc.astype(F32)[:, None] * inv_freq[None, :]
    cos_t, sin_t = jnp.cos(angles), jnp.sin(angles)
    return jnp.concatenate([cos_t, cos_t], axis=-1), jnp.concatenate([-sin_t, sin_t], axis=-1)


def norm_rope(raw, gain, cos_t, sin_t):
    raw = raw.astype(F32)
    unit = raw * lax.rsqrt(jnp.mean(raw * raw, axis=-1, keepdims=True) + EPS)
    scaled = unit * (1.0 + gain)
    return (scaled * cos_t + pltpu.roll(scaled, HD // 2, 1) * sin_t).astype(BF16)


def norm_rope_back(d_final, raw, gain, cos_t, sin_t):
    raw = raw.astype(F32)
    inv = lax.rsqrt(jnp.mean(raw * raw, axis=-1, keepdims=True) + EPS)
    unit = raw * inv
    d_scaled = d_final * cos_t - pltpu.roll(d_final, HD // 2, 1) * sin_t
    d_gain = jnp.sum(d_scaled * unit, axis=0, keepdims=True)
    d_unit = d_scaled * (1.0 + gain)
    d_raw = inv * (d_unit - unit * jnp.mean(d_unit * unit, axis=-1, keepdims=True))
    return d_raw.astype(BF16), d_gain


def kv_kernel(x_ref, wpre_ref, wk_ref, wv_ref, kn_ref, cos_ref, sin_ref, first_ref, later_ref, kv_ref, kraw_ref):
    x = x_ref[...].astype(F32)
    inv = lax.rsqrt(jnp.mean(x * x, axis=-1, keepdims=True) + EPS)
    normed = (x * inv * (1.0 + wpre_ref[...])).astype(BF16)
    first = pl.program_id(0) == 0

    @pl.when(first)
    def _():
        first_ref[...] = normed

    @pl.when(jnp.logical_not(first))
    def _():
        later_ref[...] = normed

    k_raw = dot(normed, wk_ref[...]).astype(BF16)
    kraw_ref[...] = k_raw
    width = k_raw.shape[1]
    for h in range(width // HD):
        cols = slice(h * HD, (h + 1) * HD)
        kv_ref[:, cols] = norm_rope(k_raw[:, cols], kn_ref[...], cos_ref[...], sin_ref[...])
    kv_ref[:, width:] = dot(normed, wv_ref[...]).astype(BF16)


def parts_spec(rows, dim):
    return [pl.BlockSpec((rows, dim), lambda i: (0, 0)), pl.BlockSpec((rows, dim), lambda i: (jnp.maximum(i - 1, 0), 0))]


def project_kv(x, w_pre, w_k, w_v, k_norm, cos_t, sin_t, rows):
    seq, dim = x.shape
    width = w_k.shape[1]
    row = lambda n: pl.BlockSpec((rows, n), lambda i: (i, 0))
    return pl.pallas_call(
        kv_kernel,
        name="pkv",
        grid=(seq // rows,),
        in_specs=[row(dim), whole((1, dim)), fixed(w_k.shape), fixed(w_v.shape), whole((1, HD)), row(HD), row(HD)],
        out_specs=parts_spec(rows, dim) + [row(2 * width), row(width)],
        out_shape=[
            jax.ShapeDtypeStruct((rows, dim), BF16),
            jax.ShapeDtypeStruct((seq - rows, dim), BF16),
            jax.ShapeDtypeStruct((seq, 2 * width), BF16),
            jax.ShapeDtypeStruct((seq, width), BF16),
        ],
        compiler_params=params(1),
        cost_estimate=cost(4 * seq * dim * width, 4 * seq * dim + 4 * dim * width),
    )(x, w_pre, w_k, w_v, k_norm, cos_t, sin_t)


def q_kernel(first_ref, later_ref, wq_ref, qn_ref, cos_ref, sin_ref, qfin_ref, qraw_ref):
    normed = jnp.where(pl.program_id(0) == 0, first_ref[...], later_ref[...])
    q_raw = dot(normed, wq_ref[...]).astype(BF16)
    for h in range(qfin_ref.shape[0]):
        part = q_raw[:, h * HD:(h + 1) * HD]
        qraw_ref[h] = part
        qfin_ref[h] = norm_rope(part, qn_ref[...], cos_ref[...], sin_ref[...])


def project_q(first, later, w_q, q_norm, cos_t, sin_t):
    rows, dim = first.shape
    seq = rows + later.shape[0]
    heads = w_q.shape[1] // HD
    row = lambda n: pl.BlockSpec((rows, n), lambda i: (i, 0))
    head_rows = pl.BlockSpec((heads, rows, HD), lambda i: (0, i, 0))
    shape = jax.ShapeDtypeStruct((heads, seq, HD), BF16)
    return pl.pallas_call(
        q_kernel,
        name="pq",
        grid=(seq // rows,),
        in_specs=parts_spec(rows, dim) + [fixed(w_q.shape), whole((1, HD)), row(HD), row(HD)],
        out_specs=[head_rows, head_rows],
        out_shape=[shape, shape],
        compiler_params=params(1),
        cost_estimate=cost(2 * seq * dim * heads * HD, 2 * seq * dim + 2 * dim * heads * HD),
    )(first, later, w_q, q_norm, cos_t, sin_t)


def load_kv(kv_refs, k_buf, v_buf, sems, heads):
    kv_heads = kv_refs[0].shape[1] // (2 * HD)
    copies = []
    for s, ref in enumerate(kv_refs):
        for i, h in enumerate(heads):
            for t, buf in enumerate((k_buf, v_buf)):
                src = ref.at[:, pl.ds((t * kv_heads + h) * HD, HD)]
                copies.append(pltpu.make_async_copy(src, buf.at[i, s], sems.at[s, i, t]))
    for copy in copies:
        copy.start()
    for copy in copies:
        copy.wait()


def piece_place(piece, me, n_cp):
    upper = piece >= n_cp
    owner = jnp.where(upper, 2 * n_cp - 1 - piece, piece)
    return jnp.bitwise_xor(owner, me), upper.astype(jnp.int32)


def fwd_kernel(n_cp, me_ref, q_ref, *rest):
    kv_refs = rest[:n_cp]
    o_ref, lse_ref, k_buf, v_buf, m_scr, acc_scr, sems = rest[n_cp:]
    h, half = pl.program_id(0), pl.program_id(1)
    groups, rows, _ = q_ref.shape

    @pl.when((h == 0) & (half == 0))
    def _():
        load_kv(kv_refs, k_buf, v_buf, sems, range(k_buf.shape[0]))

    me = me_ref[0]
    piece = jnp.where(half == 0, me, 2 * n_cp - 1 - me)
    scale = HD ** -0.5 * LOG2E
    m_scr[...] = jnp.full(m_scr.shape, NEG_BIG, F32)
    acc_scr[...] = jnp.zeros(acc_scr.shape, F32)

    def block(j, masked):
        slot, upper = piece_place(j, me, n_cp)
        span = pl.ds(pl.multiple_of(upper * rows, rows), rows)
        k = k_buf[h, slot, span, :]
        v_ext = jnp.concatenate([v_buf[h, slot, span, :], jnp.ones((rows, HD), BF16)], axis=1)
        scores = [dot(q_ref[g], k, NT) * scale for g in range(groups)]
        for g in range(groups):
            s = scores[g]
            if masked:
                q_pos = lax.broadcasted_iota(jnp.int32, s.shape, 0)
                k_pos = lax.broadcasted_iota(jnp.int32, s.shape, 1)
                s = jnp.where(k_pos <= q_pos, s, NEG_BIG)
            m_old = m_scr[g]
            m_new = jnp.maximum(m_old, jnp.max(s, axis=1, keepdims=True))
            alpha = jnp.exp2(m_old - m_new)
            p = jnp.exp2(s - jnp.concatenate([m_new] * (rows // HD), axis=1)).astype(BF16)
            acc_scr[g] = acc_scr[g] * jnp.concatenate([alpha, alpha], axis=1) + dot(p, v_ext)
            m_scr[g] = m_new

    def full(j, carry):
        block(j, False)
        return carry

    lax.fori_loop(0, piece, full, 0)
    block(piece, True)
    for g in range(groups):
        l = acc_scr[g, :, HD:]
        o_ref[0, :, g * HD:(g + 1) * HD] = (acc_scr[g, :, :HD] / l).astype(BF16)
        lse_ref[0, g:g + 1, :] = jnp.transpose(m_scr[g] + jnp.log2(l))[0:1, :]


def attention_fwd(me, q_fin, kv_blocks, kv_heads):
    heads, seq, _ = q_fin.shape
    n_cp = len(kv_blocks)
    groups = heads // kv_heads
    rows = seq // 2
    grid_spec = pltpu.PrefetchScalarGridSpec(
        num_scalar_prefetch=1,
        grid=(kv_heads, 2),
        in_specs=[pl.BlockSpec((groups, rows, HD), lambda h, i, *_: (h, i, 0))] + [pl.BlockSpec(memory_space=pl.ANY)] * n_cp,
        out_specs=[
            pl.BlockSpec((1, rows, groups * HD), lambda h, i, *_: (i, 0, h)),
            pl.BlockSpec((1, 8, rows), lambda h, i, *_: (h, 0, i)),
        ],
        scratch_shapes=[
            pltpu.VMEM((kv_heads, n_cp, seq, HD), BF16),
            pltpu.VMEM((kv_heads, n_cp, seq, HD), BF16),
            pltpu.VMEM((groups, rows, HD), F32),
            pltpu.VMEM((groups, rows, 2 * HD), F32),
            pltpu.SemaphoreType.DMA((n_cp, kv_heads, 2)),
        ],
    )
    pairs = heads * rows * rows * (2 * n_cp + 1)
    return pl.pallas_call(
        functools.partial(fwd_kernel, n_cp),
        name="fwd",
        grid_spec=grid_spec,
        out_shape=[
            jax.ShapeDtypeStruct((2, rows, heads * HD), BF16),
            jax.ShapeDtypeStruct((kv_heads, 8, seq), F32),
        ],
        compiler_params=params(2),
        cost_estimate=cost(4 * pairs * HD, 8 * seq * heads * HD, pairs),
    )(me, q_fin, *kv_blocks)


def bwd_kernel(n_cp, half, me_ref, q_ref, do_ref, o_ref, lse_ref, qraw_ref, cos_ref, sin_ref, qn_ref, *rest):
    kv_refs, rest = rest[:n_cp], rest[n_cp:]
    if half:
        dq_ref, keep_ref, send_ref, low_ref, gain_ref = rest[:5]
    else:
        low_ref, dq_ref, keep_ref, send_ref, gain_ref = rest[:5]
    k_buf, v_buf, dq_scr, dkv_scr, sems = rest[5:]
    h = pl.program_id(0)
    groups, rows, _ = q_ref.shape
    two = n_cp // 2

    @pl.when(h == 0)
    def _():
        load_kv(kv_refs, k_buf, v_buf, sems, range(k_buf.shape[0]))
        gain_ref[...] = jnp.zeros(gain_ref.shape, F32)

    if half:
        dkv_scr[...] = jnp.zeros(dkv_scr.shape, F32)
    else:
        dkv_scr[...] = low_ref[:, :, 0]

    me = me_ref[0]
    piece = 2 * n_cp - 1 - me if half else me
    scale = HD ** -0.5
    delta = []
    for g in range(groups):
        prod = do_ref[g].astype(F32) * o_ref[0, :, g * HD:(g + 1) * HD].astype(F32)
        column = jnp.broadcast_to(jnp.sum(prod, axis=1, keepdims=True), (rows, HD))
        delta.append(jnp.transpose(column)[0:1, :])
    dq_scr[...] = jnp.zeros(dq_scr.shape, F32)

    def block(j, masked):
        slot, upper = piece_place(j, me, n_cp)
        span = pl.ds(pl.multiple_of(upper * rows, rows), rows)
        k = k_buf[h, slot, span, :]
        v = v_buf[h, slot, span, :]
        probs, d_scores = [], []
        for g in range(groups):
            s = dot(k, q_ref[g], NT)
            p = jnp.exp2(s * (scale * LOG2E) - lse_ref[0, g:g + 1, :])
            if masked:
                k_pos = lax.broadcasted_iota(jnp.int32, s.shape, 0)
                q_pos = lax.broadcasted_iota(jnp.int32, s.shape, 1)
                p = jnp.where(k_pos <= q_pos, p, 0.0)
            probs.append(p.astype(BF16))
            d_scores.append((p * (dot(v, do_ref[g], NT) - delta[g])).astype(BF16))
        for g in range(groups):
            dq_scr[g] += dot(d_scores[g], k, TN)
        index = (slot % 2) * two + slot // 2
        into = span if half else pl.ds(0, rows)
        d_all = jnp.concatenate(d_scores, axis=1)
        p_all = jnp.concatenate(probs, axis=1)
        dkv_scr[index, 0, into, :] += dot(d_all, q_ref[...].reshape(groups * rows, HD)) * scale
        dkv_scr[index, 1, into, :] += dot(p_all, do_ref[...].reshape(groups * rows, HD))

    def full(j, carry):
        block(j, False)
        return carry

    lax.fori_loop(0, piece, full, 0)
    block(piece, True)
    for g in range(groups):
        d_raw, d_gain = norm_rope_back(dq_scr[g] * scale, qraw_ref[g], qn_ref[...], cos_ref[...], sin_ref[...])
        dq_ref[:, g * HD:(g + 1) * HD] = d_raw
        gain_ref[0:1, :] += d_gain
    for i in range(two):
        own = slice(rows, 2 * rows) if half else slice(0, rows)
        keep_ref[i, :, 0] = dkv_scr[i, :, own]
        send_ref[i, :, 0] = dkv_scr[two + i, :, own]
    if half:
        low_ref[:, :, 0] = dkv_scr[:, :, :rows]


def attention_bwd(half, me, q_fin, d_out, out, lse, q_raw, cos_t, sin_t, q_norm, kv_blocks, kv_heads, low=None):
    heads, seq, _ = q_fin.shape
    n_cp = len(kv_blocks)
    groups = heads // kv_heads
    rows = seq // 2
    by_head = pl.BlockSpec((groups, rows, HD), lambda h, *_: (h, half, 0))
    table = pl.BlockSpec((rows, HD), lambda h, *_: (half, 0))
    by_owner = lambda n: pl.BlockSpec((n, 2, 1, rows, HD), lambda h, *_: (0, 0, h, 0, 0))
    grads = lambda n: jax.ShapeDtypeStruct((n, 2, kv_heads, rows, HD), F32)
    extra = () if low is None else (low,)
    carried = [n_cp] if half else []
    grid_spec = pltpu.PrefetchScalarGridSpec(
        num_scalar_prefetch=1,
        grid=(kv_heads,),
        in_specs=[
            by_head,
            pl.BlockSpec((groups, rows, HD), lambda h, *_: (h, 0, 0)),
            pl.BlockSpec((1, rows, groups * HD), lambda h, *_: (half, 0, h)),
            pl.BlockSpec((1, 8, rows), lambda h, *_: (h, 0, half)),
            by_head,
            table,
            table,
            whole((1, HD)),
        ]
        + [pl.BlockSpec(memory_space=pl.ANY)] * n_cp
        + [by_owner(n_cp)] * len(extra),
        out_specs=[
            pl.BlockSpec((rows, groups * HD), lambda h, *_: (0, h)),
            by_owner(n_cp // 2),
            by_owner(n_cp // 2),
            *map(by_owner, carried),
            whole((8, HD)),
        ],
        scratch_shapes=[
            pltpu.VMEM((kv_heads, n_cp, seq, HD), BF16),
            pltpu.VMEM((kv_heads, n_cp, seq, HD), BF16),
            pltpu.VMEM((groups, rows, HD), F32),
            pltpu.VMEM((n_cp, 2, seq if half else rows, HD), F32),
            pltpu.SemaphoreType.DMA((n_cp, kv_heads, 2)),
        ],
    )
    pairs = heads * rows * rows * (n_cp + 1)
    return pl.pallas_call(
        functools.partial(bwd_kernel, n_cp, half),
        grid_spec=grid_spec,
        out_shape=[
            jax.ShapeDtypeStruct((rows, heads * HD), BF16),
            grads(n_cp // 2),
            grads(n_cp // 2),
            *map(grads, carried),
            jax.ShapeDtypeStruct((8, HD), F32),
        ],
        compiler_params=params(1),
        cost_estimate=cost(10 * pairs * HD, 16 * seq * groups * HD, pairs),
    )(me, q_fin, d_out, out, lse, q_raw, cos_t, sin_t, q_norm, *kv_blocks, *extra)


def post_kernel(n_w, later, at_ref, o_ref, *rest):
    w_refs, rest = rest[:n_w], rest[n_w:]
    mine_ref, wmine_ref, x_ref, dy_ref, wpost_ref = rest[:5]
    y_ref, do_ref, give_ref, keep_ref, dpost_ref = rest[-13:-8]
    o_buf, w_buf, attn_scr, dattn_scr, o_sem, w_sem, sum_sem, _ = rest[-8:]
    i = pl.program_id(0)
    n_tp, _, width = o_ref.shape
    rows, dim = x_ref.shape
    cols = attn_scr.shape[2]
    sums = [pltpu.make_async_copy(rest[5 + j], (give_ref, keep_ref)[j], sum_sem.at[j]) for j in range(2)] if later else []

    def weight_copy(s, par):
        return pltpu.make_async_copy(w_refs[s], w_buf.at[par], w_sem.at[par])

    @pl.when(i == 0)
    def _():
        copies = [
            pltpu.make_async_copy(o_ref.at[t], o_buf.at[:, pl.ds(t * width, width)], o_sem.at[t]) for t in range(n_tp)
        ]
        for copy in copies:
            copy.start()
        weight_copy(0, 0).start()
        for copy in sums:
            copy.start()
        for copy in copies:
            copy.wait()

    for s in range(1, n_w):

        @pl.when(i == s - 1)
        def _():
            weight_copy(s, s % 2).start()

    @pl.when(i < n_w)
    def _():
        par = lax.rem(i, 2)
        weight_copy(0, par).wait()
        attn_scr[jnp.bitwise_xor(at_ref[0], i)] = dot(o_buf[...], w_buf[par])

    @pl.when(i == n_w)
    def _():
        dpost_ref[...] = jnp.zeros(dpost_ref.shape, F32)
        if later:
            for copy in sums:
                copy.wait()
        else:
            give_ref[...] = jnp.zeros(give_ref.shape, F32)
            keep_ref[...] = jnp.zeros(keep_ref.shape, F32)

    @pl.when(i >= n_w)
    def _():
        tiles = [(s, t * HD, slice(s * cols + t * HD, s * cols + (t + 1) * HD)) for s in range(n_w) for t in range(cols // HD)]
        sub = 64

        def some_rows(r, carry):
            here = pl.ds(pl.multiple_of(r * sub, sub), sub)
            there = pl.ds(pl.multiple_of((i - n_w) * rows + r * sub, sub), sub)
            square = jnp.zeros((sub, HD), F32)
            cross = jnp.zeros((sub, HD), F32)
            for s, t, at in tiles:
                attn = attn_scr[s, there, t:t + HD]
                square += attn * attn
                cross += attn * (dy_ref[here, at].astype(F32) * (1.0 + wpost_ref[:, at]))
            inv = lax.rsqrt(jnp.sum(square, axis=1, keepdims=True) * (1.0 / dim) + EPS)
            shrink = inv * inv * inv * (jnp.sum(cross, axis=1, keepdims=True) * (1.0 / dim))
            for s, t, at in tiles:
                attn = attn_scr[s, there, t:t + HD]
                gain = 1.0 + wpost_ref[:, at]
                dy = dy_ref[here, at].astype(F32)
                unit = attn * inv
                y_ref[here, at] = (x_ref[here, at].astype(F32) + unit * gain).astype(BF16)
                dpost_ref[:, at] += jnp.sum((dy * unit).reshape(sub // 8, 8, HD), axis=0)
                dattn_scr[here, at] = (inv * (dy * gain) - attn * shrink).astype(BF16)
            return carry

        lax.fori_loop(0, rows // sub, some_rows, 0)
        d_attn = dattn_scr[...]
        d_out = dot(d_attn, wmine_ref[...], NT)
        for h in range(do_ref.shape[0]):
            do_ref[h] = d_out[:, h * HD:(h + 1) * HD].astype(BF16)
        half = give_ref.shape[0]
        core = at_ref[1]
        give_ref[...] += dot(mine_ref[0, :, pl.ds(pl.multiple_of((1 - core) * half, HD), half)], d_attn, TN)
        keep_ref[...] += dot(mine_ref[0, :, pl.ds(pl.multiple_of(core * half, HD), half)], d_attn, TN)


def post(half, at, out_all, w_all, out, w_mine, x, dy, w_post, before=None):
    n_tp, chunk, width = out_all.shape
    seq, dim = x.shape
    rows = min(256, chunk)
    heads = width // HD
    n_w = len(w_all)
    n = chunk // rows
    block = lambda i: jnp.maximum(i - n_w, 0)
    row = lambda cols: pl.BlockSpec((rows, cols), lambda i, *_: (half * n + block(i), 0))
    anywhere = pl.BlockSpec(memory_space=pl.ANY)
    sums = jax.ShapeDtypeStruct((width // 2, dim), F32)
    extra = () if before is None else tuple(before)
    grid_spec = pltpu.PrefetchScalarGridSpec(
        num_scalar_prefetch=1,
        grid=(n_w + n,),
        in_specs=[anywhere] * (1 + n_w)
        + [pl.BlockSpec((1, rows, width), lambda i, *_: (half, block(i), 0))]
        + [fixed(w_mine.shape), row(dim), row(dim), whole((1, dim))]
        + [anywhere] * len(extra),
        out_specs=[
            row(dim),
            pl.BlockSpec((heads, rows, HD), lambda i, *_: (0, block(i), 0)),
            fixed(sums.shape),
            fixed(sums.shape),
            whole((8, dim)),
        ],
        scratch_shapes=[
            pltpu.VMEM((chunk, n_tp * width), BF16),
            pltpu.VMEM((2, n_tp * width, dim // n_w), BF16),
            pltpu.VMEM((n_w, chunk, dim // n_w), F32),
            pltpu.VMEM((rows, dim), BF16),
            pltpu.SemaphoreType.DMA((n_tp,)),
            pltpu.SemaphoreType.DMA((2,)),
            pltpu.SemaphoreType.DMA((2,)),
            pltpu.SemaphoreType.DMA((1,)),
        ],
    )
    return pl.pallas_call(
        functools.partial(post_kernel, n_w, bool(extra)),
        grid_spec=grid_spec,
        out_shape=[
            jax.ShapeDtypeStruct((seq, dim), BF16),
            jax.ShapeDtypeStruct((heads, chunk, HD), BF16),
            sums,
            sums,
            jax.ShapeDtypeStruct((8, dim), F32),
        ],
        input_output_aliases={7 + n_w + 2: 0} if extra else {},
        compiler_params=params(1, VMEM_TOP),
        cost_estimate=cost(2 * chunk * dim * width * (n_tp + 2), 8 * chunk * dim + 2 * dim * width * (n_tp + 1)),
    )(at, out_all, *w_all, out, w_mine, x, dy, w_post, *extra)


def kback_kernel(own_ref, near_ref, far_ref, kraw_ref, cos_ref, sin_ref, kn_ref, out_ref, gain_ref):
    @pl.when(pl.program_id(0) == 0)
    def _():
        gain_ref[...] = jnp.zeros(gain_ref.shape, F32)

    kv_heads = own_ref.shape[2]
    for h in range(kv_heads):
        cols = slice(h * HD, (h + 1) * HD)
        d_k = own_ref[0, 0, h] + near_ref[0, 0, h] + far_ref[0, h]
        d_raw, d_gain = norm_rope_back(d_k, kraw_ref[:, cols], kn_ref[...], cos_ref[...], sin_ref[...])
        out_ref[:, cols] = d_raw
        gain_ref[0:1, :] += d_gain
        d_v = own_ref[0, 1, h] + near_ref[0, 1, h] + far_ref[1, h]
        out_ref[:, (kv_heads + h) * HD:(kv_heads + h + 1) * HD] = d_v.astype(BF16)


def key_back(half, own, near, far, k_raw, cos_t, sin_t, k_norm):
    _, _, kv_heads, chunk, _ = own.shape
    rows = min(256, chunk)
    n = chunk // rows
    two = pl.BlockSpec((1, 2, kv_heads, rows, HD), lambda i: (0, 0, 0, i, 0))
    row = lambda cols: pl.BlockSpec((rows, cols), lambda i: (half * n + i, 0))
    return pl.pallas_call(
        kback_kernel,
        grid=(n,),
        in_specs=[
            two,
            two,
            pl.BlockSpec((2, kv_heads, rows, HD), lambda i: (0, 0, i, 0)),
            row(kv_heads * HD),
            row(HD),
            row(HD),
            whole((1, HD)),
        ],
        out_specs=[pl.BlockSpec((rows, 2 * kv_heads * HD), lambda i: (i, 0)), whole((8, HD))],
        out_shape=[
            jax.ShapeDtypeStruct((chunk, 2 * kv_heads * HD), BF16),
            jax.ShapeDtypeStruct((8, HD), F32),
        ],
        compiler_params=params(1),
        cost_estimate=cost(50 * chunk * kv_heads * HD, 12 * chunk * kv_heads * HD),
    )(own, near, far, k_raw, cos_t, sin_t, k_norm)


def dx_kernel(n_tp, tp_ref, *refs):
    g_refs, refs = refs[:2 * n_tp], refs[2 * n_tp:]
    w_refs, x_refs, dy_refs, wpre_ref = refs[0:2], refs[2:4], refs[4:6], refs[6]
    dx_ref, dpre_ref, g_scr, acc = refs[7:]
    i = pl.program_id(0)
    rows = g_refs[0].shape[0]

    @pl.when(i == 0)
    def _():
        for s in range(n_tp):
            t = lax.rem(tp_ref[0] + n_tp - s, n_tp)
            for half in range(2):
                g_scr[t, half * rows:(half + 1) * rows, :] = g_refs[half * n_tp + s][...]

    start = 0
    for w_ref in w_refs:
        shares, cols = w_ref.shape[1:3]
        for j in range(shares):
            total = dot(g_scr[0], w_ref[0, j], NT)
            for t in range(1, n_tp):
                total += dot(g_scr[t], w_ref[t, j], NT)
            acc[i * shares + j, :, start:start + cols] = total
        start += cols

    @pl.when(i == pl.num_programs(0) - 1)
    def _():
        dpre_ref[...] = jnp.zeros(dpre_ref.shape, F32)
        n, _, width = acc.shape
        tiles = [(s, t, slice(s * width + t, s * width + t + HD)) for s in range(n) for t in range(0, width, HD)]
        dim = n * width
        sub = min(64, rows)
        for half in range(2):
            x_ref, dy_ref = x_refs[half], dy_refs[half]

            def some_rows(r, carry):
                here = pl.ds(pl.multiple_of(r * sub, sub), sub)
                there = pl.ds(pl.multiple_of(half * rows + r * sub, sub), sub)
                square = jnp.zeros((sub, HD), F32)
                cross = jnp.zeros((sub, HD), F32)
                for s, t, at in tiles:
                    x = x_ref[here, at].astype(F32)
                    square += x * x
                    cross += x * (acc[s, there, t:t + HD] * (1.0 + wpre_ref[:, at]))
                inv = lax.rsqrt(jnp.sum(square, axis=1, keepdims=True) * (1.0 / dim) + EPS)
                shrink = inv * inv * inv * (jnp.sum(cross, axis=1, keepdims=True) * (1.0 / dim))
                for s, t, at in tiles:
                    x = x_ref[here, at].astype(F32)
                    d_normed = acc[s, there, t:t + HD]
                    dpre_ref[:, at] += jnp.sum((d_normed * (x * inv)).reshape(sub // 8, 8, HD), axis=0)
                    d_x = inv * (d_normed * (1.0 + wpre_ref[:, at])) - x * shrink
                    dx_ref[there, at] = (dy_ref[here, at].astype(F32) + d_x).astype(BF16)
                return carry

            lax.fori_loop(0, rows // sub, some_rows, 0)


def input_grad(tp, grads, w_all, x, dy, w_pre, shares=2):
    n_tp = len(grads) // 2
    rows, width = grads[0].shape
    dim = x.shape[1]
    n = w_all[0].shape[1]
    cols = dim // n
    here = lambda half: pl.BlockSpec((rows, dim), lambda i, t: (half * n_tp + t[0], 0))
    grid_spec = pltpu.PrefetchScalarGridSpec(
        num_scalar_prefetch=1,
        grid=(n // shares,),
        in_specs=[whole((rows, width))] * (2 * n_tp)
        + [pl.BlockSpec((n_tp, shares, w.shape[2], width), lambda i, *_: (0, i, 0, 0)) for w in w_all]
        + [here(0), here(1), here(0), here(1), whole((1, dim))],
        out_specs=[whole((2 * rows, dim)), whole((8, dim))],
        scratch_shapes=[pltpu.VMEM((n_tp, 2 * rows, width), BF16), pltpu.VMEM((n, 2 * rows, cols), F32)],
    )
    return pl.pallas_call(
        functools.partial(dx_kernel, n_tp),
        name="dx",
        grid_spec=grid_spec,
        out_shape=[jax.ShapeDtypeStruct((2 * rows, dim), BF16), jax.ShapeDtypeStruct((8, dim), F32)],
        compiler_params=params(1),
        cost_estimate=cost(4 * n_tp * rows * width * dim, 2 * n_tp * width * dim),
    )(tp, *grads, *w_all, x, x, dy, dy, w_pre)


def dw_kernel(n_cp, me_ref, *refs):
    g_refs, n_refs = refs[:2 * n_cp], refs[2 * n_cp:-7]
    dwq_ref, dwk_ref, dwv_ref, n_buf, g_buf, n_sem, g_sem = refs[-7:]
    i = pl.program_id(0)
    cols = n_buf.shape[3]
    chunk, width = g_refs[0].shape
    me = me_ref[0]

    def place(refs_in, buf, sem):
        copies = []
        for j, (ref, shape) in enumerate(refs_in):
            start = sum(r[1] for r in refs_in[:j - j % n_cp:n_cp])
            to = buf.at[jnp.bitwise_xor(me, j % n_cp), pl.ds(start, shape)]
            copies.append(pltpu.make_async_copy(ref, to, sem.at[j]))
        return copies

    def fetch(step, par):
        span = pl.ds(pl.multiple_of(step * cols, cols), cols)
        return place([(r.at[:, span], r.shape[0]) for r in n_refs], n_buf.at[par], n_sem.at[par])

    @pl.when(i == 0)
    def _():
        grads = place([(r, chunk) for r in g_refs], g_buf, g_sem)
        for copy in fetch(0, 0) + grads:
            copy.start()
        for copy in grads:
            copy.wait()

    @pl.when(i + 1 < pl.num_programs(0))
    def _():
        for copy in fetch(i + 1, (i + 1) % 2):
            copy.start()

    for copy in fetch(i, i % 2):
        copy.wait()
    seq = 2 * chunk
    grad = dot(n_buf[i % 2].reshape(n_cp * seq, cols), g_buf[...].reshape(n_cp * seq, width), TN)
    q_width, kv_width = dwq_ref.shape[1], dwk_ref.shape[1]
    dwq_ref[...] = grad[:, :q_width]
    dwk_ref[...] = grad[:, q_width:q_width + kv_width]
    dwv_ref[...] = grad[:, q_width + kv_width:]


def weight_grads(me, normed, grads, q_width, cols=256):
    n_cp = len(grads) // 2
    chunk, width = grads[0].shape
    dim = normed[0].shape[1]
    kv_width = (width - q_width) // 2
    anywhere = pl.BlockSpec(memory_space=pl.ANY)
    tile = lambda n: pl.BlockSpec((cols, n), lambda i, *_: (i, 0))
    grid_spec = pltpu.PrefetchScalarGridSpec(
        num_scalar_prefetch=1,
        grid=(dim // cols,),
        in_specs=[anywhere] * (len(grads) + len(normed)),
        out_specs=[tile(q_width), tile(kv_width), tile(kv_width)],
        scratch_shapes=[
            pltpu.VMEM((2, n_cp, 2 * chunk, cols), BF16),
            pltpu.VMEM((n_cp, 2 * chunk, width), BF16),
            pltpu.SemaphoreType.DMA((2, len(normed))),
            pltpu.SemaphoreType.DMA((len(grads),)),
        ],
    )
    return pl.pallas_call(
        functools.partial(dw_kernel, n_cp),
        name="dw",
        grid_spec=grid_spec,
        out_shape=[jax.ShapeDtypeStruct((dim, n), F32) for n in (q_width, kv_width, kv_width)],
        compiler_params=params(1),
        cost_estimate=cost(4 * n_cp * chunk * dim * width, 4 * n_cp * chunk * (dim + width)),
    )(me, *grads, *normed)


def join_kernel(core_ref, keep_ref, other_ref, *rest):
    half = pl.program_id(0)

    @pl.when(half == core_ref[0])
    def _():
        rest[-1][...] = keep_ref[...]

    @pl.when(half != core_ref[0])
    def _():
        rest[-1][...] = other_ref[...]


def join_halves(core, keep, other, start, half, total=None):
    block, width = HD, keep.shape[1]
    n = keep.shape[0] // block
    extra = () if total is None else (total,)
    part = pl.BlockSpec((block, width), lambda i, j, c: (j, 0))
    grid_spec = pltpu.PrefetchScalarGridSpec(
        num_scalar_prefetch=1,
        grid=(2, n),
        in_specs=[part, part] + [pl.BlockSpec(memory_space=pl.ANY)] * len(extra),
        out_specs=pl.BlockSpec((block, width), lambda i, j, c: (i * (half // block) + start // block + j, 0)),
    )
    return pl.pallas_call(
        join_kernel,
        name="join",
        grid_spec=grid_spec,
        out_shape=jax.ShapeDtypeStruct((2 * half, width), F32),
        input_output_aliases={3: 0} if extra else {},
        compiler_params=params(2),
        cost_estimate=cost(n * block * width, 16 * n * block * width),
    )(core, keep, other, *extra)


def solution(mesh):
    n_cp, n_tp, n_dp = mesh.shape["cp"], mesh.shape["tp"], mesh.shape["dp"]
    near = [(i, i ^ 1) for i in range(n_cp)]
    across = [(i, i ^ 2) for i in range(n_cp)]
    beside = [(i, i ^ 1) for i in range(n_dp)]

    def from_cp(value):
        far = lax.ppermute(value, "cp", across)
        return [value, lax.ppermute(value, "cp", near), far, lax.ppermute(far, "cp", near)]

    def per_device(hidden, cotangent, pos_loc, w_q, w_k, w_v, w_o, w_pre, w_post, q_norm, k_norm):
        _, seq, dim = hidden.shape
        x, dy = hidden[0], cotangent[0]
        kv_heads = w_k.shape[1] // HD
        cp, tp, dp = (lax.axis_index(a).astype(jnp.int32) for a in ("cp", "tp", "dp"))
        core = cp % 2
        me, one_tp, one_core = cp.reshape(1), tp.reshape(1), core.reshape(1)

        share = dp * n_cp + cp
        shares = n_dp * n_cp
        cols = dim // shares
        mine = lax.all_gather(lax.dynamic_slice_in_dim(w_o, share * cols, cols, 1), "tp", axis=0, tiled=True)
        w_o_all = from_cp(mine)
        if n_dp == 2:
            own, far = lax.ppermute(mine, "dp", beside), lax.ppermute(w_o_all[2], "dp", beside)
            w_o_all += [own, lax.ppermute(own, "cp", near), far, lax.ppermute(far, "cp", near)]

        cos_t, sin_t = rope_tables(pos_loc)
        qn, kn = q_norm.reshape(1, HD), k_norm.reshape(1, HD)
        wpre, wpost = w_pre.reshape(1, dim), w_post.reshape(1, dim)
        first, later, kv_own, k_raw = project_kv(x, wpre, w_k, w_v, kn, cos_t, sin_t, seq // 4)
        kv_blocks = from_cp(kv_own)
        q_fin, q_raw = project_q(first, later, w_q, qn, cos_t, sin_t)
        normed_all = from_cp(first) + from_cp(later)
        out, lse = attention_fwd(me, q_fin, kv_blocks, kv_heads)

        w_rows = dim // shares
        third = w_rows // 3 // HD * HD or w_rows // 2

        def gather_w(start, stop):
            parts = [lax.dynamic_slice_in_dim(w, share * w_rows + start, stop - start, 0) for w in (w_q, w_k, w_v)]
            parts = jnp.concatenate(parts, axis=1)
            whole_w = lax.all_gather(parts, ("tp", "dp", "cp"), axis=0, tiled=True)
            return whole_w.reshape(n_tp, shares, stop - start, parts.shape[1])

        w_a = gather_w(0, third)
        out_sent, _ = lax.optimization_barrier((out, mine))
        out_all = [None, None]
        for half in (1, 0):
            out_all[half] = lax.all_gather(out_sent[half], "tp", axis=0, tiled=False)
        w_b = gather_w(third, w_rows)

        at = jnp.stack([share, core])
        done, low, dq, d_post, gains, carried = None, [], [None] * 2, [], [], [None] * 2
        for half in (1, 0):
            y, d_out, give, keep, part = post(half, at, out_all[half], w_o_all, out, w_o, x, dy, wpost, done)
            done = (give, keep, y)
            d_post.append(part)
            dq[half], kept, sent, *low, gain = attention_bwd(
                half, me, q_fin, d_out, out, lse, q_raw, cos_t, sin_t, qn, kv_blocks, kv_heads, *low
            )
            gains.append(gain[0])
            got = lax.ppermute(sent, "cp", near)
            carried[half] = (kept, got, lax.ppermute(kept[1] + got[1], "cp", across))

        got = lax.ppermute(give, "cp", near)
        rows = keep.shape[0]
        d_wo = None
        for start, stop in ((0, rows - HD), (rows - HD, rows)):
            mine_part = keep[start:stop] + got[start:stop]
            mine_part = mine_part + lax.ppermute(mine_part, "cp", across)
            other = lax.ppermute(mine_part, "cp", near)
            d_wo = join_halves(one_core, mine_part, other, start, rows, d_wo)

        rows = seq // 2 // n_tp
        grads, pieces = [], [None] * 2
        for half in (1, 0):
            d_kv, gain = key_back(half, *carried[half], k_raw, cos_t, sin_t, kn)
            gains.append(gain[0])
            g = jnp.concatenate([dq[half], d_kv], axis=1)
            pieces[half] = [lax.dynamic_slice_in_dim(g, tp * rows, rows, 0)]
            for s in range(1, n_tp):
                part = lax.dynamic_slice_in_dim(g, ((tp + s) % n_tp) * rows, rows, 0)
                pieces[half].append(lax.ppermute(part, "tp", [(i, (i + s) % n_tp) for i in range(n_tp)]))
            grads.append(g)
        dx_rows, d_pre = input_grad(one_tp, pieces[0] + pieces[1], (w_a, w_b), x, dy, wpre)
        d_hidden = lax.all_gather(dx_rows, "tp", axis=0, tiled=False)
        d_hidden = d_hidden.reshape(n_tp, 2, rows, dim).transpose(1, 0, 2, 3).reshape(seq, dim)

        grads_all = from_cp(grads[1]) + from_cp(grads[0])
        d_wq, d_wk, d_wv = weight_grads(me, normed_all, grads_all, w_q.shape[1])

        d_post = jnp.sum(d_post[0] + d_post[1], axis=0)
        small = jnp.concatenate([jnp.where(tp == 0, d_post, 0.0), jnp.sum(d_pre, axis=0), gains[0] + gains[1], gains[2] + gains[3]])
        small = small + lax.ppermute(small, "cp", near)
        small = small + lax.ppermute(small, "cp", across)
        small = small + lax.ppermute(small, "tp", [(i, i ^ 1) for i in range(n_tp)])
        small = small + lax.ppermute(small, "tp", [(i, i ^ 2) for i in range(n_tp)])
        d_post, d_pre = small[:dim], small[dim:2 * dim]
        d_qn, d_kn = small[2 * dim:2 * dim + HD], small[2 * dim + HD:]
        return y[None], d_hidden[None], d_wq, d_wk, d_wv, d_wo, d_pre, d_post, d_qn, d_kn

    specs_in = (P('dp', 'cp', None), P('dp', 'cp', None), P(('dp', 'cp')), P(None, 'tp'), P(None, 'tp'), P(None, 'tp'), P('tp', None), P(None), P(None), P(None), P(None))
    specs_out = (P('dp', 'cp', None), P('dp', 'cp', None), P('dp', 'tp'), P('dp', 'tp'), P('dp', 'tp'), P(('dp', 'tp'), None), P('dp'), P('dp'), P('dp'), P('dp'))
    return jax.shard_map(per_device, mesh=mesh, in_specs=specs_in, out_specs=specs_out, check_vma=False)
```

```python
import functools

import jax
import jax.numpy as jnp
import numpy as np
from jax import lax
from jax.experimental import pallas as pl
from jax.experimental.pallas import tpu as pltpu
from jax.sharding import PartitionSpec as P


EPS = 1e-6
ROPE_BASE = 1000000.0
ROPE_SCALE = 8.0
NEG_BIG = -1e30
LOG2E = 1.4426950408889634
HD = 128
F32 = jnp.float32
BF16 = jnp.bfloat16
VMEM_MAX = 62914560
VMEM_TOP = 67043328
NT = (((1,), (1,)), ((), ()))
TN = (((0,), (0,)), ((), ()))


def dot(a, b, dims=(((1,), (0,)), ((), ()))):
    return lax.dot_general(a, b, dims, preferred_element_type=F32)


def params(dims, vmem=VMEM_MAX):
    return pltpu.CompilerParams(dimension_semantics=("arbitrary",) * dims, vmem_limit_bytes=vmem)


def cost(products, values, trans=0):
    return pl.CostEstimate(flops=2 * products, bytes_accessed=2 * values, transcendentals=trans)


def row_sum(values):
    return jnp.sum(values, axis=1, keepdims=True)


def inv_rms(square, dim):
    return lax.rsqrt(row_sum(square) * (1.0 / dim) + EPS)


def whole(shape):
    return pl.BlockSpec(shape, lambda *_: (0,) * len(shape))


def fixed(shape):
    return pl.BlockSpec(shape, lambda *_: (0,) * len(shape), pipeline_mode=pl.Buffered(buffer_count=1))


def rows_of(rows, cols, at=lambda i: i):
    return pl.BlockSpec((rows, cols), lambda i, *_: (at(i), 0))


def anywhere(n):
    return [pl.BlockSpec(memory_space=pl.ANY)] * n


def like(shape, dtype):
    return jax.ShapeDtypeStruct(shape, dtype)


def rope_tables(pos_loc):
    half_dim = HD // 2
    inv_freq = 1.0 / (ROPE_SCALE * ROPE_BASE ** (jnp.arange(half_dim, dtype=F32) * (2.0 / HD)))
    angles = pos_loc.astype(F32)[:, None] * inv_freq[None, :]
    cos_t, sin_t = jnp.cos(angles), jnp.sin(angles)
    return jnp.concatenate([cos_t, cos_t], axis=-1), jnp.concatenate([-sin_t, sin_t], axis=-1)


def norm_rope(raw, gain, cos_t, sin_t):
    raw = raw.astype(F32)
    unit = raw * inv_rms(raw * raw, HD)
    scaled = unit * (1.0 + gain)
    return (scaled * cos_t + pltpu.roll(scaled, HD // 2, 1) * sin_t).astype(BF16)


def norm_rope_back(d_final, raw, gain, cos_t, sin_t):
    raw = raw.astype(F32)
    inv = inv_rms(raw * raw, HD)
    unit = raw * inv
    d_scaled = d_final * cos_t - pltpu.roll(d_final, HD // 2, 1) * sin_t
    d_gain = jnp.sum(d_scaled * unit, axis=0, keepdims=True)
    d_unit = d_scaled * (1.0 + gain)
    d_raw = inv * (d_unit - unit * (row_sum(d_unit * unit) * (1.0 / HD)))
    return d_raw.astype(BF16), d_gain


def kv_kernel(x_ref, wpre_ref, wk_ref, wv_ref, kn_ref, cos_ref, sin_ref, first_ref, later_ref, kv_ref, kraw_ref, buf, sem):
    i = pl.program_id(0)
    rows, dim = x_ref.shape
    par = i % 2

    def first_copy():
        return pltpu.make_async_copy(buf.at[0], first_ref, sem.at[0])

    def later_copy(step):
        to = later_ref.at[pl.ds(pl.multiple_of((step - 1) * rows, rows), rows)]
        return pltpu.make_async_copy(buf.at[step % 2], to, sem.at[step % 2])

    @pl.when(i == 2)
    def _():
        first_copy().wait()

    @pl.when(i > 2)
    def _():
        later_copy(i - 2).wait()

    tiles = [slice(t, t + HD) for t in range(0, dim, HD)]
    sub = min(64, rows)

    def some_rows(r, carry):
        here = pl.ds(pl.multiple_of(r * sub, sub), sub)
        square = jnp.zeros((sub, HD), F32)
        for at in tiles:
            x = x_ref[here, at].astype(F32)
            square += x * x
        inv = inv_rms(square, dim)
        for at in tiles:
            buf[par, here, at] = (x_ref[here, at].astype(F32) * inv * (1.0 + wpre_ref[:, at])).astype(BF16)
        return carry

    lax.fori_loop(0, rows // sub, some_rows, 0)

    @pl.when(i == 0)
    def _():
        first_copy().start()

    @pl.when(i > 0)
    def _():
        later_copy(i).start()

    normed = buf[par]
    k_raw = dot(normed, wk_ref[:]).astype(BF16)
    kraw_ref[:] = k_raw
    width = k_raw.shape[1]
    for h in range(width // HD):
        cols = slice(h * HD, (h + 1) * HD)
        kv_ref[:, cols] = norm_rope(k_raw[:, cols], kn_ref[:], cos_ref[:], sin_ref[:])
    kv_ref[:, width:] = dot(normed, wv_ref[:]).astype(BF16)

    @pl.when(i == pl.num_programs(0) - 1)
    def _():
        later_copy(i - 1).wait()
        later_copy(i).wait()


def project_kv(x, w_pre, w_k, w_v, k_norm, cos_t, sin_t, rows):
    seq, dim = x.shape
    width = w_k.shape[1]
    grid_spec = pl.GridSpec(
        grid=(seq // rows,),
        in_specs=[rows_of(rows, dim), whole((1, dim)), fixed(w_k.shape), fixed(w_v.shape), whole((1, HD))]
        + [rows_of(rows, HD)] * 2,
        out_specs=anywhere(2) + [rows_of(rows, 2 * width), rows_of(rows, width)],
        scratch_shapes=[pltpu.VMEM((2, rows, dim), BF16), pltpu.SemaphoreType.DMA((2,))],
    )
    return pl.pallas_call(
        kv_kernel,
        name="pkv",
        grid_spec=grid_spec,
        out_shape=[like((rows, dim), BF16), like((seq - rows, dim), BF16), like((seq, 2 * width), BF16), like((seq, width), BF16)],
        compiler_params=params(1),
        cost_estimate=cost(2 * seq * dim * width, 2 * dim * (seq + width)),
    )(x, w_pre, w_k, w_v, k_norm, cos_t, sin_t)


def q_kernel(first_ref, later_ref, wq_ref, qn_ref, cos_ref, sin_ref, qfin_ref, qraw_ref):
    normed = jnp.where(pl.program_id(0) == 0, first_ref[:], later_ref[:])
    q_raw = dot(normed, wq_ref[:]).astype(BF16)
    for h in range(qfin_ref.shape[0]):
        part = q_raw[:, h * HD:(h + 1) * HD]
        qraw_ref[h] = part
        qfin_ref[h] = norm_rope(part, qn_ref[:], cos_ref[:], sin_ref[:])


def project_q(first, later, w_q, q_norm, cos_t, sin_t):
    rows, dim = first.shape
    seq = rows + later.shape[0]
    heads = w_q.shape[1] // HD
    head_rows = pl.BlockSpec((heads, rows, HD), lambda i: (0, i, 0))
    shape = like((heads, seq, HD), BF16)
    return pl.pallas_call(
        q_kernel,
        name="pq",
        grid=(seq // rows,),
        in_specs=[whole((rows, dim)), rows_of(rows, dim, lambda i: jnp.maximum(i - 1, 0)), fixed(w_q.shape), whole((1, HD))]
        + [rows_of(rows, HD)] * 2,
        out_specs=[head_rows, head_rows],
        out_shape=[shape, shape],
        compiler_params=params(1),
        cost_estimate=cost(seq * dim * heads * HD, dim * (seq + heads * HD)),
    )(first, later, w_q, q_norm, cos_t, sin_t)


def load_kv(kv_refs, k_buf, v_buf, sems, heads):
    kv_heads = kv_refs[0].shape[1] // (2 * HD)
    copies = []
    for s, ref in enumerate(kv_refs):
        for i, h in enumerate(heads):
            for t, buf in enumerate((k_buf, v_buf)):
                src = ref.at[:, pl.ds((t * kv_heads + h) * HD, HD)]
                copies.append(pltpu.make_async_copy(src, buf.at[i, s], sems.at[s, i, t]))
    for copy in copies:
        copy.start()
    for copy in copies:
        copy.wait()


def piece_place(piece, me, n_cp):
    upper = piece >= n_cp
    owner = jnp.where(upper, 2 * n_cp - 1 - piece, piece)
    return jnp.bitwise_xor(owner, me), upper.astype(jnp.int32)


def fwd_kernel(n_cp, me_ref, q_ref, *rest):
    kv_refs = rest[:n_cp]
    o_ref, lse_ref, k_buf, v_buf, m_scr, acc_scr, sems = rest[n_cp:]
    h, half = pl.program_id(0), pl.program_id(1)
    groups, rows, _ = q_ref.shape

    @pl.when((h == 0) & (half == 0))
    def _():
        load_kv(kv_refs, k_buf, v_buf, sems, range(k_buf.shape[0]))

    me = me_ref[0]
    piece = jnp.where(half == 0, me, 2 * n_cp - 1 - me)
    scale = HD ** -0.5 * LOG2E
    m_scr[:] = jnp.full(m_scr.shape, NEG_BIG, F32)
    acc_scr[:] = jnp.zeros(acc_scr.shape, F32)

    def block(j, masked):
        slot, upper = piece_place(j, me, n_cp)
        span = pl.ds(pl.multiple_of(upper * rows, rows), rows)
        k = k_buf[h, slot, span, :]
        v_ext = jnp.concatenate([v_buf[h, slot, span, :], jnp.ones((rows, HD), BF16)], axis=1)
        scores = [dot(q_ref[g], k, NT) * scale for g in range(groups)]
        for g in range(groups):
            s = scores[g]
            if masked:
                q_pos = lax.broadcasted_iota(jnp.int32, s.shape, 0)
                k_pos = lax.broadcasted_iota(jnp.int32, s.shape, 1)
                s = jnp.where(k_pos <= q_pos, s, NEG_BIG)
            m_old = m_scr[g]
            m_new = jnp.maximum(m_old, jnp.max(s, axis=1, keepdims=True))
            alpha = jnp.exp2(m_old - m_new)
            p = jnp.exp2(s - jnp.concatenate([m_new] * (rows // HD), axis=1)).astype(BF16)
            acc_scr[g] = acc_scr[g] * jnp.concatenate([alpha, alpha], axis=1) + dot(p, v_ext)
            m_scr[g] = m_new

    def full(j, carry):
        block(j, False)
        return carry

    lax.fori_loop(0, piece, full, 0)
    block(piece, True)
    for g in range(groups):
        l = acc_scr[g, :, HD:]
        o_ref[0, :, g * HD:(g + 1) * HD] = (acc_scr[g, :, :HD] / l).astype(BF16)
        lse_ref[0, g:g + 1, :] = jnp.transpose(m_scr[g] + jnp.log2(l))[0:1, :]


def attention_fwd(me, q_fin, kv_blocks, kv_heads):
    heads, seq, _ = q_fin.shape
    n_cp = len(kv_blocks)
    groups = heads // kv_heads
    rows = seq // 2
    grid_spec = pltpu.PrefetchScalarGridSpec(
        num_scalar_prefetch=1,
        grid=(kv_heads, 2),
        in_specs=[pl.BlockSpec((groups, rows, HD), lambda h, i, *_: (h, i, 0))] + anywhere(n_cp),
        out_specs=[
            pl.BlockSpec((1, rows, groups * HD), lambda h, i, *_: (i, 0, h)),
            pl.BlockSpec((1, 8, rows), lambda h, i, *_: (h, 0, i)),
        ],
        scratch_shapes=[
            pltpu.VMEM((kv_heads, n_cp, seq, HD), BF16),
            pltpu.VMEM((kv_heads, n_cp, seq, HD), BF16),
            pltpu.VMEM((groups, rows, HD), F32),
            pltpu.VMEM((groups, rows, 2 * HD), F32),
            pltpu.SemaphoreType.DMA((n_cp, kv_heads, 2)),
        ],
    )
    pairs = heads * rows * rows * (2 * n_cp + 1)
    return pl.pallas_call(
        functools.partial(fwd_kernel, n_cp),
        name="fwd",
        grid_spec=grid_spec,
        out_shape=[
            like((2, rows, heads * HD), BF16),
            like((kv_heads, 8, seq), F32),
        ],
        compiler_params=params(2),
        cost_estimate=cost(2 * pairs * HD, 4 * seq * heads * HD, pairs),
    )(me, q_fin, *kv_blocks)


def bwd_kernel(n_cp, half, me_ref, q_ref, do_ref, o_ref, lse_ref, qraw_ref, cos_ref, sin_ref, qn_ref, *rest):
    kv_refs, rest = rest[:n_cp], rest[n_cp:]
    if half:
        dq_ref, keep_ref, send_ref, low_ref, gain_ref = rest[:5]
    else:
        low_ref, dq_ref, keep_ref, send_ref, gain_ref = rest[:5]
    k_buf, v_buf, dq_scr, dkv_scr, sems = rest[5:]
    h = pl.program_id(0)
    groups, rows, _ = q_ref.shape
    two = n_cp // 2

    @pl.when(h == 0)
    def _():
        load_kv(kv_refs, k_buf, v_buf, sems, range(k_buf.shape[0]))
        gain_ref[:] = jnp.zeros(gain_ref.shape, F32)

    if half:
        dkv_scr[:] = jnp.zeros(dkv_scr.shape, F32)
    else:
        dkv_scr[:] = low_ref[:, :, 0]

    me = me_ref[0]
    piece = 2 * n_cp - 1 - me if half else me
    scale = HD ** -0.5
    delta = []
    for g in range(groups):
        prod = do_ref[g].astype(F32) * o_ref[0, :, g * HD:(g + 1) * HD].astype(F32)
        column = jnp.broadcast_to(row_sum(prod), (rows, HD))
        delta.append(jnp.transpose(column)[0:1, :])
    dq_scr[:] = jnp.zeros(dq_scr.shape, F32)

    def block(j, masked):
        slot, upper = piece_place(j, me, n_cp)
        span = pl.ds(pl.multiple_of(upper * rows, rows), rows)
        k = k_buf[h, slot, span, :]
        v = v_buf[h, slot, span, :]
        probs, d_scores = [], []
        for g in range(groups):
            s = dot(k, q_ref[g], NT)
            p = jnp.exp2(s * (scale * LOG2E) - lse_ref[0, g:g + 1, :])
            if masked:
                k_pos = lax.broadcasted_iota(jnp.int32, s.shape, 0)
                q_pos = lax.broadcasted_iota(jnp.int32, s.shape, 1)
                p = jnp.where(k_pos <= q_pos, p, 0.0)
            probs.append(p.astype(BF16))
            d_scores.append((p * (dot(v, do_ref[g], NT) - delta[g])).astype(BF16))
        for g in range(groups):
            dq_scr[g] += dot(d_scores[g], k, TN)
        index = (slot % 2) * two + slot // 2
        into = span if half else pl.ds(0, rows)
        d_all = jnp.concatenate(d_scores, axis=1)
        p_all = jnp.concatenate(probs, axis=1)
        dkv_scr[index, 0, into, :] += dot(d_all, q_ref[:].reshape(groups * rows, HD)) * scale
        dkv_scr[index, 1, into, :] += dot(p_all, do_ref[:].reshape(groups * rows, HD))

    def full(j, carry):
        block(j, False)
        return carry

    lax.fori_loop(0, piece, full, 0)
    block(piece, True)
    for g in range(groups):
        d_raw, d_gain = norm_rope_back(dq_scr[g] * scale, qraw_ref[g], qn_ref[:], cos_ref[:], sin_ref[:])
        dq_ref[:, g * HD:(g + 1) * HD] = d_raw
        gain_ref[0:1, :] += d_gain
    for i in range(two):
        own = slice(rows, 2 * rows) if half else slice(0, rows)
        keep_ref[i, :, 0] = dkv_scr[i, :, own]
        send_ref[i, :, 0] = dkv_scr[two + i, :, own]
    if half:
        low_ref[:, :, 0] = dkv_scr[:, :, :rows]


def attention_bwd(half, me, q_fin, d_out, out, lse, q_raw, cos_t, sin_t, q_norm, kv_blocks, kv_heads, low=None):
    heads, seq, _ = q_fin.shape
    n_cp = len(kv_blocks)
    groups = heads // kv_heads
    rows = seq // 2
    by_head = pl.BlockSpec((groups, rows, HD), lambda h, *_: (h, half, 0))
    table = rows_of(rows, HD, lambda h: half)
    by_owner = lambda n: pl.BlockSpec((n, 2, 1, rows, HD), lambda h, *_: (0, 0, h, 0, 0))
    grads = lambda n: like((n, 2, kv_heads, rows, HD), F32)
    extra = () if low is None else (low,)
    carried = [n_cp] if half else []
    grid_spec = pltpu.PrefetchScalarGridSpec(
        num_scalar_prefetch=1,
        grid=(kv_heads,),
        in_specs=[
            by_head,
            pl.BlockSpec((groups, rows, HD), lambda h, *_: (h, 0, 0)),
            pl.BlockSpec((1, rows, groups * HD), lambda h, *_: (half, 0, h)),
            pl.BlockSpec((1, 8, rows), lambda h, *_: (h, 0, half)),
            by_head,
            table,
            table,
            whole((1, HD)),
        ]
        + anywhere(n_cp)
        + [by_owner(n_cp)] * len(extra),
        out_specs=[
            pl.BlockSpec((rows, groups * HD), lambda h, *_: (0, h)),
            by_owner(n_cp // 2),
            by_owner(n_cp // 2),
            *map(by_owner, carried),
            whole((8, HD)),
        ],
        scratch_shapes=[
            pltpu.VMEM((kv_heads, n_cp, seq, HD), BF16),
            pltpu.VMEM((kv_heads, n_cp, seq, HD), BF16),
            pltpu.VMEM((groups, rows, HD), F32),
            pltpu.VMEM((n_cp, 2, seq if half else rows, HD), F32),
            pltpu.SemaphoreType.DMA((n_cp, kv_heads, 2)),
        ],
    )
    pairs = heads * rows * rows * (n_cp + 1)
    return pl.pallas_call(
        functools.partial(bwd_kernel, n_cp, half),
        grid_spec=grid_spec,
        out_shape=[
            like((rows, heads * HD), BF16),
            grads(n_cp // 2),
            grads(n_cp // 2),
            *map(grads, carried),
            like((8, HD), F32),
        ],
        compiler_params=params(1),
        cost_estimate=cost(5 * pairs * HD, 8 * seq * heads * HD, pairs),
    )(me, q_fin, d_out, out, lse, q_raw, cos_t, sin_t, q_norm, *kv_blocks, *extra)


def post_kernel(n_w, later, at_ref, o_ref, *rest):
    w_refs, rest = rest[:n_w], rest[n_w:]
    mine_ref, wmine_ref, x_ref, dy_ref, wpost_ref = rest[:5]
    y_ref, do_ref, give_ref, keep_ref, dpost_ref = rest[-12:-7]
    o_buf, w_buf, attn_scr, dattn_scr, o_sem, w_sem, sum_sem = rest[-7:]
    i = pl.program_id(0)
    n_tp, _, width = o_ref.shape
    rows, dim = x_ref.shape
    cols = attn_scr.shape[2]
    steps = n_w // 2
    sums = [pltpu.make_async_copy(rest[5 + j], (give_ref, keep_ref)[j], sum_sem.at[j]) for j in range(2)] if later else []

    def weight_copies(pair, par):
        to = [w_buf.at[par, :, pl.ds(j * cols, cols)] for j in range(2)]
        return [pltpu.make_async_copy(w_refs[2 * pair + j], to[j], w_sem.at[par, j]) for j in range(2)]

    @pl.when(i == 0)
    def _():
        copies = [
            pltpu.make_async_copy(o_ref.at[t], o_buf.at[:, pl.ds(t * width, width)], o_sem.at[t]) for t in range(n_tp)
        ]
        for copy in copies + weight_copies(0, 0) + sums:
            copy.start()
        for copy in copies:
            copy.wait()

    for pair in range(1, steps):

        @pl.when(i == pair - 1)
        def _():
            for copy in weight_copies(pair, pair % 2):
                copy.start()

    @pl.when(i < steps)
    def _():
        par = lax.rem(i, 2)
        for copy in weight_copies(0, par):
            copy.wait()
        both = dot(o_buf[:], w_buf[par])
        for j in range(2):
            attn_scr[jnp.bitwise_xor(at_ref[0], 2 * i + j)] = both[:, j * cols:(j + 1) * cols]

    @pl.when(i == steps)
    def _():
        dpost_ref[:] = jnp.zeros(dpost_ref.shape, F32)
        if later:
            for copy in sums:
                copy.wait()
        else:
            give_ref[:] = jnp.zeros(give_ref.shape, F32)
            keep_ref[:] = jnp.zeros(keep_ref.shape, F32)

    @pl.when(i >= steps)
    def _():
        tiles = [(s, t * HD, slice(s * cols + t * HD, s * cols + (t + 1) * HD)) for s in range(n_w) for t in range(cols // HD)]
        sub = min(64, rows)

        def some_rows(r, carry):
            here = pl.ds(pl.multiple_of(r * sub, sub), sub)
            there = pl.ds(pl.multiple_of((i - steps) * rows + r * sub, sub), sub)
            square = jnp.zeros((sub, HD), F32)
            cross = jnp.zeros((sub, HD), F32)
            for s, t, at in tiles:
                attn = attn_scr[s, there, t:t + HD]
                square += attn * attn
                cross += attn * (dy_ref[here, at].astype(F32) * (1.0 + wpost_ref[:, at]))
            inv = inv_rms(square, dim)
            shrink = inv * inv * inv * (row_sum(cross) * (1.0 / dim))
            for s, t, at in tiles:
                attn = attn_scr[s, there, t:t + HD]
                gain = 1.0 + wpost_ref[:, at]
                dy = dy_ref[here, at].astype(F32)
                unit = attn * inv
                y_ref[here, at] = (x_ref[here, at].astype(F32) + unit * gain).astype(BF16)
                dpost_ref[:, at] += jnp.sum((dy * unit).reshape(sub // 8, 8, HD), axis=0)
                dattn_scr[here, at] = (inv * (dy * gain) - attn * shrink).astype(BF16)
            return carry

        lax.fori_loop(0, rows // sub, some_rows, 0)
        d_attn = dattn_scr[:]
        d_out = dot(d_attn, wmine_ref[:], NT)
        for h in range(do_ref.shape[0]):
            do_ref[h] = d_out[:, h * HD:(h + 1) * HD].astype(BF16)
        half = give_ref.shape[0]
        core = at_ref[1]
        give_ref[:] += dot(mine_ref[0, :, pl.ds(pl.multiple_of((1 - core) * half, HD), half)], d_attn, TN)
        keep_ref[:] += dot(mine_ref[0, :, pl.ds(pl.multiple_of(core * half, HD), half)], d_attn, TN)


def post(half, at, out_all, w_all, out, w_mine, x, dy, w_post, before=None):
    n_tp, chunk, width = out_all.shape
    seq, dim = x.shape
    rows = min(256, chunk)
    heads = width // HD
    n_w = len(w_all)
    n = chunk // rows
    steps = n_w // 2
    block = lambda i: jnp.maximum(i - steps, 0)
    row = rows_of(rows, dim, lambda i: half * n + block(i))
    sums = like((width // 2, dim), F32)
    extra = () if before is None else tuple(before)
    grid_spec = pltpu.PrefetchScalarGridSpec(
        num_scalar_prefetch=1,
        grid=(steps + n,),
        in_specs=anywhere(1 + n_w)
        + [pl.BlockSpec((1, rows, width), lambda i, *_: (half, block(i), 0))]
        + [fixed(w_mine.shape), row, row, whole((1, dim))]
        + anywhere(len(extra)),
        out_specs=[
            row,
            pl.BlockSpec((heads, rows, HD), lambda i, *_: (0, block(i), 0)),
            fixed(sums.shape),
            fixed(sums.shape),
            whole((8, dim)),
        ],
        scratch_shapes=[
            pltpu.VMEM((chunk, n_tp * width), BF16),
            pltpu.VMEM((2, n_tp * width, dim // steps), BF16),
            pltpu.VMEM((n_w, chunk, dim // n_w), F32),
            pltpu.VMEM((rows, dim), BF16),
            pltpu.SemaphoreType.DMA((n_tp,)),
            pltpu.SemaphoreType.DMA((2, 2)),
            pltpu.SemaphoreType.DMA((2,)),
        ],
    )
    return pl.pallas_call(
        functools.partial(post_kernel, n_w, bool(extra)),
        grid_spec=grid_spec,
        out_shape=[like((seq, dim), BF16), like((heads, chunk, HD), BF16), sums, sums, like((8, dim), F32)],
        input_output_aliases={n_w + 9: 0} if extra else {},
        compiler_params=params(1, VMEM_TOP),
        cost_estimate=cost(chunk * dim * width * (n_tp + 2), dim * (4 * chunk + width * n_tp)),
    )(at, out_all, *w_all, out, w_mine, x, dy, w_post, *extra)


def kback_kernel(own_ref, near_ref, far_ref, kraw_ref, cos_ref, sin_ref, kn_ref, out_ref, gain_ref):
    @pl.when(pl.program_id(0) == 0)
    def _():
        gain_ref[:] = jnp.zeros(gain_ref.shape, F32)

    kv_heads = own_ref.shape[2]
    for h in range(kv_heads):
        cols = slice(h * HD, (h + 1) * HD)
        d_k = own_ref[0, 0, h] + near_ref[0, 0, h] + far_ref[0, h]
        d_raw, d_gain = norm_rope_back(d_k, kraw_ref[:, cols], kn_ref[:], cos_ref[:], sin_ref[:])
        out_ref[:, cols] = d_raw
        gain_ref[0:1, :] += d_gain
        d_v = own_ref[0, 1, h] + near_ref[0, 1, h] + far_ref[1, h]
        out_ref[:, (kv_heads + h) * HD:(kv_heads + h + 1) * HD] = d_v.astype(BF16)


def key_back(half, own, near, far, k_raw, cos_t, sin_t, k_norm):
    _, _, kv_heads, chunk, _ = own.shape
    rows = min(256, chunk)
    n = chunk // rows
    two = pl.BlockSpec((1, 2, kv_heads, rows, HD), lambda i: (0, 0, 0, i, 0))
    row = lambda cols: rows_of(rows, cols, lambda i: half * n + i)
    return pl.pallas_call(
        kback_kernel,
        grid=(n,),
        in_specs=[
            two,
            two,
            pl.BlockSpec((2, kv_heads, rows, HD), lambda i: (0, 0, i, 0)),
            row(kv_heads * HD),
            row(HD),
            row(HD),
            whole((1, HD)),
        ],
        out_specs=[rows_of(rows, 2 * kv_heads * HD), whole((8, HD))],
        out_shape=[
            like((chunk, 2 * kv_heads * HD), BF16),
            like((8, HD), F32),
        ],
        compiler_params=params(1),
        cost_estimate=cost(32 * chunk * kv_heads * HD, 8 * chunk * kv_heads * HD),
    )(own, near, far, k_raw, cos_t, sin_t, k_norm)


def dx_kernel(n_tp, n_w, at_ref, *refs):
    g_refs, refs = refs[:2 * n_tp], refs[2 * n_tp:]
    w_refs, refs = refs[:n_w], refs[n_w:]
    x_refs, dy_refs, wpre_ref = refs[:2], refs[2:4], refs[4]
    dx_ref, dpre_ref, g_scr, w_buf, acc, sem = refs[5:]
    i = pl.program_id(0)
    rows, width = g_refs[0].shape
    cols = acc.shape[2]

    def weight_copies(pair, par):
        return [pltpu.make_async_copy(w_refs[2 * pair + j], w_buf.at[par, :, j], sem.at[par, j]) for j in range(2)]

    @pl.when(i == 0)
    def _():
        for copy in weight_copies(0, 0):
            copy.start()
        for s in range(n_tp):
            t = lax.rem(at_ref[1] + n_tp - s, n_tp)
            for half in range(2):
                g_scr[t, half * rows:(half + 1) * rows, :] = g_refs[half * n_tp + s][:]

    for pair in range(1, n_w // 2):

        @pl.when(i == pair - 1)
        def _():
            for copy in weight_copies(pair, pair % 2):
                copy.start()

    par = lax.rem(i, 2)
    for copy in weight_copies(0, par):
        copy.wait()
    total = dot(g_scr[0], w_buf[par, 0].reshape(2 * cols, width), NT)
    for t in range(1, n_tp):
        total += dot(g_scr[t], w_buf[par, t].reshape(2 * cols, width), NT)
    for j in range(2):
        acc[jnp.bitwise_xor(at_ref[0], 2 * i + j)] = total[:, j * cols:(j + 1) * cols]

    @pl.when(i == pl.num_programs(0) - 1)
    def _():
        dpre_ref[:] = jnp.zeros(dpre_ref.shape, F32)
        n, _, width = acc.shape
        tiles = [(s, t, slice(s * width + t, s * width + t + HD)) for s in range(n) for t in range(0, width, HD)]
        dim = n * width
        sub = min(64, rows)
        for half in range(2):
            x_ref, dy_ref = x_refs[half], dy_refs[half]

            def some_rows(r, carry):
                here = pl.ds(pl.multiple_of(r * sub, sub), sub)
                there = pl.ds(pl.multiple_of(half * rows + r * sub, sub), sub)
                square = jnp.zeros((sub, HD), F32)
                cross = jnp.zeros((sub, HD), F32)
                for s, t, at in tiles:
                    x = x_ref[here, at].astype(F32)
                    square += x * x
                    cross += x * (acc[s, there, t:t + HD] * (1.0 + wpre_ref[:, at]))
                inv = inv_rms(square, dim)
                shrink = inv * inv * inv * (row_sum(cross) * (1.0 / dim))
                for s, t, at in tiles:
                    x = x_ref[here, at].astype(F32)
                    d_normed = acc[s, there, t:t + HD]
                    dpre_ref[:, at] += jnp.sum((d_normed * (x * inv)).reshape(sub // 8, 8, HD), axis=0)
                    d_x = inv * (d_normed * (1.0 + wpre_ref[:, at])) - x * shrink
                    dx_ref[there, at] = (dy_ref[here, at].astype(F32) + d_x).astype(BF16)
                return carry

            lax.fori_loop(0, rows // sub, some_rows, 0)


def input_grad(at, grads, w_all, x, dy, w_pre):
    n_tp = len(grads) // 2
    n = len(w_all)
    rows, width = grads[0].shape
    dim = x.shape[1]
    cols = dim // n
    here = [pl.BlockSpec((rows, dim), lambda i, t, half=half: (half * n_tp + t[1], 0)) for half in range(2)]
    grid_spec = pltpu.PrefetchScalarGridSpec(
        num_scalar_prefetch=1,
        grid=(n // 2,),
        in_specs=[whole((rows, width))] * len(grads) + anywhere(n) + here + here + [whole((1, dim))],
        out_specs=[whole((2 * rows, dim)), whole((8, dim))],
        scratch_shapes=[
            pltpu.VMEM((n_tp, 2 * rows, width), BF16),
            pltpu.VMEM((2, n_tp, 2, cols, width), BF16),
            pltpu.VMEM((n, 2 * rows, cols), F32),
            pltpu.SemaphoreType.DMA((2, 2)),
        ],
    )
    return pl.pallas_call(
        functools.partial(dx_kernel, n_tp, n),
        name="dx",
        grid_spec=grid_spec,
        out_shape=[like((2 * rows, dim), BF16), like((8, dim), F32)],
        compiler_params=params(1),
        cost_estimate=cost(2 * n_tp * rows * width * dim, n_tp * width * dim),
    )(at, *grads, *w_all, x, x, dy, dy, w_pre)


def dw_kernel(n_cp, me_ref, *refs):
    g_refs, n_refs = refs[:2 * n_cp], refs[2 * n_cp:-7]
    dwq_ref, dwk_ref, dwv_ref, n_buf, g_buf, n_sem, g_sem = refs[-7:]
    i = pl.program_id(0)
    cols = n_buf.shape[3]
    chunk, width = g_refs[0].shape
    me = me_ref[0]

    def place(refs_in, buf, sem):
        copies = []
        for j, (ref, shape) in enumerate(refs_in):
            start = sum(r[1] for r in refs_in[:j - j % n_cp:n_cp])
            to = buf.at[jnp.bitwise_xor(me, j % n_cp), pl.ds(start, shape)]
            copies.append(pltpu.make_async_copy(ref, to, sem.at[j]))
        return copies

    def fetch(step, par):
        span = pl.ds(pl.multiple_of(step * cols, cols), cols)
        return place([(r.at[:, span], r.shape[0]) for r in n_refs], n_buf.at[par], n_sem.at[par])

    @pl.when(i == 0)
    def _():
        grads = place([(r, chunk) for r in g_refs], g_buf, g_sem)
        for copy in fetch(0, 0) + grads:
            copy.start()
        for copy in grads:
            copy.wait()

    @pl.when(i + 1 < pl.num_programs(0))
    def _():
        for copy in fetch(i + 1, (i + 1) % 2):
            copy.start()

    for copy in fetch(i, i % 2):
        copy.wait()
    seq = 2 * chunk
    grad = dot(n_buf[i % 2].reshape(n_cp * seq, cols), g_buf[:].reshape(n_cp * seq, width), TN)
    q_width, kv_width = dwq_ref.shape[1], dwk_ref.shape[1]
    dwq_ref[:] = grad[:, :q_width]
    dwk_ref[:] = grad[:, q_width:q_width + kv_width]
    dwv_ref[:] = grad[:, q_width + kv_width:]


def weight_grads(me, normed, grads, q_width, cols=256):
    n_cp = len(grads) // 2
    chunk, width = grads[0].shape
    dim = normed[0].shape[1]
    kv_width = (width - q_width) // 2
    tile = lambda n: rows_of(cols, n)
    grid_spec = pltpu.PrefetchScalarGridSpec(
        num_scalar_prefetch=1,
        grid=(dim // cols,),
        in_specs=anywhere(len(grads) + len(normed)),
        out_specs=[tile(q_width), tile(kv_width), tile(kv_width)],
        scratch_shapes=[
            pltpu.VMEM((2, n_cp, 2 * chunk, cols), BF16),
            pltpu.VMEM((n_cp, 2 * chunk, width), BF16),
            pltpu.SemaphoreType.DMA((2, len(normed))),
            pltpu.SemaphoreType.DMA((len(grads),)),
        ],
    )
    return pl.pallas_call(
        functools.partial(dw_kernel, n_cp),
        name="dw",
        grid_spec=grid_spec,
        out_shape=[like((dim, n), F32) for n in (q_width, kv_width, kv_width)],
        compiler_params=params(1),
        cost_estimate=cost(2 * n_cp * chunk * dim * width, 2 * n_cp * chunk * (dim + width)),
    )(me, *grads, *normed)


def join_kernel(core_ref, keep_ref, other_ref, *rest):
    half = pl.program_id(0)

    @pl.when(half == core_ref[0])
    def _():
        rest[-1][:] = keep_ref[:]

    @pl.when(half != core_ref[0])
    def _():
        rest[-1][:] = other_ref[:]


def join_halves(core, keep, other, start, half, total=None):
    block, width = HD, keep.shape[1]
    n = keep.shape[0] // block
    extra = () if total is None else (total,)
    part = pl.BlockSpec((block, width), lambda i, j, c: (j, 0))
    grid_spec = pltpu.PrefetchScalarGridSpec(
        num_scalar_prefetch=1,
        grid=(2, n),
        in_specs=[part, part] + anywhere(len(extra)),
        out_specs=pl.BlockSpec((block, width), lambda i, j, c: (i * (half // block) + start // block + j, 0)),
    )
    return pl.pallas_call(
        join_kernel,
        name="join",
        grid_spec=grid_spec,
        out_shape=like((2 * half, width), F32),
        input_output_aliases={3: 0} if extra else {},
        compiler_params=params(2),
        cost_estimate=cost(n * block * width, 8 * n * block * width),
    )(core, keep, other, *extra)


def solution(mesh):
    n_cp, n_tp, n_dp = mesh.shape["cp"], mesh.shape["tp"], mesh.shape["dp"]
    near = [(i, i ^ 1) for i in range(n_cp)]
    across = [(i, i ^ 2) for i in range(n_cp)]
    beside = [(i, i ^ 1) for i in range(n_dp)]

    def from_cp(value):
        far = lax.ppermute(value, "cp", across)
        return [value, lax.ppermute(value, "cp", near), far, lax.ppermute(far, "cp", near)]

    def per_device(hidden, cotangent, pos_loc, w_q, w_k, w_v, w_o, w_pre, w_post, q_norm, k_norm):
        _, seq, dim = hidden.shape
        x, dy = hidden[0], cotangent[0]
        kv_heads = w_k.shape[1] // HD
        cp, tp, dp = (lax.axis_index(a).astype(jnp.int32) for a in ("cp", "tp", "dp"))
        core = cp % 2
        me, one_core = cp.reshape(1), core.reshape(1)

        share = dp * n_cp + cp
        shares = n_dp * n_cp
        cols = dim // shares

        def over_tp(part):
            return lax.all_gather(part, "tp", axis=0, tiled=True)

        def spread(own):
            blocks = from_cp(own)
            if n_dp == 2:
                for value in (own, blocks[2]):
                    other = lax.ppermute(value, "dp", beside)
                    blocks += [other, lax.ppermute(other, "cp", near)]
            return blocks

        w_o_all = spread(over_tp(lax.dynamic_slice_in_dim(w_o, share * cols, cols, 1)))
        w_in = jnp.concatenate([lax.dynamic_slice_in_dim(w, share * cols, cols, 0) for w in (w_q, w_k, w_v)], axis=1)
        w_in_all = spread(over_tp(w_in).reshape(n_tp, cols, w_in.shape[1]))

        cos_t, sin_t = rope_tables(pos_loc)
        qn, kn = q_norm.reshape(1, HD), k_norm.reshape(1, HD)
        wpre, wpost = w_pre.reshape(1, dim), w_post.reshape(1, dim)
        first, later, kv_own, k_raw = project_kv(x, wpre, w_k, w_v, kn, cos_t, sin_t, seq // 4)
        kv_blocks = from_cp(kv_own)
        q_fin, q_raw = project_q(first, later, w_q, qn, cos_t, sin_t)
        normed_all = from_cp(first) + from_cp(later)
        out, lse = attention_fwd(me, q_fin, kv_blocks, kv_heads)

        out_all = [None, None]
        for half in (1, 0):
            out_all[half] = lax.all_gather(out[half], "tp", axis=0, tiled=False)
        at = jnp.stack([share, core])

        done, low, dq, d_post, gains, carried = None, [], [None] * 2, [], [], [None] * 2
        for half in (1, 0):
            y, d_out, give, keep, part = post(half, at, out_all[half], w_o_all, out, w_o, x, dy, wpost, done)
            done = (give, keep, y)
            d_post.append(part)
            dq[half], kept, sent, *low, gain = attention_bwd(
                half, me, q_fin, d_out, out, lse, q_raw, cos_t, sin_t, qn, kv_blocks, kv_heads, *low
            )
            gains.append(gain[0])
            got = lax.ppermute(sent, "cp", near)
            carried[half] = (kept, got, lax.ppermute(kept[1] + got[1], "cp", across))

        got = lax.ppermute(give, "cp", near)
        rows = keep.shape[0]
        d_wo = None
        for start, stop in ((0, rows - HD), (rows - HD, rows)):
            mine_part = keep[start:stop] + got[start:stop]
            mine_part = mine_part + lax.ppermute(mine_part, "cp", across)
            other = lax.ppermute(mine_part, "cp", near)
            d_wo = join_halves(one_core, mine_part, other, start, rows, d_wo)

        rows = seq // 2 // n_tp
        grads, pieces = [], [None] * 2
        for half in (1, 0):
            d_kv, gain = key_back(half, *carried[half], k_raw, cos_t, sin_t, kn)
            gains.append(gain[0])
            g = jnp.concatenate([dq[half], d_kv], axis=1)
            pieces[half] = [lax.dynamic_slice_in_dim(g, tp * rows, rows, 0)]
            for s in range(1, n_tp):
                part = lax.dynamic_slice_in_dim(g, ((tp + s) % n_tp) * rows, rows, 0)
                pieces[half].append(lax.ppermute(part, "tp", [(i, (i + s) % n_tp) for i in range(n_tp)]))
            grads.append(g)
        dx_rows, d_pre = input_grad(jnp.stack([share, tp]), pieces[0] + pieces[1], w_in_all, x, dy, wpre)
        d_hidden = lax.all_gather(dx_rows, "tp", axis=0, tiled=False)
        d_hidden = d_hidden.reshape(n_tp, 2, rows, dim).swapaxes(0, 1).reshape(seq, dim)

        grads_all = from_cp(grads[1]) + from_cp(grads[0])
        d_wq, d_wk, d_wv = weight_grads(me, normed_all, grads_all, w_q.shape[1])

        d_post = jnp.sum(sum(d_post), axis=0)
        small = jnp.concatenate([jnp.where(tp == 0, d_post, 0.0), jnp.sum(d_pre, axis=0), sum(gains[:2]), sum(gains[2:])])
        small = small + lax.ppermute(small, "cp", near)
        small = small + lax.ppermute(small, "cp", across)
        small = small + lax.ppermute(small, "tp", [(i, i ^ 1) for i in range(n_tp)])
        small = small + lax.ppermute(small, "tp", [(i, i ^ 2) for i in range(n_tp)])
        d_post, d_pre, d_qn, d_kn = jnp.split(small, np.cumsum([dim, dim, HD]))
        return y[None], d_hidden[None], d_wq, d_wk, d_wv, d_wo, d_pre, d_post, d_qn, d_kn

    rows, cols, all_of = P('dp', 'cp'), P(None, 'tp'), P()
    specs_in = (rows, rows, P(('dp', 'cp')), cols, cols, cols, P('tp'), all_of, all_of, all_of, all_of)
    grid, by_dp = P('dp', 'tp'), P('dp')
    specs_out = (rows, rows, grid, grid, grid, P(('dp', 'tp')), by_dp, by_dp, by_dp, by_dp)
    return jax.shard_map(per_device, mesh=mesh, in_specs=specs_in, out_specs=specs_out, check_vma=False)
```

```python
import functools

import jax
import jax.numpy as jnp
import numpy as np
from jax import lax
from jax.experimental import pallas as pl
from jax.experimental.pallas import tpu as pltpu
from jax.sharding import PartitionSpec as P


EPS = 1e-6
ROPE_BASE = 1000000.0
ROPE_SCALE = 8.0
NEG_BIG = -1e30
LOG2E = 1.4426950408889634
HD = 128
F32 = jnp.float32
BF16 = jnp.bfloat16
VMEM_MAX = 62914560
NT = (((1,), (1,)), ((), ()))
TN = (((0,), (0,)), ((), ()))


def dot(a, b, dims=(((1,), (0,)), ((), ()))):
    return lax.dot_general(a, b, dims, preferred_element_type=F32)


def params(dims, vmem=VMEM_MAX):
    return pltpu.CompilerParams(dimension_semantics=("arbitrary",) * dims, vmem_limit_bytes=vmem)


def cost(products, values, trans=0):
    return pl.CostEstimate(flops=2 * products, bytes_accessed=2 * values, transcendentals=trans)


def row_sum(values):
    return jnp.sum(values, axis=1, keepdims=True)


def inv_rms(square, dim):
    return lax.rsqrt(row_sum(square) * (1.0 / dim) + EPS)


def whole(shape):
    return pl.BlockSpec(shape, lambda *_: (0,) * len(shape))


def fixed(shape):
    return pl.BlockSpec(shape, lambda *_: (0,) * len(shape), pipeline_mode=pl.Buffered(buffer_count=1))


def rows_of(rows, cols, at=lambda i: i):
    return pl.BlockSpec((rows, cols), lambda i, *_: (at(i), 0))


def anywhere(n):
    return [pl.BlockSpec(memory_space=pl.ANY)] * n


def like(shape, dtype):
    return jax.ShapeDtypeStruct(shape, dtype)


def rope_tables(pos_loc):
    half_dim = HD // 2
    inv_freq = 1.0 / (ROPE_SCALE * ROPE_BASE ** (jnp.arange(half_dim, dtype=F32) * (2.0 / HD)))
    angles = pos_loc.astype(F32)[:, None] * inv_freq[None, :]
    cos_t, sin_t = jnp.cos(angles), jnp.sin(angles)
    return jnp.concatenate([cos_t, cos_t], axis=-1), jnp.concatenate([-sin_t, sin_t], axis=-1)


def norm_rope(raw, gain, cos_t, sin_t):
    raw = raw.astype(F32)
    unit = raw * inv_rms(raw * raw, HD)
    scaled = unit * (1.0 + gain)
    return (scaled * cos_t + pltpu.roll(scaled, HD // 2, 1) * sin_t).astype(BF16)


def norm_rope_back(d_final, raw, gain, cos_t, sin_t):
    raw = raw.astype(F32)
    inv = inv_rms(raw * raw, HD)
    unit = raw * inv
    d_scaled = d_final * cos_t - pltpu.roll(d_final, HD // 2, 1) * sin_t
    d_gain = jnp.sum(d_scaled * unit, axis=0, keepdims=True)
    d_unit = d_scaled * (1.0 + gain)
    d_raw = inv * (d_unit - unit * (row_sum(d_unit * unit) * (1.0 / HD)))
    return d_raw.astype(BF16), d_gain


def normalise(x_ref, wpre_ref, write):
    rows, dim = x_ref.shape
    tiles = [slice(t, t + HD) for t in range(0, dim, HD)]
    sub = min(64, rows)

    def some_rows(r, carry):
        here = pl.ds(pl.multiple_of(r * sub, sub), sub)
        square = jnp.zeros((sub, HD), F32)
        for at in tiles:
            x = x_ref[here, at].astype(F32)
            square += x * x
        inv = inv_rms(square, dim)
        for at in tiles:
            write(here, at, (x_ref[here, at].astype(F32) * inv * (1.0 + wpre_ref[:, at])).astype(BF16))
        return carry

    lax.fori_loop(0, rows // sub, some_rows, 0)


def norm_kernel(x_ref, wpre_ref, out_ref):
    def write(rows, cols, value):
        out_ref[rows, cols] = value

    normalise(x_ref, wpre_ref, write)


def norm_rows(x, w_pre):
    return pl.pallas_call(
        norm_kernel,
        name="norm",
        grid=(1,),
        in_specs=[whole(x.shape), whole(w_pre.shape)],
        out_specs=whole(x.shape),
        out_shape=like(x.shape, BF16),
        compiler_params=params(1),
        cost_estimate=cost(4 * x.shape[0] * x.shape[1], 2 * x.shape[0] * x.shape[1]),
    )(x, w_pre)


def kv_kernel(parts, x_ref, wpre_ref, wk_ref, wv_ref, kn_ref, cos_ref, sin_ref, *rest):
    n = len(parts)
    out_refs, (kv_ref, kraw_ref, buf, sem) = rest[:n], rest[n:]
    i = pl.program_id(0)
    rows = x_ref.shape[0]
    par = i % 2
    steps = [(j, step) for j, size in enumerate(parts) for step in range(size)]

    def out_copy(step):
        j, at = steps[step]
        return pltpu.make_async_copy(buf.at[step % 2], out_refs[j].at[pl.ds(at * rows, rows)], sem.at[step % 2])

    for step in range(2, len(steps)):

        @pl.when(i == step)
        def _():
            out_copy(step - 2).wait()

    def write(here, cols, value):
        buf[par, here, cols] = value

    normalise(x_ref, wpre_ref, write)
    for step in range(len(steps)):

        @pl.when(i == step)
        def _():
            out_copy(step).start()

    normed = buf[par]
    k_raw = dot(normed, wk_ref[:]).astype(BF16)
    kraw_ref[:] = k_raw
    width = k_raw.shape[1]
    for h in range(width // HD):
        cols = slice(h * HD, (h + 1) * HD)
        kv_ref[:, cols] = norm_rope(k_raw[:, cols], kn_ref[:], cos_ref[:], sin_ref[:])
    kv_ref[:, width:] = dot(normed, wv_ref[:]).astype(BF16)

    @pl.when(i == len(steps) - 1)
    def _():
        for step in range(len(steps))[-2:]:
            out_copy(step).wait()


def project_kv(x, w_pre, w_k, w_v, k_norm, cos_t, sin_t, rows, parts):
    seq, dim = x.shape
    width = w_k.shape[1]
    grid_spec = pl.GridSpec(
        grid=(seq // rows,),
        in_specs=[rows_of(rows, dim), whole((1, dim)), fixed(w_k.shape), fixed(w_v.shape), whole((1, HD))]
        + [rows_of(rows, HD)] * 2,
        out_specs=anywhere(len(parts)) + [rows_of(rows, 2 * width), rows_of(rows, width)],
        scratch_shapes=[pltpu.VMEM((2, rows, dim), BF16), pltpu.SemaphoreType.DMA((2,))],
    )
    return pl.pallas_call(
        functools.partial(kv_kernel, parts),
        name="pkv",
        grid_spec=grid_spec,
        out_shape=[like((n * rows, dim), BF16) for n in parts] + [like((seq, 2 * width), BF16), like((seq, width), BF16)],
        compiler_params=params(1),
        cost_estimate=cost(2 * seq * dim * width, 2 * dim * (seq + width)),
    )(x, w_pre, w_k, w_v, k_norm, cos_t, sin_t)


def q_kernel(starts, *refs):
    n_refs, (wq_ref, qn_ref, cos_ref, sin_ref, qfin_ref, qraw_ref) = refs[:len(starts)], refs[len(starts):]
    normed = n_refs[0][:]
    for start, ref in zip(starts[1:], n_refs[1:]):
        normed = jnp.where(pl.program_id(0) >= start, ref[:], normed)
    q_raw = dot(normed, wq_ref[:]).astype(BF16)
    for h in range(qfin_ref.shape[0]):
        part = q_raw[:, h * HD:(h + 1) * HD]
        qraw_ref[h] = part
        qfin_ref[h] = norm_rope(part, qn_ref[:], cos_ref[:], sin_ref[:])


def project_q(normed, w_q, q_norm, cos_t, sin_t, rows):
    dim, width = w_q.shape
    sizes = [part.shape[0] // rows for part in normed]
    starts = [sum(sizes[:j]) for j in range(len(sizes))]
    n = sum(sizes)
    heads = width // HD
    block = lambda start, size: rows_of(rows, dim, lambda i: jnp.clip(i - start, 0, size - 1))
    head_rows = pl.BlockSpec((heads, rows, HD), lambda i: (0, i, 0))
    shape = like((heads, n * rows, HD), BF16)
    return pl.pallas_call(
        functools.partial(q_kernel, starts),
        name="pq",
        grid=(n,),
        in_specs=list(map(block, starts, sizes)) + [fixed(w_q.shape), whole((1, HD))] + [rows_of(rows, HD)] * 2,
        out_specs=[head_rows, head_rows],
        out_shape=[shape, shape],
        compiler_params=params(1),
        cost_estimate=cost(n * rows * dim * width, dim * (n * rows + width)),
    )(*normed, w_q, q_norm, cos_t, sin_t)


def load_kv(kv_refs, k_buf, v_buf, sems, heads):
    kv_heads = kv_refs[0].shape[1] // (2 * HD)
    copies = []
    for s, ref in enumerate(kv_refs):
        for i, h in enumerate(heads):
            for t, buf in enumerate((k_buf, v_buf)):
                src = ref.at[:, pl.ds((t * kv_heads + h) * HD, HD)]
                copies.append(pltpu.make_async_copy(src, buf.at[i, s], sems.at[s, i, t]))
    for copy in copies:
        copy.start()
    for copy in copies:
        copy.wait()


def piece_place(piece, me, n_cp):
    upper = piece >= n_cp
    owner = jnp.where(upper, 2 * n_cp - 1 - piece, piece)
    return jnp.bitwise_xor(owner, me), upper.astype(jnp.int32)


def fwd_kernel(n_cp, me_ref, q_ref, *rest):
    kv_refs = rest[:n_cp]
    o_ref, lse_ref, k_buf, v_buf, m_scr, acc_scr, sems = rest[n_cp:]
    h, half = pl.program_id(0), pl.program_id(1)
    groups, rows, _ = q_ref.shape

    @pl.when((h == 0) & (half == 0))
    def _():
        load_kv(kv_refs, k_buf, v_buf, sems, range(k_buf.shape[0]))

    me = me_ref[0]
    piece = jnp.where(half == 0, me, 2 * n_cp - 1 - me)
    scale = HD ** -0.5 * LOG2E
    m_scr[:] = jnp.full(m_scr.shape, NEG_BIG, F32)
    acc_scr[:] = jnp.zeros(acc_scr.shape, F32)

    def block(j, masked):
        slot, upper = piece_place(j, me, n_cp)
        span = pl.ds(pl.multiple_of(upper * rows, rows), rows)
        k = k_buf[h, slot, span, :]
        v_ext = jnp.concatenate([v_buf[h, slot, span, :], jnp.ones((rows, HD), BF16)], axis=1)
        scores = [dot(q_ref[g], k, NT) * scale for g in range(groups)]
        for g in range(groups):
            s = scores[g]
            if masked:
                q_pos = lax.broadcasted_iota(jnp.int32, s.shape, 0)
                k_pos = lax.broadcasted_iota(jnp.int32, s.shape, 1)
                s = jnp.where(k_pos <= q_pos, s, NEG_BIG)
            m_old = m_scr[g]
            m_new = jnp.maximum(m_old, jnp.max(s, axis=1, keepdims=True))
            alpha = jnp.exp2(m_old - m_new)
            p = jnp.exp2(s - jnp.concatenate([m_new] * (rows // HD), axis=1)).astype(BF16)
            acc_scr[g] = acc_scr[g] * jnp.concatenate([alpha, alpha], axis=1) + dot(p, v_ext)
            m_scr[g] = m_new

    def full(j, carry):
        block(j, False)
        return carry

    lax.fori_loop(0, piece, full, 0)
    block(piece, True)
    for g in range(groups):
        l = acc_scr[g, :, HD:]
        o_ref[0, :, g * HD:(g + 1) * HD] = (acc_scr[g, :, :HD] / l).astype(BF16)
        lse_ref[0, g:g + 1, :] = jnp.transpose(m_scr[g] + jnp.log2(l))[0:1, :]


def attention_fwd(me, q_fin, kv_blocks, kv_heads):
    heads, seq, _ = q_fin.shape
    n_cp = len(kv_blocks)
    groups = heads // kv_heads
    rows = seq // 2
    grid_spec = pltpu.PrefetchScalarGridSpec(
        num_scalar_prefetch=1,
        grid=(kv_heads, 2),
        in_specs=[pl.BlockSpec((groups, rows, HD), lambda h, i, *_: (h, i, 0))] + anywhere(n_cp),
        out_specs=[
            pl.BlockSpec((1, rows, groups * HD), lambda h, i, *_: (i, 0, h)),
            pl.BlockSpec((1, 8, rows), lambda h, i, *_: (h, 0, i)),
        ],
        scratch_shapes=[
            pltpu.VMEM((kv_heads, n_cp, seq, HD), BF16),
            pltpu.VMEM((kv_heads, n_cp, seq, HD), BF16),
            pltpu.VMEM((groups, rows, HD), F32),
            pltpu.VMEM((groups, rows, 2 * HD), F32),
            pltpu.SemaphoreType.DMA((n_cp, kv_heads, 2)),
        ],
    )
    pairs = heads * rows * rows * (2 * n_cp + 1)
    return pl.pallas_call(
        functools.partial(fwd_kernel, n_cp),
        name="fwd",
        grid_spec=grid_spec,
        out_shape=[
            like((2, rows, heads * HD), BF16),
            like((kv_heads, 8, seq), F32),
        ],
        compiler_params=params(2),
        cost_estimate=cost(2 * pairs * HD, 4 * seq * heads * HD, pairs),
    )(me, q_fin, *kv_blocks)


def bwd_kernel(n_cp, half, me_ref, q_ref, do_ref, o_ref, lse_ref, qraw_ref, cos_ref, sin_ref, qn_ref, *rest):
    kv_refs, rest = rest[:n_cp], rest[n_cp:]
    if half:
        dq_ref, keep_ref, send_ref, low_ref, gain_ref = rest[:5]
    else:
        low_ref, dq_ref, keep_ref, send_ref, gain_ref = rest[:5]
    k_buf, v_buf, dq_scr, dkv_scr, sems = rest[5:]
    h = pl.program_id(0)
    groups, rows, _ = q_ref.shape
    two = n_cp // 2

    @pl.when(h == 0)
    def _():
        load_kv(kv_refs, k_buf, v_buf, sems, range(k_buf.shape[0]))
        gain_ref[:] = jnp.zeros(gain_ref.shape, F32)

    if half:
        dkv_scr[:] = jnp.zeros(dkv_scr.shape, F32)
    else:
        dkv_scr[:] = low_ref[:, :, 0]

    me = me_ref[0]
    piece = 2 * n_cp - 1 - me if half else me
    scale = HD ** -0.5
    delta = []
    for g in range(groups):
        prod = do_ref[g].astype(F32) * o_ref[0, :, g * HD:(g + 1) * HD].astype(F32)
        column = jnp.broadcast_to(row_sum(prod), (rows, HD))
        delta.append(jnp.transpose(column)[0:1, :])
    dq_scr[:] = jnp.zeros(dq_scr.shape, F32)

    def block(j, masked):
        slot, upper = piece_place(j, me, n_cp)
        span = pl.ds(pl.multiple_of(upper * rows, rows), rows)
        k = k_buf[h, slot, span, :]
        v = v_buf[h, slot, span, :]
        probs, d_scores = [], []
        for g in range(groups):
            s = dot(k, q_ref[g], NT)
            p = jnp.exp2(s * (scale * LOG2E) - lse_ref[0, g:g + 1, :])
            if masked:
                k_pos = lax.broadcasted_iota(jnp.int32, s.shape, 0)
                q_pos = lax.broadcasted_iota(jnp.int32, s.shape, 1)
                p = jnp.where(k_pos <= q_pos, p, 0.0)
            probs.append(p.astype(BF16))
            d_scores.append((p * (dot(v, do_ref[g], NT) - delta[g])).astype(BF16))
        for g in range(groups):
            dq_scr[g] += dot(d_scores[g], k, TN)
        index = (slot % 2) * two + slot // 2
        into = span if half else pl.ds(0, rows)
        d_all = jnp.concatenate(d_scores, axis=1)
        p_all = jnp.concatenate(probs, axis=1)
        dkv_scr[index, 0, into, :] += dot(d_all, q_ref[:].reshape(groups * rows, HD)) * scale
        dkv_scr[index, 1, into, :] += dot(p_all, do_ref[:].reshape(groups * rows, HD))

    def full(j, carry):
        block(j, False)
        return carry

    lax.fori_loop(0, piece, full, 0)
    block(piece, True)
    for g in range(groups):
        d_raw, d_gain = norm_rope_back(dq_scr[g] * scale, qraw_ref[g], qn_ref[:], cos_ref[:], sin_ref[:])
        dq_ref[:, g * HD:(g + 1) * HD] = d_raw
        gain_ref[0:1, :] += d_gain
    for i in range(two):
        own = slice(rows, 2 * rows) if half else slice(0, rows)
        keep_ref[i, :, 0] = dkv_scr[i, :, own]
        send_ref[i, :, 0] = dkv_scr[two + i, :, own]
    if half:
        low_ref[:, :, 0] = dkv_scr[:, :, :rows]


def attention_bwd(half, me, q_fin, d_out, out, lse, q_raw, cos_t, sin_t, q_norm, kv_blocks, kv_heads, low=None):
    heads, seq, _ = q_fin.shape
    n_cp = len(kv_blocks)
    groups = heads // kv_heads
    rows = seq // 2
    by_head = pl.BlockSpec((groups, rows, HD), lambda h, *_: (h, half, 0))
    table = rows_of(rows, HD, lambda h: half)
    by_owner = lambda n: pl.BlockSpec((n, 2, 1, rows, HD), lambda h, *_: (0, 0, h, 0, 0))
    grads = lambda n: like((n, 2, kv_heads, rows, HD), F32)
    extra = () if low is None else (low,)
    carried = [n_cp] if half else []
    grid_spec = pltpu.PrefetchScalarGridSpec(
        num_scalar_prefetch=1,
        grid=(kv_heads,),
        in_specs=[
            by_head,
            pl.BlockSpec((groups, rows, HD), lambda h, *_: (h, 0, 0)),
            pl.BlockSpec((1, rows, groups * HD), lambda h, *_: (half, 0, h)),
            pl.BlockSpec((1, 8, rows), lambda h, *_: (h, 0, half)),
            by_head,
            table,
            table,
            whole((1, HD)),
        ]
        + anywhere(n_cp)
        + [by_owner(n_cp)] * len(extra),
        out_specs=[
            pl.BlockSpec((rows, groups * HD), lambda h, *_: (0, h)),
            by_owner(n_cp // 2),
            by_owner(n_cp // 2),
            *map(by_owner, carried),
            whole((8, HD)),
        ],
        scratch_shapes=[
            pltpu.VMEM((kv_heads, n_cp, seq, HD), BF16),
            pltpu.VMEM((kv_heads, n_cp, seq, HD), BF16),
            pltpu.VMEM((groups, rows, HD), F32),
            pltpu.VMEM((n_cp, 2, seq if half else rows, HD), F32),
            pltpu.SemaphoreType.DMA((n_cp, kv_heads, 2)),
        ],
    )
    pairs = heads * rows * rows * (n_cp + 1)
    return pl.pallas_call(
        functools.partial(bwd_kernel, n_cp, half),
        grid_spec=grid_spec,
        out_shape=[
            like((rows, heads * HD), BF16),
            grads(n_cp // 2),
            grads(n_cp // 2),
            *map(grads, carried),
            like((8, HD), F32),
        ],
        compiler_params=params(1),
        cost_estimate=cost(5 * pairs * HD, 8 * seq * heads * HD, pairs),
    )(me, q_fin, d_out, out, lse, q_raw, cos_t, sin_t, q_norm, *kv_blocks, *extra)


def post_kernel(n_w, at_ref, o_ref, wmine_ref, *rest):
    w_refs = rest[:n_w]
    x_ref, dy_ref, wpost_ref = rest[n_w:n_w + 3]
    y_ref, dattn_ref, do_ref, dpost_ref, o_buf, m_buf, w_buf, attn_scr, o_sem, m_sem, w_sem = rest[-11:]
    i = pl.program_id(0)
    n_tp, _, width = o_ref.shape
    rows, dim = x_ref.shape
    cols = attn_scr.shape[2]
    steps = n_w // 2
    mine = pltpu.make_async_copy(wmine_ref, m_buf, m_sem.at[0])

    def weight_copies(pair, par):
        to = [w_buf.at[par, :, pl.ds(j * cols, cols)] for j in range(2)]
        return [pltpu.make_async_copy(w_refs[2 * pair + j], to[j], w_sem.at[par, j]) for j in range(2)]

    @pl.when(i == 0)
    def _():
        copies = [
            pltpu.make_async_copy(o_ref.at[t], o_buf.at[:, pl.ds(t * width, width)], o_sem.at[t]) for t in range(n_tp)
        ]
        for copy in copies + weight_copies(0, 0):
            copy.start()
        for copy in copies:
            copy.wait()

    @pl.when(i == 1)
    def _():
        mine.start()

    for pair in range(1, steps):

        @pl.when(i == pair - 1)
        def _():
            for copy in weight_copies(pair, pair % 2):
                copy.start()

    @pl.when(i < steps)
    def _():
        par = lax.rem(i, 2)
        for copy in weight_copies(0, par):
            copy.wait()
        both = dot(o_buf[:], w_buf[par])
        for j in range(2):
            attn_scr[jnp.bitwise_xor(at_ref[0], 2 * i + j)] = both[:, j * cols:(j + 1) * cols]

    @pl.when(i == steps)
    def _():
        dpost_ref[:] = jnp.zeros(dpost_ref.shape, F32)
        mine.wait()

    @pl.when(i >= steps)
    def _():
        tiles = [(s, t * HD, slice(s * cols + t * HD, s * cols + (t + 1) * HD)) for s in range(n_w) for t in range(cols // HD)]
        sub = min(64, rows)

        def some_rows(r, carry):
            here = pl.ds(pl.multiple_of(r * sub, sub), sub)
            there = pl.ds(pl.multiple_of((i - steps) * rows + r * sub, sub), sub)
            square = jnp.zeros((sub, HD), F32)
            cross = jnp.zeros((sub, HD), F32)
            for s, t, at in tiles:
                attn = attn_scr[s, there, t:t + HD]
                square += attn * attn
                cross += attn * (dy_ref[here, at].astype(F32) * (1.0 + wpost_ref[:, at]))
            inv = inv_rms(square, dim)
            shrink = inv * inv * inv * (row_sum(cross) * (1.0 / dim))
            for s, t, at in tiles:
                attn = attn_scr[s, there, t:t + HD]
                gain = 1.0 + wpost_ref[:, at]
                dy = dy_ref[here, at].astype(F32)
                unit = attn * inv
                y_ref[here, at] = (x_ref[here, at].astype(F32) + unit * gain).astype(BF16)
                dpost_ref[:, at] += jnp.sum((dy * unit).reshape(sub // 8, 8, HD), axis=0)
                dattn_ref[here, at] = (inv * (dy * gain) - attn * shrink).astype(BF16)
            return carry

        lax.fori_loop(0, rows // sub, some_rows, 0)
        d_out = dot(dattn_ref[:], m_buf[:], NT)
        for h in range(do_ref.shape[0]):
            do_ref[h] = d_out[:, h * HD:(h + 1) * HD].astype(BF16)


def post(half, at, out_all, w_all, w_mine, x, dy, w_post, y=None):
    n_tp, chunk, width = out_all.shape
    seq, dim = x.shape
    rows = min(256, chunk)
    heads = width // HD
    n_w = len(w_all)
    n = chunk // rows
    steps = n_w // 2
    block = lambda i: jnp.maximum(i - steps, 0)
    row = rows_of(rows, dim, lambda i: half * n + block(i))
    extra = () if y is None else (y,)
    grid_spec = pltpu.PrefetchScalarGridSpec(
        num_scalar_prefetch=1,
        grid=(steps + n,),
        in_specs=anywhere(2 + n_w) + [row, row, whole((1, dim))] + anywhere(len(extra)),
        out_specs=[
            row,
            rows_of(rows, dim, block),
            pl.BlockSpec((heads, rows, HD), lambda i, *_: (0, block(i), 0)),
            whole((8, dim)),
        ],
        scratch_shapes=[
            pltpu.VMEM((chunk, n_tp * width), BF16),
            pltpu.VMEM(w_mine.shape, BF16),
            pltpu.VMEM((2, n_tp * width, dim // steps), BF16),
            pltpu.VMEM((n_w, chunk, dim // n_w), F32),
            pltpu.SemaphoreType.DMA((n_tp,)),
            pltpu.SemaphoreType.DMA((1,)),
            pltpu.SemaphoreType.DMA((2, 2)),
        ],
    )
    return pl.pallas_call(
        functools.partial(post_kernel, n_w),
        grid_spec=grid_spec,
        out_shape=[like((seq, dim), BF16), like((chunk, dim), BF16), like((heads, chunk, HD), BF16), like((8, dim), F32)],
        input_output_aliases={n_w + 6: 0} if extra else {},
        compiler_params=params(1),
        cost_estimate=cost(chunk * dim * width * (n_tp + 1), dim * (4 * chunk + width * n_tp)),
    )(at, out_all, w_mine, *w_all, x, dy, w_post, *extra)


def dwo_kernel(core_ref, o_ref, *refs):
    d_refs, (give_ref, keep_ref) = refs[:2], refs[2:]
    half = give_ref.shape[0]
    for ref, core in ((give_ref, 1 - core_ref[0]), (keep_ref, core_ref[0])):
        span = pl.ds(pl.multiple_of(core * half, HD), half)
        ref[:] = sum(dot(o_ref[j, :, span], d_refs[j][:], TN) for j in range(2))


def out_weight_grad(core, out, d_attn, cols=512):
    _, chunk, width = out.shape
    dim = d_attn[0].shape[1]
    tile = lambda n: pl.BlockSpec((n, cols), lambda i, *_: (0, i))
    sums = like((width // 2, dim), F32)
    grid_spec = pltpu.PrefetchScalarGridSpec(
        num_scalar_prefetch=1,
        grid=(dim // cols,),
        in_specs=[fixed(out.shape), tile(chunk), tile(chunk)],
        out_specs=[tile(width // 2), tile(width // 2)],
    )
    return pl.pallas_call(
        dwo_kernel,
        name="dwo",
        grid_spec=grid_spec,
        out_shape=[sums, sums],
        compiler_params=params(1),
        cost_estimate=cost(2 * chunk * dim * width, 2 * dim * (width + chunk)),
    )(core, out, *d_attn)


def kback_kernel(own_ref, near_ref, far_ref, kraw_ref, cos_ref, sin_ref, kn_ref, out_ref, gain_ref):
    @pl.when(pl.program_id(0) == 0)
    def _():
        gain_ref[:] = jnp.zeros(gain_ref.shape, F32)

    kv_heads = own_ref.shape[2]
    for h in range(kv_heads):
        cols = slice(h * HD, (h + 1) * HD)
        d_k = own_ref[0, 0, h] + near_ref[0, 0, h] + far_ref[0, h]
        d_raw, d_gain = norm_rope_back(d_k, kraw_ref[:, cols], kn_ref[:], cos_ref[:], sin_ref[:])
        out_ref[:, cols] = d_raw
        gain_ref[0:1, :] += d_gain
        d_v = own_ref[0, 1, h] + near_ref[0, 1, h] + far_ref[1, h]
        out_ref[:, (kv_heads + h) * HD:(kv_heads + h + 1) * HD] = d_v.astype(BF16)


def key_back(half, own, near, far, k_raw, cos_t, sin_t, k_norm):
    _, _, kv_heads, chunk, _ = own.shape
    rows = min(256, chunk)
    n = chunk // rows
    two = pl.BlockSpec((1, 2, kv_heads, rows, HD), lambda i: (0, 0, 0, i, 0))
    row = lambda cols: rows_of(rows, cols, lambda i: half * n + i)
    return pl.pallas_call(
        kback_kernel,
        grid=(n,),
        in_specs=[
            two,
            two,
            pl.BlockSpec((2, kv_heads, rows, HD), lambda i: (0, 0, i, 0)),
            row(kv_heads * HD),
            row(HD),
            row(HD),
            whole((1, HD)),
        ],
        out_specs=[rows_of(rows, 2 * kv_heads * HD), whole((8, HD))],
        out_shape=[
            like((chunk, 2 * kv_heads * HD), BF16),
            like((8, HD), F32),
        ],
        compiler_params=params(1),
        cost_estimate=cost(32 * chunk * kv_heads * HD, 8 * chunk * kv_heads * HD),
    )(own, near, far, k_raw, cos_t, sin_t, k_norm)


def dx_kernel(n_tp, n_w, at_ref, *refs):
    g_refs, w_refs, refs = refs[:n_tp], refs[n_tp:n_tp + n_w], refs[n_tp + n_w:]
    x_ref, dy_ref, wpre_ref, dx_ref, dpre_ref, g_scr, w_buf, acc, sem = refs
    i = pl.program_id(0)
    rows, width = g_refs[0].shape
    cols = acc.shape[2]

    def weight_copies(pair, par):
        return [pltpu.make_async_copy(w_refs[2 * pair + j], w_buf.at[par, :, j], sem.at[par, j]) for j in range(2)]

    @pl.when(i == 0)
    def _():
        for copy in weight_copies(0, 0):
            copy.start()
        for s in range(n_tp):
            g_scr[lax.rem(at_ref[1] + n_tp - s, n_tp)] = g_refs[s][:]

    for pair in range(1, n_w // 2):

        @pl.when(i == pair - 1)
        def _():
            for copy in weight_copies(pair, pair % 2):
                copy.start()

    par = lax.rem(i, 2)
    for copy in weight_copies(0, par):
        copy.wait()
    total = sum(dot(w_buf[par, t].reshape(2 * cols, width), g_scr[t], NT) for t in range(n_tp))
    total = jnp.transpose(total)
    for j in range(2):
        acc[jnp.bitwise_xor(at_ref[0], 2 * i + j)] = total[:, j * cols:(j + 1) * cols]

    @pl.when(i == pl.num_programs(0) - 1)
    def _():
        dpre_ref[:] = jnp.zeros(dpre_ref.shape, F32)
        tiles = [(s, t, slice(s * cols + t, s * cols + t + HD)) for s in range(n_w) for t in range(0, cols, HD)]
        dim = n_w * cols
        sub = min(64, rows)

        def some_rows(r, carry):
            here = pl.ds(pl.multiple_of(r * sub, sub), sub)
            square = jnp.zeros((sub, HD), F32)
            cross = jnp.zeros((sub, HD), F32)
            for s, t, at in tiles:
                x = x_ref[here, at].astype(F32)
                square += x * x
                cross += x * (acc[s, here, t:t + HD] * (1.0 + wpre_ref[:, at]))
            inv = inv_rms(square, dim)
            shrink = inv * inv * inv * (row_sum(cross) * (1.0 / dim))
            for s, t, at in tiles:
                x = x_ref[here, at].astype(F32)
                d_normed = acc[s, here, t:t + HD]
                dpre_ref[:, at] += jnp.sum((d_normed * (x * inv)).reshape(sub // 8, 8, HD), axis=0)
                d_x = inv * (d_normed * (1.0 + wpre_ref[:, at])) - x * shrink
                dx_ref[here, at] = (dy_ref[here, at].astype(F32) + d_x).astype(BF16)
            return carry

        lax.fori_loop(0, rows // sub, some_rows, 0)


def input_grad(half, at, grads, w_all, x, dy, w_pre):
    n_tp, n = len(grads), len(w_all)
    rows, width = grads[0].shape
    dim = x.shape[1]
    cols = dim // n
    here = pl.BlockSpec((rows, dim), lambda i, t: (half * n_tp + t[1], 0))
    grid_spec = pltpu.PrefetchScalarGridSpec(
        num_scalar_prefetch=1,
        grid=(n // 2,),
        in_specs=[whole((rows, width))] * n_tp + anywhere(n) + [here, here, whole((1, dim))],
        out_specs=[whole((rows, dim)), whole((8, dim))],
        scratch_shapes=[
            pltpu.VMEM((n_tp, rows, width), BF16),
            pltpu.VMEM((2, n_tp, 2, cols, width), BF16),
            pltpu.VMEM((n, rows, cols), F32),
            pltpu.SemaphoreType.DMA((2, 2)),
        ],
    )
    return pl.pallas_call(
        functools.partial(dx_kernel, n_tp, n),
        grid_spec=grid_spec,
        out_shape=[like((rows, dim), BF16), like((8, dim), F32)],
        compiler_params=params(1),
        cost_estimate=cost(n_tp * rows * width * dim, n_tp * width * dim),
    )(at, *grads, *w_all, x, dy, w_pre)


def dw_kernel(n_cp, me_ref, *refs):
    g_refs, n_refs = refs[:2 * n_cp], refs[2 * n_cp:-7]
    dwq_ref, dwk_ref, dwv_ref, n_buf, g_buf, n_sem, g_sem = refs[-7:]
    i = pl.program_id(0)
    cols = n_buf.shape[3]
    chunk, width = g_refs[0].shape
    me = me_ref[0]

    def place(refs_in, buf, sem):
        copies = []
        for j, (ref, shape) in enumerate(refs_in):
            start = sum(r[1] for r in refs_in[:j - j % n_cp:n_cp])
            to = buf.at[jnp.bitwise_xor(me, j % n_cp), pl.ds(start, shape)]
            copies.append(pltpu.make_async_copy(ref, to, sem.at[j]))
        return copies

    def fetch(step, par):
        span = pl.ds(pl.multiple_of(step * cols, cols), cols)
        return place([(r.at[:, span], r.shape[0]) for r in n_refs], n_buf.at[par], n_sem.at[par])

    @pl.when(i == 0)
    def _():
        grads = place([(r, chunk) for r in g_refs], g_buf, g_sem)
        for copy in fetch(0, 0) + grads:
            copy.start()
        for copy in grads:
            copy.wait()

    @pl.when(i + 1 < pl.num_programs(0))
    def _():
        for copy in fetch(i + 1, (i + 1) % 2):
            copy.start()

    for copy in fetch(i, i % 2):
        copy.wait()
    seq = 2 * chunk
    grad = dot(n_buf[i % 2].reshape(n_cp * seq, cols), g_buf[:].reshape(n_cp * seq, width), TN)
    q_width, kv_width = dwq_ref.shape[1], dwk_ref.shape[1]
    dwq_ref[:] = grad[:, :q_width]
    dwk_ref[:] = grad[:, q_width:q_width + kv_width]
    dwv_ref[:] = grad[:, q_width + kv_width:]


def weight_grads(me, normed, grads, q_width, cols=256):
    n_cp = len(grads) // 2
    chunk, width = grads[0].shape
    dim = normed[0].shape[1]
    kv_width = (width - q_width) // 2
    tile = lambda n: rows_of(cols, n)
    grid_spec = pltpu.PrefetchScalarGridSpec(
        num_scalar_prefetch=1,
        grid=(dim // cols,),
        in_specs=anywhere(len(grads) + len(normed)),
        out_specs=[tile(q_width), tile(kv_width), tile(kv_width)],
        scratch_shapes=[
            pltpu.VMEM((2, n_cp, 2 * chunk, cols), BF16),
            pltpu.VMEM((n_cp, 2 * chunk, width), BF16),
            pltpu.SemaphoreType.DMA((2, len(normed))),
            pltpu.SemaphoreType.DMA((len(grads),)),
        ],
    )
    return pl.pallas_call(
        functools.partial(dw_kernel, n_cp),
        name="dw",
        grid_spec=grid_spec,
        out_shape=[like((dim, n), F32) for n in (q_width, kv_width, kv_width)],
        compiler_params=params(1),
        cost_estimate=cost(2 * n_cp * chunk * dim * width, 2 * n_cp * chunk * (dim + width)),
    )(me, *grads, *normed)


def join_kernel(core_ref, keep_ref, other_ref, *rest):
    half = pl.program_id(0)

    @pl.when(half == core_ref[0])
    def _():
        rest[-1][:] = keep_ref[:]

    @pl.when(half != core_ref[0])
    def _():
        rest[-1][:] = other_ref[:]


def join_halves(core, keep, other, start, half, total=None):
    block, width = HD, keep.shape[1]
    n = keep.shape[0] // block
    extra = () if total is None else (total,)
    part = pl.BlockSpec((block, width), lambda i, j, c: (j, 0))
    grid_spec = pltpu.PrefetchScalarGridSpec(
        num_scalar_prefetch=1,
        grid=(2, n),
        in_specs=[part, part] + anywhere(len(extra)),
        out_specs=pl.BlockSpec((block, width), lambda i, j, c: (i * (half // block) + start // block + j, 0)),
    )
    return pl.pallas_call(
        join_kernel,
        name="join",
        grid_spec=grid_spec,
        out_shape=like((2 * half, width), F32),
        input_output_aliases={3: 0} if extra else {},
        compiler_params=params(2),
        cost_estimate=cost(n * block * width, 8 * n * block * width),
    )(core, keep, other, *extra)


def solution(mesh):
    n_cp, n_tp, n_dp = mesh.shape["cp"], mesh.shape["tp"], mesh.shape["dp"]
    near = [(i, i ^ 1) for i in range(n_cp)]
    across = [(i, i ^ 2) for i in range(n_cp)]
    beside = [(i, i ^ 1) for i in range(n_dp)]

    def from_cp(value):
        far = lax.ppermute(value, "cp", across)
        return [value, lax.ppermute(value, "cp", near), far, lax.ppermute(far, "cp", near)]

    def per_device(hidden, cotangent, pos_loc, w_q, w_k, w_v, w_o, w_pre, w_post, q_norm, k_norm):
        _, seq, dim = hidden.shape
        x, dy = hidden[0], cotangent[0]
        kv_heads = w_k.shape[1] // HD
        cp, tp, dp = (lax.axis_index(a).astype(jnp.int32) for a in ("cp", "tp", "dp"))
        core = cp % 2
        me, one_core = cp.reshape(1), core.reshape(1)

        share = dp * n_cp + cp
        shares = n_dp * n_cp
        cols = dim // shares

        def over_tp(part):
            return lax.all_gather(part, "tp", axis=0, tiled=True)

        def spread(own):
            blocks = from_cp(own)
            if n_dp == 2:
                for value in (own, blocks[2]):
                    other = lax.ppermute(value, "dp", beside)
                    blocks += [other, lax.ppermute(other, "cp", near)]
            return blocks

        w_o_all = spread(over_tp(lax.dynamic_slice_in_dim(w_o, share * cols, cols, 1)))
        w_in = jnp.concatenate([lax.dynamic_slice_in_dim(w, share * cols, cols, 0) for w in (w_q, w_k, w_v)], axis=1)
        w_in_all = spread(over_tp(w_in).reshape(n_tp, cols, w_in.shape[1]))

        cos_t, sin_t = rope_tables(pos_loc)
        qn, kn = q_norm.reshape(1, HD), k_norm.reshape(1, HD)
        wpre, wpost = w_pre.reshape(1, dim), w_post.reshape(1, dim)
        rows = seq // 4
        x_far = lax.ppermute(x[:rows], "cp", across)
        *normed, kv_own, k_raw = project_kv(x, wpre, w_k, w_v, kn, cos_t, sin_t, rows, (1, 1, 2))
        kv_blocks = from_cp(kv_own)
        q_fin, q_raw = project_q(normed, w_q, qn, cos_t, sin_t, rows)
        far = norm_rows(x_far, wpre)
        normed_all = [normed[0], lax.ppermute(normed[0], "cp", near), far, lax.ppermute(far, "cp", near)]
        normed_all += from_cp(normed[1]) + from_cp(normed[2])
        out, lse = attention_fwd(me, q_fin, kv_blocks, kv_heads)

        out_all = [None, None]
        for half in (1, 0):
            out_all[half] = lax.all_gather(out[half], "tp", axis=0, tiled=False)
        at = jnp.stack([share, core])

        low, dq, d_attn, d_post, gains, carried, y = [], [None] * 2, [None] * 2, [], [], [None] * 2, None
        for half in (1, 0):
            y, d_attn[half], d_out, part = post(half, at, out_all[half], w_o_all, w_o, x, dy, wpost, y)
            d_post.append(part)
            dq[half], kept, sent, *low, gain = attention_bwd(
                half, me, q_fin, d_out, out, lse, q_raw, cos_t, sin_t, qn, kv_blocks, kv_heads, *low
            )
            gains.append(gain[0])
            got = lax.ppermute(sent, "cp", near)
            carried[half] = (kept, got, lax.ppermute(kept[1] + got[1], "cp", across))

        give, keep = out_weight_grad(one_core, out, d_attn)
        got = lax.ppermute(give, "cp", near)
        rows = keep.shape[0]
        d_wo = None
        for start, stop in ((0, rows - HD), (rows - HD, rows)):
            mine_part = keep[start:stop] + got[start:stop]
            mine_part = mine_part + lax.ppermute(mine_part, "cp", across)
            other = lax.ppermute(mine_part, "cp", near)
            d_wo = join_halves(one_core, mine_part, other, start, rows, d_wo)

        rows = seq // 2 // n_tp
        at_tp = jnp.stack([share, tp])
        grads, d_hidden, d_pre = [None] * 2, [None] * 2, []
        for half in (1, 0):
            d_kv, gain = key_back(half, *carried[half], k_raw, cos_t, sin_t, kn)
            gains.append(gain[0])
            g = grads[half] = jnp.concatenate([dq[half], d_kv], axis=1)
            pieces = [lax.dynamic_slice_in_dim(g, tp * rows, rows, 0)]
            for s in range(1, n_tp):
                part = lax.dynamic_slice_in_dim(g, ((tp + s) % n_tp) * rows, rows, 0)
                pieces.append(lax.ppermute(part, "tp", [(i, (i + s) % n_tp) for i in range(n_tp)]))
            dx_rows, part = input_grad(half, at_tp, pieces, w_in_all, x, dy, wpre)
            d_pre.append(part)
            d_hidden[half] = lax.all_gather(dx_rows, "tp", axis=0, tiled=True)
        d_hidden = jnp.concatenate(d_hidden, axis=0)

        grads_all = from_cp(grads[0]) + from_cp(grads[1])
        d_wq, d_wk, d_wv = weight_grads(me, normed_all, grads_all, w_q.shape[1])

        d_post, d_pre = jnp.sum(sum(d_post), axis=0), jnp.sum(sum(d_pre), axis=0)
        small = jnp.concatenate([jnp.where(tp == 0, d_post, 0.0), d_pre, sum(gains[:2]), sum(gains[2:])])
        small = small + lax.ppermute(small, "cp", near)
        small = small + lax.ppermute(small, "cp", across)
        small = small + lax.ppermute(small, "tp", [(i, i ^ 1) for i in range(n_tp)])
        small = small + lax.ppermute(small, "tp", [(i, i ^ 2) for i in range(n_tp)])
        d_post, d_pre, d_qn, d_kn = jnp.split(small, np.cumsum([dim, dim, HD]))
        return y[None], d_hidden[None], d_wq, d_wk, d_wv, d_wo, d_pre, d_post, d_qn, d_kn

    rows, cols, all_of = P('dp', 'cp'), P(None, 'tp'), P()
    specs_in = (rows, rows, P(('dp', 'cp')), cols, cols, cols, P('tp'), all_of, all_of, all_of, all_of)
    grid, by_dp = P('dp', 'tp'), P('dp')
    specs_out = (rows, rows, grid, grid, grid, P(('dp', 'tp')), by_dp, by_dp, by_dp, by_dp)
    return jax.shard_map(per_device, mesh=mesh, in_specs=specs_in, out_specs=specs_out, check_vma=False)
```

```python
import functools

import jax
import jax.numpy as jnp
import numpy as np
from jax import lax
from jax.experimental import pallas as pl
from jax.experimental.pallas import tpu as pltpu
from jax.sharding import PartitionSpec as P


EPS = 1e-6
ROPE_BASE = 1000000.0
ROPE_SCALE = 8.0
NEG_BIG = -1e30
LOG2E = 1.4426950408889634
HD = 128
F32 = jnp.float32
BF16 = jnp.bfloat16
VMEM_MAX = 62914560
NT = (((1,), (1,)), ((), ()))
TN = (((0,), (0,)), ((), ()))


def dot(a, b, dims=(((1,), (0,)), ((), ()))):
    return lax.dot_general(a, b, dims, preferred_element_type=F32)


def params(dims, vmem=VMEM_MAX):
    return pltpu.CompilerParams(dimension_semantics=("arbitrary",) * dims, vmem_limit_bytes=vmem)


def cost(products, values, trans=0):
    return pl.CostEstimate(flops=2 * products, bytes_accessed=2 * values, transcendentals=trans)


def row_sum(values):
    return jnp.sum(values, axis=1, keepdims=True)


def inv_rms(square, dim):
    return lax.rsqrt(row_sum(square) * (1.0 / dim) + EPS)


def whole(shape):
    return pl.BlockSpec(shape, lambda *_: (0,) * len(shape))


def fixed(shape):
    return pl.BlockSpec(shape, lambda *_: (0,) * len(shape), pipeline_mode=pl.Buffered(buffer_count=1))


def rows_of(rows, cols, at=lambda i: i):
    return pl.BlockSpec((rows, cols), lambda i, *_: (at(i), 0))


def anywhere(n):
    return [pl.BlockSpec(memory_space=pl.ANY)] * n


def like(shape, dtype):
    return jax.ShapeDtypeStruct(shape, dtype)


def rope_tables(pos_loc):
    half_dim = HD // 2
    inv_freq = 1.0 / (ROPE_SCALE * ROPE_BASE ** (jnp.arange(half_dim, dtype=F32) * (2.0 / HD)))
    angles = pos_loc.astype(F32)[:, None] * inv_freq[None, :]
    cos_t, sin_t = jnp.cos(angles), jnp.sin(angles)
    return jnp.concatenate([cos_t, cos_t], axis=-1), jnp.concatenate([-sin_t, sin_t], axis=-1)


def norm_rope(raw, gain, cos_t, sin_t):
    raw = raw.astype(F32)
    unit = raw * inv_rms(raw * raw, HD)
    scaled = unit * (1.0 + gain)
    return (scaled * cos_t + pltpu.roll(scaled, HD // 2, 1) * sin_t).astype(BF16)


def norm_rope_back(d_final, raw, gain, cos_t, sin_t):
    raw = raw.astype(F32)
    inv = inv_rms(raw * raw, HD)
    unit = raw * inv
    d_scaled = d_final * cos_t - pltpu.roll(d_final, HD // 2, 1) * sin_t
    d_gain = jnp.sum(d_scaled * unit, axis=0, keepdims=True)
    d_unit = d_scaled * (1.0 + gain)
    d_raw = inv * (d_unit - unit * (row_sum(d_unit * unit) * (1.0 / HD)))
    return d_raw.astype(BF16), d_gain


def normalise(x_ref, wpre_ref, write):
    rows, dim = x_ref.shape
    tiles = [slice(t, t + HD) for t in range(0, dim, HD)]
    sub = min(64, rows)

    def some_rows(r, carry):
        here = pl.ds(pl.multiple_of(r * sub, sub), sub)
        square = jnp.zeros((sub, HD), F32)
        for at in tiles:
            x = x_ref[here, at].astype(F32)
            square += x * x
        inv = inv_rms(square, dim)
        for at in tiles:
            write(here, at, (x_ref[here, at].astype(F32) * inv * (1.0 + wpre_ref[:, at])).astype(BF16))
        return carry

    lax.fori_loop(0, rows // sub, some_rows, 0)


def norm_kernel(x_ref, wpre_ref, out_ref):
    def write(rows, cols, value):
        out_ref[rows, cols] = value

    normalise(x_ref, wpre_ref, write)


def norm_rows(x, w_pre):
    return pl.pallas_call(
        norm_kernel,
        name="norm",
        grid=(1,),
        in_specs=[whole(x.shape), whole(w_pre.shape)],
        out_specs=whole(x.shape),
        out_shape=like(x.shape, BF16),
        compiler_params=params(1),
        cost_estimate=cost(4 * x.shape[0] * x.shape[1], 2 * x.shape[0] * x.shape[1]),
    )(x, w_pre)


def kv_kernel(parts, x_ref, wpre_ref, wk_ref, wv_ref, kn_ref, cos_ref, sin_ref, *rest):
    n = len(parts)
    out_refs, (kv_ref, kraw_ref, buf, sem) = rest[:n], rest[n:]
    i = pl.program_id(0)
    rows = x_ref.shape[0]
    par = i % 2
    steps = [(j, step) for j, size in enumerate(parts) for step in range(size)]

    def out_copy(step):
        j, at = steps[step]
        return pltpu.make_async_copy(buf.at[step % 2], out_refs[j].at[pl.ds(at * rows, rows)], sem.at[step % 2])

    for step in range(2, len(steps)):

        @pl.when(i == step)
        def _():
            out_copy(step - 2).wait()

    def write(here, cols, value):
        buf[par, here, cols] = value

    normalise(x_ref, wpre_ref, write)
    for step in range(len(steps)):

        @pl.when(i == step)
        def _():
            out_copy(step).start()

    normed = buf[par]
    k_raw = dot(normed, wk_ref[:]).astype(BF16)
    kraw_ref[:] = k_raw
    width = k_raw.shape[1]
    for h in range(width // HD):
        cols = slice(h * HD, (h + 1) * HD)
        kv_ref[:, cols] = norm_rope(k_raw[:, cols], kn_ref[:], cos_ref[:], sin_ref[:])
    kv_ref[:, width:] = dot(normed, wv_ref[:]).astype(BF16)

    @pl.when(i == len(steps) - 1)
    def _():
        for step in range(len(steps))[-2:]:
            out_copy(step).wait()


def project_kv(x, w_pre, w_k, w_v, k_norm, cos_t, sin_t, rows, parts):
    seq, dim = x.shape
    width = w_k.shape[1]
    grid_spec = pl.GridSpec(
        grid=(seq // rows,),
        in_specs=[rows_of(rows, dim), whole((1, dim)), fixed(w_k.shape), fixed(w_v.shape), whole((1, HD))]
        + [rows_of(rows, HD)] * 2,
        out_specs=anywhere(len(parts)) + [rows_of(rows, 2 * width), rows_of(rows, width)],
        scratch_shapes=[pltpu.VMEM((2, rows, dim), BF16), pltpu.SemaphoreType.DMA((2,))],
    )
    return pl.pallas_call(
        functools.partial(kv_kernel, parts),
        name="pkv",
        grid_spec=grid_spec,
        out_shape=[like((n * rows, dim), BF16) for n in parts] + [like((seq, 2 * width), BF16), like((seq, width), BF16)],
        compiler_params=params(1),
        cost_estimate=cost(2 * seq * dim * width, 2 * dim * (seq + width)),
    )(x, w_pre, w_k, w_v, k_norm, cos_t, sin_t)


def q_kernel(starts, *refs):
    n_refs, (wq_ref, qn_ref, cos_ref, sin_ref, qfin_ref, qraw_ref) = refs[:len(starts)], refs[len(starts):]
    normed = n_refs[0][:]
    for start, ref in zip(starts[1:], n_refs[1:]):
        normed = jnp.where(pl.program_id(0) >= start, ref[:], normed)
    q_raw = dot(normed, wq_ref[:]).astype(BF16)
    for h in range(qfin_ref.shape[0]):
        part = q_raw[:, h * HD:(h + 1) * HD]
        qraw_ref[h] = part
        qfin_ref[h] = norm_rope(part, qn_ref[:], cos_ref[:], sin_ref[:])


def project_q(normed, w_q, q_norm, cos_t, sin_t, rows):
    dim, width = w_q.shape
    sizes = [part.shape[0] // rows for part in normed]
    starts = [sum(sizes[:j]) for j in range(len(sizes))]
    n = sum(sizes)
    heads = width // HD
    block = lambda start, size: rows_of(rows, dim, lambda i: jnp.clip(i - start, 0, size - 1))
    head_rows = pl.BlockSpec((heads, rows, HD), lambda i: (0, i, 0))
    shape = like((heads, n * rows, HD), BF16)
    return pl.pallas_call(
        functools.partial(q_kernel, starts),
        name="pq",
        grid=(n,),
        in_specs=list(map(block, starts, sizes)) + [fixed(w_q.shape), whole((1, HD))] + [rows_of(rows, HD)] * 2,
        out_specs=[head_rows, head_rows],
        out_shape=[shape, shape],
        compiler_params=params(1),
        cost_estimate=cost(n * rows * dim * width, dim * (n * rows + width)),
    )(*normed, w_q, q_norm, cos_t, sin_t)


def load_kv(kv_refs, k_buf, v_buf, sems, heads):
    kv_heads = kv_refs[0].shape[1] // (2 * HD)
    copies = []
    for s, ref in enumerate(kv_refs):
        for i, h in enumerate(heads):
            for t, buf in enumerate((k_buf, v_buf)):
                src = ref.at[:, pl.ds((t * kv_heads + h) * HD, HD)]
                copies.append(pltpu.make_async_copy(src, buf.at[i, s], sems.at[s, i, t]))
    for copy in copies:
        copy.start()
    for copy in copies:
        copy.wait()


def piece_place(piece, me, n_cp):
    upper = piece >= n_cp
    owner = jnp.where(upper, 2 * n_cp - 1 - piece, piece)
    return jnp.bitwise_xor(owner, me), upper.astype(jnp.int32)


def fwd_kernel(n_cp, me_ref, q_ref, *rest):
    kv_refs = rest[:n_cp]
    o_ref, lse_ref, k_buf, v_buf, m_scr, acc_scr, sems = rest[n_cp:]
    h, half = pl.program_id(0), pl.program_id(1)
    groups, rows, _ = q_ref.shape

    @pl.when((h == 0) & (half == 0))
    def _():
        load_kv(kv_refs, k_buf, v_buf, sems, range(k_buf.shape[0]))

    me = me_ref[0]
    piece = jnp.where(half == 0, me, 2 * n_cp - 1 - me)
    scale = HD ** -0.5 * LOG2E
    m_scr[:] = jnp.full(m_scr.shape, NEG_BIG, F32)
    acc_scr[:] = jnp.zeros(acc_scr.shape, F32)

    def block(j, masked):
        slot, upper = piece_place(j, me, n_cp)
        span = pl.ds(pl.multiple_of(upper * rows, rows), rows)
        k = k_buf[h, slot, span, :]
        v_ext = jnp.concatenate([v_buf[h, slot, span, :], jnp.ones((rows, HD), BF16)], axis=1)
        scores = [dot(q_ref[g], k, NT) * scale for g in range(groups)]
        for g in range(groups):
            s = scores[g]
            if masked:
                q_pos = lax.broadcasted_iota(jnp.int32, s.shape, 0)
                k_pos = lax.broadcasted_iota(jnp.int32, s.shape, 1)
                s = jnp.where(k_pos <= q_pos, s, NEG_BIG)
            m_old = m_scr[g]
            m_new = jnp.maximum(m_old, jnp.max(s, axis=1, keepdims=True))
            alpha = jnp.exp2(m_old - m_new)
            p = jnp.exp2(s - jnp.concatenate([m_new] * (rows // HD), axis=1)).astype(BF16)
            acc_scr[g] = acc_scr[g] * jnp.concatenate([alpha, alpha], axis=1) + dot(p, v_ext)
            m_scr[g] = m_new

    def full(j, carry):
        block(j, False)
        return carry

    lax.fori_loop(0, piece, full, 0)
    block(piece, True)
    for g in range(groups):
        l = acc_scr[g, :, HD:]
        o_ref[0, :, g * HD:(g + 1) * HD] = (acc_scr[g, :, :HD] / l).astype(BF16)
        lse_ref[0, g:g + 1, :] = jnp.transpose(m_scr[g] + jnp.log2(l))[0:1, :]


def attention_fwd(me, q_fin, kv_blocks, kv_heads):
    heads, seq, _ = q_fin.shape
    n_cp = len(kv_blocks)
    groups = heads // kv_heads
    rows = seq // 2
    grid_spec = pltpu.PrefetchScalarGridSpec(
        num_scalar_prefetch=1,
        grid=(kv_heads, 2),
        in_specs=[pl.BlockSpec((groups, rows, HD), lambda h, i, *_: (h, i, 0))] + anywhere(n_cp),
        out_specs=[
            pl.BlockSpec((1, rows, groups * HD), lambda h, i, *_: (i, 0, h)),
            pl.BlockSpec((1, 8, rows), lambda h, i, *_: (h, 0, i)),
        ],
        scratch_shapes=[
            pltpu.VMEM((kv_heads, n_cp, seq, HD), BF16),
            pltpu.VMEM((kv_heads, n_cp, seq, HD), BF16),
            pltpu.VMEM((groups, rows, HD), F32),
            pltpu.VMEM((groups, rows, 2 * HD), F32),
            pltpu.SemaphoreType.DMA((n_cp, kv_heads, 2)),
        ],
    )
    pairs = heads * rows * rows * (2 * n_cp + 1)
    return pl.pallas_call(
        functools.partial(fwd_kernel, n_cp),
        name="fwd",
        grid_spec=grid_spec,
        out_shape=[
            like((2, rows, heads * HD), BF16),
            like((kv_heads, 8, seq), F32),
        ],
        compiler_params=params(2),
        cost_estimate=cost(2 * pairs * HD, 4 * seq * heads * HD, pairs),
    )(me, q_fin, *kv_blocks)


def bwd_kernel(n_cp, half, me_ref, q_ref, do_ref, o_ref, lse_ref, qraw_ref, cos_ref, sin_ref, qn_ref, *rest):
    kv_refs, rest = rest[:n_cp], rest[n_cp:]
    if half:
        dq_ref, keep_ref, send_ref, low_ref, gain_ref = rest[:5]
    else:
        low_ref, dq_ref, keep_ref, send_ref, gain_ref = rest[:5]
    k_buf, v_buf, dq_scr, dkv_scr, sems = rest[5:]
    h = pl.program_id(0)
    groups, rows, _ = q_ref.shape
    two = n_cp // 2

    @pl.when(h == 0)
    def _():
        load_kv(kv_refs, k_buf, v_buf, sems, range(k_buf.shape[0]))
        gain_ref[:] = jnp.zeros(gain_ref.shape, F32)

    if half:
        dkv_scr[:] = jnp.zeros(dkv_scr.shape, F32)
    else:
        dkv_scr[:] = low_ref[:, :, 0]

    me = me_ref[0]
    piece = 2 * n_cp - 1 - me if half else me
    scale = HD ** -0.5
    delta = []
    for g in range(groups):
        prod = do_ref[g].astype(F32) * o_ref[0, :, g * HD:(g + 1) * HD].astype(F32)
        column = jnp.broadcast_to(row_sum(prod), (rows, HD))
        delta.append(jnp.transpose(column)[0:1, :])
    dq_scr[:] = jnp.zeros(dq_scr.shape, F32)

    def block(j, masked):
        slot, upper = piece_place(j, me, n_cp)
        span = pl.ds(pl.multiple_of(upper * rows, rows), rows)
        k = k_buf[h, slot, span, :]
        v = v_buf[h, slot, span, :]
        probs, d_scores = [], []
        for g in range(groups):
            s = dot(k, q_ref[g], NT)
            p = jnp.exp2(s * (scale * LOG2E) - lse_ref[0, g:g + 1, :])
            if masked:
                k_pos = lax.broadcasted_iota(jnp.int32, s.shape, 0)
                q_pos = lax.broadcasted_iota(jnp.int32, s.shape, 1)
                p = jnp.where(k_pos <= q_pos, p, 0.0)
            probs.append(p.astype(BF16))
            d_scores.append((p * (dot(v, do_ref[g], NT) - delta[g])).astype(BF16))
        for g in range(groups):
            dq_scr[g] += dot(d_scores[g], k, TN)
        index = (slot % 2) * two + slot // 2
        into = span if half else pl.ds(0, rows)
        d_all = jnp.concatenate(d_scores, axis=1)
        p_all = jnp.concatenate(probs, axis=1)
        dkv_scr[index, 0, into, :] += dot(d_all, q_ref[:].reshape(groups * rows, HD)) * scale
        dkv_scr[index, 1, into, :] += dot(p_all, do_ref[:].reshape(groups * rows, HD))

    def full(j, carry):
        block(j, False)
        return carry

    lax.fori_loop(0, piece, full, 0)
    block(piece, True)
    for g in range(groups):
        d_raw, d_gain = norm_rope_back(dq_scr[g] * scale, qraw_ref[g], qn_ref[:], cos_ref[:], sin_ref[:])
        dq_ref[:, g * HD:(g + 1) * HD] = d_raw
        gain_ref[0:1, :] += d_gain
    for i in range(two):
        own = slice(rows, 2 * rows) if half else slice(0, rows)
        keep_ref[i, :, 0] = dkv_scr[i, :, own]
        send_ref[i, :, 0] = dkv_scr[two + i, :, own]
    if half:
        low_ref[:, :, 0] = dkv_scr[:, :, :rows]


def attention_bwd(half, me, q_fin, d_out, out, lse, q_raw, cos_t, sin_t, q_norm, kv_blocks, kv_heads, low=None):
    heads, seq, _ = q_fin.shape
    n_cp = len(kv_blocks)
    groups = heads // kv_heads
    rows = seq // 2
    by_head = pl.BlockSpec((groups, rows, HD), lambda h, *_: (h, half, 0))
    table = rows_of(rows, HD, lambda h: half)
    by_owner = lambda n: pl.BlockSpec((n, 2, 1, rows, HD), lambda h, *_: (0, 0, h, 0, 0))
    grads = lambda n: like((n, 2, kv_heads, rows, HD), F32)
    extra = () if low is None else (low,)
    carried = [n_cp] if half else []
    grid_spec = pltpu.PrefetchScalarGridSpec(
        num_scalar_prefetch=1,
        grid=(kv_heads,),
        in_specs=[
            by_head,
            pl.BlockSpec((groups, rows, HD), lambda h, *_: (h, 0, 0)),
            pl.BlockSpec((1, rows, groups * HD), lambda h, *_: (half, 0, h)),
            pl.BlockSpec((1, 8, rows), lambda h, *_: (h, 0, half)),
            by_head,
            table,
            table,
            whole((1, HD)),
        ]
        + anywhere(n_cp)
        + [by_owner(n_cp)] * len(extra),
        out_specs=[
            pl.BlockSpec((rows, groups * HD), lambda h, *_: (0, h)),
            by_owner(n_cp // 2),
            by_owner(n_cp // 2),
            *map(by_owner, carried),
            whole((8, HD)),
        ],
        scratch_shapes=[
            pltpu.VMEM((kv_heads, n_cp, seq, HD), BF16),
            pltpu.VMEM((kv_heads, n_cp, seq, HD), BF16),
            pltpu.VMEM((groups, rows, HD), F32),
            pltpu.VMEM((n_cp, 2, seq if half else rows, HD), F32),
            pltpu.SemaphoreType.DMA((n_cp, kv_heads, 2)),
        ],
    )
    pairs = heads * rows * rows * (n_cp + 1)
    return pl.pallas_call(
        functools.partial(bwd_kernel, n_cp, half),
        grid_spec=grid_spec,
        out_shape=[
            like((rows, heads * HD), BF16),
            grads(n_cp // 2),
            grads(n_cp // 2),
            *map(grads, carried),
            like((8, HD), F32),
        ],
        compiler_params=params(1),
        cost_estimate=cost(5 * pairs * HD, 8 * seq * heads * HD, pairs),
    )(me, q_fin, d_out, out, lse, q_raw, cos_t, sin_t, q_norm, *kv_blocks, *extra)


def post_kernel(n_w, at_ref, o_ref, wmine_ref, *rest):
    w_refs = rest[:n_w]
    x_ref, dy_ref, wpost_ref = rest[n_w:n_w + 3]
    y_ref, dattn_ref, do_ref, dpost_ref, o_buf, m_buf, w_buf, attn_scr, o_sem, m_sem, w_sem = rest[-11:]
    i = pl.program_id(0)
    n_tp, _, width = o_ref.shape
    rows, dim = x_ref.shape
    cols = attn_scr.shape[2]
    steps = n_w // 2
    mine = pltpu.make_async_copy(wmine_ref, m_buf, m_sem.at[0])

    def weight_copies(pair, at):
        to = [w_buf.at[at, :, pl.ds(j * cols, cols)] for j in range(2)]
        return [pltpu.make_async_copy(w_refs[2 * pair + j], to[j], w_sem.at[at, j]) for j in range(2)]

    @pl.when(i == 0)
    def _():
        copies = [
            pltpu.make_async_copy(o_ref.at[t], o_buf.at[:, pl.ds(t * width, width)], o_sem.at[t]) for t in range(n_tp)
        ]
        for copy in sum((weight_copies(pair, pair) for pair in range(steps)), copies) + [mine]:
            copy.start()
        for copy in copies:
            copy.wait()

    @pl.when(i < steps)
    def _():
        for copy in weight_copies(0, i):
            copy.wait()
        both = dot(o_buf[:], w_buf[i])
        for j in range(2):
            attn_scr[jnp.bitwise_xor(at_ref[0], 2 * i + j)] = both[:, j * cols:(j + 1) * cols]

    @pl.when(i == steps)
    def _():
        dpost_ref[:] = jnp.zeros(dpost_ref.shape, F32)
        mine.wait()

    @pl.when(i >= steps)
    def _():
        tiles = [(s, t * HD, slice(s * cols + t * HD, s * cols + (t + 1) * HD)) for s in range(n_w) for t in range(cols // HD)]
        sub = min(64, rows)

        def some_rows(r, carry):
            here = pl.ds(pl.multiple_of(r * sub, sub), sub)
            there = pl.ds(pl.multiple_of((i - steps) * rows + r * sub, sub), sub)
            square = jnp.zeros((sub, HD), F32)
            cross = jnp.zeros((sub, HD), F32)
            for s, t, at in tiles:
                attn = attn_scr[s, there, t:t + HD]
                square += attn * attn
                cross += attn * (dy_ref[here, at].astype(F32) * (1.0 + wpost_ref[:, at]))
            inv = inv_rms(square, dim)
            shrink = inv * inv * inv * (row_sum(cross) * (1.0 / dim))
            for s, t, at in tiles:
                attn = attn_scr[s, there, t:t + HD]
                gain = 1.0 + wpost_ref[:, at]
                dy = dy_ref[here, at].astype(F32)
                unit = attn * inv
                y_ref[here, at] = (x_ref[here, at].astype(F32) + unit * gain).astype(BF16)
                dpost_ref[:, at] += jnp.sum((dy * unit).reshape(sub // 8, 8, HD), axis=0)
                dattn_ref[here, at] = (inv * (dy * gain) - attn * shrink).astype(BF16)
            return carry

        lax.fori_loop(0, rows // sub, some_rows, 0)
        d_out = dot(dattn_ref[:], m_buf[:], NT)
        for h in range(do_ref.shape[0]):
            do_ref[h] = d_out[:, h * HD:(h + 1) * HD].astype(BF16)


def post(half, at, out_all, w_all, w_mine, x, dy, w_post, y=None):
    n_tp, chunk, width = out_all.shape
    seq, dim = x.shape
    rows = min(256, chunk)
    heads = width // HD
    n_w = len(w_all)
    n = chunk // rows
    steps = n_w // 2
    block = lambda i: jnp.maximum(i - steps, 0)
    row = rows_of(rows, dim, lambda i: half * n + block(i))
    extra = () if y is None else (y,)
    grid_spec = pltpu.PrefetchScalarGridSpec(
        num_scalar_prefetch=1,
        grid=(steps + n,),
        in_specs=anywhere(2 + n_w) + [row, row, whole((1, dim))] + anywhere(len(extra)),
        out_specs=[
            row,
            rows_of(rows, dim, block),
            pl.BlockSpec((heads, rows, HD), lambda i, *_: (0, block(i), 0)),
            whole((8, dim)),
        ],
        scratch_shapes=[
            pltpu.VMEM((chunk, n_tp * width), BF16),
            pltpu.VMEM(w_mine.shape, BF16),
            pltpu.VMEM((steps, n_tp * width, dim // steps), BF16),
            pltpu.VMEM((n_w, chunk, dim // n_w), F32),
            pltpu.SemaphoreType.DMA((n_tp,)),
            pltpu.SemaphoreType.DMA((1,)),
            pltpu.SemaphoreType.DMA((steps, 2)),
        ],
    )
    return pl.pallas_call(
        functools.partial(post_kernel, n_w),
        grid_spec=grid_spec,
        out_shape=[like((seq, dim), BF16), like((chunk, dim), BF16), like((heads, chunk, HD), BF16), like((8, dim), F32)],
        input_output_aliases={n_w + 6: 0} if extra else {},
        compiler_params=params(1),
        cost_estimate=cost(chunk * dim * width * (n_tp + 1), dim * (4 * chunk + width * n_tp)),
    )(at, out_all, w_mine, *w_all, x, dy, w_post, *extra)


def dwo_kernel(core_ref, o_ref, *refs):
    d_refs, (give_ref, keep_ref) = refs[:2], refs[2:]
    half = give_ref.shape[0]
    for ref, core in ((give_ref, 1 - core_ref[0]), (keep_ref, core_ref[0])):
        span = pl.ds(pl.multiple_of(core * half, HD), half)
        ref[:] = sum(dot(o_ref[j, :, span], d_refs[j][:], TN) for j in range(2))


def out_weight_grad(core, out, d_attn, cols=512):
    _, chunk, width = out.shape
    dim = d_attn[0].shape[1]
    tile = lambda n: pl.BlockSpec((n, cols), lambda i, *_: (0, i))
    sums = like((width // 2, dim), F32)
    grid_spec = pltpu.PrefetchScalarGridSpec(
        num_scalar_prefetch=1,
        grid=(dim // cols,),
        in_specs=[fixed(out.shape), tile(chunk), tile(chunk)],
        out_specs=[tile(width // 2), tile(width // 2)],
    )
    return pl.pallas_call(
        dwo_kernel,
        name="dwo",
        grid_spec=grid_spec,
        out_shape=[sums, sums],
        compiler_params=params(1),
        cost_estimate=cost(2 * chunk * dim * width, 2 * dim * (width + chunk)),
    )(core, out, *d_attn)


def kback_kernel(own_ref, near_ref, far_ref, kraw_ref, cos_ref, sin_ref, kn_ref, out_ref, gain_ref):
    @pl.when(pl.program_id(0) == 0)
    def _():
        gain_ref[:] = jnp.zeros(gain_ref.shape, F32)

    kv_heads = own_ref.shape[2]
    for h in range(kv_heads):
        cols = slice(h * HD, (h + 1) * HD)
        d_k = own_ref[0, 0, h] + near_ref[0, 0, h] + far_ref[0, h]
        d_raw, d_gain = norm_rope_back(d_k, kraw_ref[:, cols], kn_ref[:], cos_ref[:], sin_ref[:])
        out_ref[:, cols] = d_raw
        gain_ref[0:1, :] += d_gain
        d_v = own_ref[0, 1, h] + near_ref[0, 1, h] + far_ref[1, h]
        out_ref[:, (kv_heads + h) * HD:(kv_heads + h + 1) * HD] = d_v.astype(BF16)


def key_back(half, own, near, far, k_raw, cos_t, sin_t, k_norm):
    _, _, kv_heads, chunk, _ = own.shape
    rows = min(256, chunk)
    n = chunk // rows
    two = pl.BlockSpec((1, 2, kv_heads, rows, HD), lambda i: (0, 0, 0, i, 0))
    row = lambda cols: rows_of(rows, cols, lambda i: half * n + i)
    return pl.pallas_call(
        kback_kernel,
        grid=(n,),
        in_specs=[
            two,
            two,
            pl.BlockSpec((2, kv_heads, rows, HD), lambda i: (0, 0, i, 0)),
            row(kv_heads * HD),
            row(HD),
            row(HD),
            whole((1, HD)),
        ],
        out_specs=[rows_of(rows, 2 * kv_heads * HD), whole((8, HD))],
        out_shape=[
            like((chunk, 2 * kv_heads * HD), BF16),
            like((8, HD), F32),
        ],
        compiler_params=params(1),
        cost_estimate=cost(32 * chunk * kv_heads * HD, 8 * chunk * kv_heads * HD),
    )(own, near, far, k_raw, cos_t, sin_t, k_norm)


def dx_kernel(n_tp, n_w, at_ref, *refs):
    g_refs, refs = refs[:n_tp], refs[n_tp:]
    w_refs, refs = (refs[:n_w[0]], refs[n_w[0]:sum(n_w)]), refs[sum(n_w):]
    x_ref, dy_ref, wpre_ref, dx_ref, dpre_ref, g_scr, *bufs, acc, sem = refs
    i = pl.program_id(0)
    rows = g_refs[0].shape[0]
    cols = acc.shape[2]
    split = bufs[0].shape[3]

    def weight_copy(kind, slot, at):
        return pltpu.make_async_copy(w_refs[kind][slot], bufs[kind].at[at], sem.at[kind, at])

    @pl.when(i == 0)
    def _():
        for slot in range(n_w[0]):
            for kind in range(2):
                if slot < n_w[kind]:
                    weight_copy(kind, slot, slot).start()
        for s in range(n_tp):
            g_scr[lax.rem(at_ref[2] + n_tp - s, n_tp)] = g_refs[s][:]
        acc[:] = jnp.zeros(acc.shape, F32)

    per_step = n_w[0] // n_w[1]
    for kind, slots in ((0, per_step), (1, 1)):
        for j in range(slots):
            slot = i * slots + j
            weight_copy(kind, 0, slot).wait()
            part = slice(split, None) if kind else slice(split)
            total = sum(dot(bufs[kind][slot, t], g_scr[t, :, part], NT) for t in range(n_tp))
            total = jnp.transpose(total)
            share = jnp.bitwise_xor(at_ref[kind], slot)
            for k in range(total.shape[1] // cols):
                acc[share * (total.shape[1] // cols) + k] += total[:, k * cols:(k + 1) * cols]

    @pl.when(i == pl.num_programs(0) - 1)
    def _():
        dpre_ref[:] = jnp.zeros(dpre_ref.shape, F32)
        n = acc.shape[0]
        tiles = [(s, t, slice(s * cols + t, s * cols + t + HD)) for s in range(n) for t in range(0, cols, HD)]
        dim = n * cols
        sub = min(64, rows)

        def some_rows(r, carry):
            here = pl.ds(pl.multiple_of(r * sub, sub), sub)
            square = jnp.zeros((sub, HD), F32)
            cross = jnp.zeros((sub, HD), F32)
            for s, t, at in tiles:
                x = x_ref[here, at].astype(F32)
                square += x * x
                cross += x * (acc[s, here, t:t + HD] * (1.0 + wpre_ref[:, at]))
            inv = inv_rms(square, dim)
            shrink = inv * inv * inv * (row_sum(cross) * (1.0 / dim))
            for s, t, at in tiles:
                x = x_ref[here, at].astype(F32)
                d_normed = acc[s, here, t:t + HD]
                dpre_ref[:, at] += jnp.sum((d_normed * (x * inv)).reshape(sub // 8, 8, HD), axis=0)
                d_x = inv * (d_normed * (1.0 + wpre_ref[:, at])) - x * shrink
                dx_ref[here, at] = (dy_ref[here, at].astype(F32) + d_x).astype(BF16)
            return carry

        lax.fori_loop(0, rows // sub, some_rows, 0)


def input_grad(half, at, grads, w_all, x, dy, w_pre):
    n_tp = len(grads)
    n_w = tuple(map(len, w_all))
    rows, width = grads[0].shape
    dim = x.shape[1]
    here = pl.BlockSpec((rows, dim), lambda i, t: (half * n_tp + t[2], 0))
    grid_spec = pltpu.PrefetchScalarGridSpec(
        num_scalar_prefetch=1,
        grid=(n_w[1],),
        in_specs=[whole((rows, width))] * n_tp + anywhere(sum(n_w)) + [here, here, whole((1, dim))],
        out_specs=[whole((rows, dim)), whole((8, dim))],
        scratch_shapes=[
            pltpu.VMEM((n_tp, rows, width), BF16),
            *(pltpu.VMEM((len(w), *w[0].shape), BF16) for w in w_all),
            pltpu.VMEM((n_w[0], rows, dim // n_w[0]), F32),
            pltpu.SemaphoreType.DMA((2, n_w[0])),
        ],
    )
    return pl.pallas_call(
        functools.partial(dx_kernel, n_tp, n_w),
        grid_spec=grid_spec,
        out_shape=[like((rows, dim), BF16), like((8, dim), F32)],
        compiler_params=params(1),
        cost_estimate=cost(n_tp * rows * width * dim, n_tp * width * dim),
    )(at, *grads, *w_all[0], *w_all[1], x, dy, w_pre)


def place_kernel(rows_ref, *rest):
    rest[-1][:] = rows_ref[:]


def place(half, rows, total=None):
    chunk, dim = rows.shape
    block = min(HD, chunk)
    n = chunk // block
    extra = () if total is None else (total,)
    return pl.pallas_call(
        place_kernel,
        name="place",
        grid=(n,),
        in_specs=[rows_of(block, dim)] + anywhere(len(extra)),
        out_specs=rows_of(block, dim, lambda i: half * n + i),
        out_shape=like((2 * chunk, dim), BF16),
        input_output_aliases={1: 0} if extra else {},
        compiler_params=params(1),
        cost_estimate=cost(chunk * dim, 2 * chunk * dim),
    )(rows, *extra)


def dw_kernel(n_cp, me_ref, *refs):
    g_refs, n_refs = refs[:2 * n_cp], refs[2 * n_cp:-7]
    dwq_ref, dwk_ref, dwv_ref, n_buf, g_buf, n_sem, g_sem = refs[-7:]
    i = pl.program_id(0)
    cols = n_buf.shape[3]
    chunk, width = g_refs[0].shape
    me = me_ref[0]

    def place(refs_in, buf, sem):
        copies = []
        for j, (ref, shape) in enumerate(refs_in):
            start = sum(r[1] for r in refs_in[:j - j % n_cp:n_cp])
            to = buf.at[jnp.bitwise_xor(me, j % n_cp), pl.ds(start, shape)]
            copies.append(pltpu.make_async_copy(ref, to, sem.at[j]))
        return copies

    def fetch(step, par):
        span = pl.ds(pl.multiple_of(step * cols, cols), cols)
        return place([(r.at[:, span], r.shape[0]) for r in n_refs], n_buf.at[par], n_sem.at[par])

    @pl.when(i == 0)
    def _():
        grads = place([(r, chunk) for r in g_refs], g_buf, g_sem)
        for copy in fetch(0, 0) + grads:
            copy.start()
        for copy in grads:
            copy.wait()

    @pl.when(i + 1 < pl.num_programs(0))
    def _():
        for copy in fetch(i + 1, (i + 1) % 2):
            copy.start()

    for copy in fetch(i, i % 2):
        copy.wait()
    seq = 2 * chunk
    grad = dot(n_buf[i % 2].reshape(n_cp * seq, cols), g_buf[:].reshape(n_cp * seq, width), TN)
    q_width, kv_width = dwq_ref.shape[1], dwk_ref.shape[1]
    dwq_ref[:] = grad[:, :q_width]
    dwk_ref[:] = grad[:, q_width:q_width + kv_width]
    dwv_ref[:] = grad[:, q_width + kv_width:]


def weight_grads(me, normed, grads, q_width, cols=256):
    n_cp = len(grads) // 2
    chunk, width = grads[0].shape
    dim = normed[0].shape[1]
    kv_width = (width - q_width) // 2
    tile = lambda n: rows_of(cols, n)
    grid_spec = pltpu.PrefetchScalarGridSpec(
        num_scalar_prefetch=1,
        grid=(dim // cols,),
        in_specs=anywhere(len(grads) + len(normed)),
        out_specs=[tile(q_width), tile(kv_width), tile(kv_width)],
        scratch_shapes=[
            pltpu.VMEM((2, n_cp, 2 * chunk, cols), BF16),
            pltpu.VMEM((n_cp, 2 * chunk, width), BF16),
            pltpu.SemaphoreType.DMA((2, len(normed))),
            pltpu.SemaphoreType.DMA((len(grads),)),
        ],
    )
    return pl.pallas_call(
        functools.partial(dw_kernel, n_cp),
        name="dw",
        grid_spec=grid_spec,
        out_shape=[like((dim, n), F32) for n in (q_width, kv_width, kv_width)],
        compiler_params=params(1),
        cost_estimate=cost(2 * n_cp * chunk * dim * width, 2 * n_cp * chunk * (dim + width)),
    )(me, *grads, *normed)


def join_kernel(core_ref, keep_ref, other_ref, *rest):
    half = pl.program_id(0)

    @pl.when(half == core_ref[0])
    def _():
        rest[-1][:] = keep_ref[:]

    @pl.when(half != core_ref[0])
    def _():
        rest[-1][:] = other_ref[:]


def join_halves(core, keep, other, start, half, total=None):
    block, width = HD, keep.shape[1]
    n = keep.shape[0] // block
    extra = () if total is None else (total,)
    part = pl.BlockSpec((block, width), lambda i, j, c: (j, 0))
    grid_spec = pltpu.PrefetchScalarGridSpec(
        num_scalar_prefetch=1,
        grid=(2, n),
        in_specs=[part, part] + anywhere(len(extra)),
        out_specs=pl.BlockSpec((block, width), lambda i, j, c: (i * (half // block) + start // block + j, 0)),
    )
    return pl.pallas_call(
        join_kernel,
        name="join",
        grid_spec=grid_spec,
        out_shape=like((2 * half, width), F32),
        input_output_aliases={3: 0} if extra else {},
        compiler_params=params(2),
        cost_estimate=cost(n * block * width, 8 * n * block * width),
    )(core, keep, other, *extra)


def solution(mesh):
    n_cp, n_tp, n_dp = mesh.shape["cp"], mesh.shape["tp"], mesh.shape["dp"]
    near = [(i, i ^ 1) for i in range(n_cp)]
    across = [(i, i ^ 2) for i in range(n_cp)]
    beside = [(i, i ^ 1) for i in range(n_dp)]

    def from_cp(value):
        far = lax.ppermute(value, "cp", across)
        return [value, lax.ppermute(value, "cp", near), far, lax.ppermute(far, "cp", near)]

    def per_device(hidden, cotangent, pos_loc, w_q, w_k, w_v, w_o, w_pre, w_post, q_norm, k_norm):
        _, seq, dim = hidden.shape
        x, dy = hidden[0], cotangent[0]
        kv_heads = w_k.shape[1] // HD
        cp, tp, dp = (lax.axis_index(a).astype(jnp.int32) for a in ("cp", "tp", "dp"))
        core = cp % 2
        me, one_core = cp.reshape(1), core.reshape(1)

        share = dp * n_cp + cp
        shares = n_dp * n_cp
        cols = dim // shares

        def over_tp(part):
            return lax.all_gather(part, "tp", axis=0, tiled=True)

        def spread(own):
            blocks = from_cp(own)
            if n_dp == 2:
                for value in (own, blocks[2]):
                    other = lax.ppermute(value, "dp", beside)
                    blocks += [other, lax.ppermute(other, "cp", near)]
            return blocks

        w_o_all = spread(over_tp(lax.dynamic_slice_in_dim(w_o, share * cols, cols, 1)))
        w_a = lax.dynamic_slice_in_dim(w_q, share * cols, cols, 0)
        share_b = dp * 2 + core
        cols_b = dim // (2 * n_dp)
        w_b = jnp.concatenate([lax.dynamic_slice_in_dim(w, share_b * cols_b, cols_b, 0) for w in (w_k, w_v)], axis=1)
        w_a_all = spread(over_tp(w_a).reshape(n_tp, cols, w_a.shape[1]))

        cos_t, sin_t = rope_tables(pos_loc)
        qn, kn = q_norm.reshape(1, HD), k_norm.reshape(1, HD)
        wpre, wpost = w_pre.reshape(1, dim), w_post.reshape(1, dim)
        rows = seq // 8
        x_far = lax.ppermute(x[:rows], "cp", across)
        *normed, kv_own, k_raw = project_kv(x, wpre, w_k, w_v, kn, cos_t, sin_t, rows, (1, 3, 4))
        kv_blocks = from_cp(kv_own)
        q_fin, q_raw = project_q(normed, w_q, qn, cos_t, sin_t, rows)
        far = norm_rows(x_far, wpre)
        normed_all = [normed[0], lax.ppermute(normed[0], "cp", near), far, lax.ppermute(far, "cp", near)]
        normed_all += from_cp(normed[1]) + from_cp(normed[2])
        out, lse = attention_fwd(me, q_fin, kv_blocks, kv_heads)

        out_all = [None, None]
        for half in (1, 0):
            out_all[half] = lax.all_gather(out[half], "tp", axis=0, tiled=False)
        w_b = over_tp(w_b).reshape(n_tp, cols_b, w_b.shape[1])
        w_b_all = [w_b, lax.ppermute(w_b, "cp", near)]
        if n_dp == 2:
            w_b = lax.ppermute(w_b, "dp", beside)
            w_b_all += [w_b, lax.ppermute(w_b, "cp", near)]
        at = jnp.stack([share, core])

        low, dq, d_attn, d_post, gains, carried, y = [], [None] * 2, [None] * 2, [], [], [None] * 2, None
        for half in (1, 0):
            y, d_attn[half], d_out, part = post(half, at, out_all[half], w_o_all, w_o, x, dy, wpost, y)
            d_post.append(part)
            dq[half], kept, sent, *low, gain = attention_bwd(
                half, me, q_fin, d_out, out, lse, q_raw, cos_t, sin_t, qn, kv_blocks, kv_heads, *low
            )
            gains.append(gain[0])
            got = lax.ppermute(sent, "cp", near)
            carried[half] = (kept, got, lax.ppermute(kept[1] + got[1], "cp", across))

        give, keep = out_weight_grad(one_core, out, d_attn)
        got = lax.ppermute(give, "cp", near)
        rows = keep.shape[0]
        d_wo = None
        for start, stop in ((0, rows - HD), (rows - HD, rows)):
            mine_part = keep[start:stop] + got[start:stop]
            mine_part = mine_part + lax.ppermute(mine_part, "cp", across)
            other = lax.ppermute(mine_part, "cp", near)
            d_wo = join_halves(one_core, mine_part, other, start, rows, d_wo)

        rows = seq // 2 // n_tp
        at_tp = jnp.stack([share, share_b, tp])
        grads, d_hidden, d_pre = [None] * 2, None, []
        for half in (1, 0):
            d_kv, gain = key_back(half, *carried[half], k_raw, cos_t, sin_t, kn)
            gains.append(gain[0])
            g = grads[half] = jnp.concatenate([dq[half], d_kv], axis=1)
            pieces = [lax.dynamic_slice_in_dim(g, tp * rows, rows, 0)]
            for s in range(1, n_tp):
                part = lax.dynamic_slice_in_dim(g, ((tp + s) % n_tp) * rows, rows, 0)
                pieces.append(lax.ppermute(part, "tp", [(i, (i + s) % n_tp) for i in range(n_tp)]))
            dx_rows, part = input_grad(half, at_tp, pieces, (w_a_all, w_b_all), x, dy, wpre)
            d_pre.append(part)
            dx_rows = lax.all_gather(dx_rows, "tp", axis=0, tiled=True)
            d_hidden = place(half, dx_rows, d_hidden)

        grads_all = from_cp(grads[0]) + from_cp(grads[1])
        d_wq, d_wk, d_wv = weight_grads(me, normed_all, grads_all, w_q.shape[1])

        d_post, d_pre = jnp.sum(sum(d_post), axis=0), jnp.sum(sum(d_pre), axis=0)
        small = jnp.concatenate([jnp.where(tp == 0, d_post, 0.0), d_pre, sum(gains[:2]), sum(gains[2:])])
        small = small + lax.ppermute(small, "cp", near)
        small = small + lax.ppermute(small, "cp", across)
        small = small + lax.ppermute(small, "tp", [(i, i ^ 1) for i in range(n_tp)])
        small = small + lax.ppermute(small, "tp", [(i, i ^ 2) for i in range(n_tp)])
        d_post, d_pre, d_qn, d_kn = jnp.split(small, np.cumsum([dim, dim, HD]))
        return y[None], d_hidden[None], d_wq, d_wk, d_wv, d_wo, d_pre, d_post, d_qn, d_kn

    rows, cols, all_of = P('dp', 'cp'), P(None, 'tp'), P()
    specs_in = (rows, rows, P(('dp', 'cp')), cols, cols, cols, P('tp'), all_of, all_of, all_of, all_of)
    grid, by_dp = P('dp', 'tp'), P('dp')
    specs_out = (rows, rows, grid, grid, grid, P(('dp', 'tp')), by_dp, by_dp, by_dp, by_dp)
    return jax.shard_map(per_device, mesh=mesh, in_specs=specs_in, out_specs=specs_out, check_vma=False)
```

```python
import functools

import jax
import jax.numpy as jnp
import numpy as np
from jax import lax
from jax.experimental import pallas as pl
from jax.experimental.pallas import tpu as pltpu
from jax.sharding import PartitionSpec as P


EPS = 1e-6
ROPE_BASE = 1000000.0
ROPE_SCALE = 8.0
NEG_BIG = -1e30
LOG2E = 1.4426950408889634
HD = 128
F32 = jnp.float32
BF16 = jnp.bfloat16
VMEM_MAX = 62914560
NT = (((1,), (1,)), ((), ()))
TN = (((0,), (0,)), ((), ()))


def dot(a, b, dims=(((1,), (0,)), ((), ()))):
    return lax.dot_general(a, b, dims, preferred_element_type=F32)


def params(dims, vmem=VMEM_MAX):
    return pltpu.CompilerParams(dimension_semantics=("arbitrary",) * dims, vmem_limit_bytes=vmem)


def cost(products, values, trans=0):
    return pl.CostEstimate(flops=2 * products, bytes_accessed=2 * values, transcendentals=trans)


def row_sum(values):
    return jnp.sum(values, axis=1, keepdims=True)


def row_mean(values, dim):
    return row_sum(values) * (1.0 / dim)


def inv_rms(square, dim):
    return lax.rsqrt(row_mean(square, dim) + EPS)


def fold(values):
    return jnp.sum(values.reshape(-1, 8, HD), axis=0)


def few(rows):
    return min(64, rows)


def whole(shape):
    return pl.BlockSpec(shape, lambda *_: (0,) * len(shape))


def fixed(shape):
    return pl.BlockSpec(shape, lambda *_: (0,) * len(shape), pipeline_mode=pl.Buffered(buffer_count=1))


def rows_of(rows, cols, at=lambda i: i):
    return pl.BlockSpec((rows, cols), lambda i, *_: (at(i), 0))


def anywhere(n):
    return [pl.BlockSpec(memory_space=pl.ANY)] * n


def like(shape, dtype):
    return jax.ShapeDtypeStruct(shape, dtype)


def rope_tables(pos_loc):
    half_dim = HD // 2
    inv_freq = 1.0 / (ROPE_SCALE * ROPE_BASE ** (jnp.arange(half_dim, dtype=F32) * (2.0 / HD)))
    angles = pos_loc.astype(F32)[:, None] * inv_freq[None, :]
    cos_t, sin_t = jnp.cos(angles), jnp.sin(angles)
    return jnp.concatenate([cos_t, cos_t], axis=-1), jnp.concatenate([-sin_t, sin_t], axis=-1)


def norm_rope(raw, gain, cos_t, sin_t):
    raw = raw.astype(F32)
    unit = raw * inv_rms(raw * raw, HD)
    scaled = unit * (1.0 + gain)
    return (scaled * cos_t + pltpu.roll(scaled, HD // 2, 1) * sin_t).astype(BF16)


def norm_rope_back(d_final, raw, gain, cos_t, sin_t):
    raw = raw.astype(F32)
    inv = inv_rms(raw * raw, HD)
    unit = raw * inv
    d_scaled = d_final * cos_t - pltpu.roll(d_final, HD // 2, 1) * sin_t
    d_gain = jnp.sum(d_scaled * unit, axis=0, keepdims=True)
    d_unit = d_scaled * (1.0 + gain)
    d_raw = inv * (d_unit - unit * row_mean(d_unit * unit, HD))
    return d_raw.astype(BF16), d_gain


def normalise(x_ref, wpre_ref, write):
    rows, dim = x_ref.shape
    tiles = [slice(t, t + HD) for t in range(0, dim, HD)]
    sub = few(rows)

    def some_rows(r, carry):
        here = pl.ds(pl.multiple_of(r * sub, sub), sub)
        square = jnp.zeros((sub, HD), F32)
        for at in tiles:
            x = x_ref[here, at].astype(F32)
            square += x * x
        inv = inv_rms(square, dim)
        for at in tiles:
            write(here, at, (x_ref[here, at].astype(F32) * inv * (1.0 + wpre_ref[:, at])).astype(BF16))
        return carry

    lax.fori_loop(0, rows // sub, some_rows, 0)


def norm_kernel(x_ref, wpre_ref, out_ref):
    def write(rows, cols, value):
        out_ref[rows, cols] = value

    normalise(x_ref, wpre_ref, write)


def norm_rows(x, w_pre):
    return pl.pallas_call(
        norm_kernel,
        name="norm",
        grid=(1,),
        in_specs=[whole(x.shape), whole(w_pre.shape)],
        out_specs=whole(x.shape),
        out_shape=like(x.shape, BF16),
        compiler_params=params(1),
        cost_estimate=cost(x.size, x.size),
    )(x, w_pre)


def kv_kernel(parts, x_ref, wpre_ref, wk_ref, wv_ref, kn_ref, cos_ref, sin_ref, *rest):
    n = len(parts)
    out_refs, (kv_ref, kraw_ref, buf, sem) = rest[:n], rest[n:]
    i = pl.program_id(0)
    rows = x_ref.shape[0]
    par = i % 2
    steps = [(j, step) for j, size in enumerate(parts) for step in range(size)]

    def out_copy(step):
        j, at = steps[step]
        return pltpu.make_async_copy(buf.at[step % 2], out_refs[j].at[pl.ds(at * rows, rows)], sem.at[step % 2])

    for step in range(2, len(steps)):

        @pl.when(i == step)
        def _():
            out_copy(step - 2).wait()

    def write(here, cols, value):
        buf[par, here, cols] = value

    normalise(x_ref, wpre_ref, write)
    for step in range(len(steps)):

        @pl.when(i == step)
        def _():
            out_copy(step).start()

    normed = buf[par]
    k_raw = dot(normed, wk_ref[:]).astype(BF16)
    kraw_ref[:] = k_raw
    width = k_raw.shape[1]
    for h in range(width // HD):
        cols = slice(h * HD, (h + 1) * HD)
        kv_ref[:, cols] = norm_rope(k_raw[:, cols], kn_ref[:], cos_ref[:], sin_ref[:])
    kv_ref[:, width:] = dot(normed, wv_ref[:]).astype(BF16)

    @pl.when(i == len(steps) - 1)
    def _():
        for step in range(len(steps))[-2:]:
            out_copy(step).wait()


def project_kv(x, w_pre, w_k, w_v, k_norm, cos_t, sin_t, rows, parts):
    seq, dim = x.shape
    width = w_k.shape[1]
    grid_spec = pl.GridSpec(
        grid=(seq // rows,),
        in_specs=[rows_of(rows, dim), whole((1, dim)), fixed(w_k.shape), fixed(w_v.shape), whole((1, HD))]
        + [rows_of(rows, HD)] * 2,
        out_specs=anywhere(len(parts)) + [rows_of(rows, 2 * width), rows_of(rows, width)],
        scratch_shapes=[pltpu.VMEM((2, rows, dim), BF16), pltpu.SemaphoreType.DMA((2,))],
    )
    return pl.pallas_call(
        functools.partial(kv_kernel, parts),
        name="pkv",
        grid_spec=grid_spec,
        out_shape=[like((n * rows, dim), BF16) for n in parts] + [like((seq, 2 * width), BF16), like((seq, width), BF16)],
        compiler_params=params(1),
        cost_estimate=cost(2 * seq * dim * width, 2 * dim * (seq + width)),
    )(x, w_pre, w_k, w_v, k_norm, cos_t, sin_t)


def q_kernel(starts, *refs):
    n_refs, (wq_ref, qn_ref, cos_ref, sin_ref, qfin_ref, qraw_ref) = refs[:len(starts)], refs[len(starts):]
    normed = n_refs[0][:]
    for start, ref in zip(starts[1:], n_refs[1:]):
        normed = jnp.where(pl.program_id(0) >= start, ref[:], normed)
    q_raw = dot(normed, wq_ref[:]).astype(BF16)
    for h in range(qfin_ref.shape[0]):
        part = q_raw[:, h * HD:(h + 1) * HD]
        qraw_ref[h] = part
        qfin_ref[h] = norm_rope(part, qn_ref[:], cos_ref[:], sin_ref[:])


def project_q(normed, w_q, q_norm, cos_t, sin_t, rows):
    dim, width = w_q.shape
    sizes = [part.shape[0] // rows for part in normed]
    starts = [sum(sizes[:j]) for j in range(len(sizes))]
    n = sum(sizes)
    heads = width // HD
    block = lambda start, size: rows_of(rows, dim, lambda i: jnp.clip(i - start, 0, size - 1))
    head_rows = pl.BlockSpec((heads, rows, HD), lambda i: (0, i, 0))
    shape = like((heads, n * rows, HD), BF16)
    return pl.pallas_call(
        functools.partial(q_kernel, starts),
        name="pq",
        grid=(n,),
        in_specs=list(map(block, starts, sizes)) + [fixed(w_q.shape), whole((1, HD))] + [rows_of(rows, HD)] * 2,
        out_specs=[head_rows, head_rows],
        out_shape=[shape, shape],
        compiler_params=params(1),
        cost_estimate=cost(n * rows * dim * width, dim * (n * rows + width)),
    )(*normed, w_q, q_norm, cos_t, sin_t)


def load_kv(kv_refs, k_buf, v_buf, sems, heads):
    kv_heads = kv_refs[0].shape[1] // (2 * HD)
    copies = []
    for s, ref in enumerate(kv_refs):
        for i, h in enumerate(heads):
            for t, buf in enumerate((k_buf, v_buf)):
                src = ref.at[:, pl.ds((t * kv_heads + h) * HD, HD)]
                copies.append(pltpu.make_async_copy(src, buf.at[i, s], sems.at[s, i, t]))
    for copy in copies:
        copy.start()
    for copy in copies:
        copy.wait()


def piece_place(piece, me, n_cp):
    upper = piece >= n_cp
    owner = jnp.where(upper, 2 * n_cp - 1 - piece, piece)
    return jnp.bitwise_xor(owner, me), upper.astype(jnp.int32)


def fwd_kernel(n_cp, me_ref, q_ref, *rest):
    kv_refs = rest[:n_cp]
    o_ref, lse_ref, k_buf, v_buf, m_scr, acc_scr, sems = rest[n_cp:]
    h, half = pl.program_id(0), pl.program_id(1)
    groups, rows, _ = q_ref.shape

    @pl.when((h == 0) & (half == 0))
    def _():
        load_kv(kv_refs, k_buf, v_buf, sems, range(k_buf.shape[0]))

    me = me_ref[0]
    piece = jnp.where(half == 0, me, 2 * n_cp - 1 - me)
    scale = HD ** -0.5 * LOG2E
    m_scr[:] = jnp.full(m_scr.shape, NEG_BIG, F32)
    acc_scr[:] = jnp.zeros(acc_scr.shape, F32)

    def block(j, masked):
        slot, upper = piece_place(j, me, n_cp)
        span = pl.ds(pl.multiple_of(upper * rows, rows), rows)
        k = k_buf[h, slot, span, :]
        v_ext = jnp.concatenate([v_buf[h, slot, span, :], jnp.ones((rows, HD), BF16)], axis=1)
        scores = [dot(q_ref[g], k, NT) * scale for g in range(groups)]
        for g in range(groups):
            s = scores[g]
            if masked:
                q_pos = lax.broadcasted_iota(jnp.int32, s.shape, 0)
                k_pos = lax.broadcasted_iota(jnp.int32, s.shape, 1)
                s = jnp.where(k_pos <= q_pos, s, NEG_BIG)
            m_old = m_scr[g]
            m_new = jnp.maximum(m_old, jnp.max(s, axis=1, keepdims=True))
            alpha = jnp.exp2(m_old - m_new)
            p = jnp.exp2(s - jnp.concatenate([m_new] * (rows // HD), axis=1)).astype(BF16)
            acc_scr[g] = acc_scr[g] * jnp.concatenate([alpha, alpha], axis=1) + dot(p, v_ext)
            m_scr[g] = m_new

    def full(j, carry):
        block(j, False)
        return carry

    lax.fori_loop(0, piece, full, 0)
    block(piece, True)
    for g in range(groups):
        l = acc_scr[g, :, HD:]
        o_ref[0, :, g * HD:(g + 1) * HD] = (acc_scr[g, :, :HD] / l).astype(BF16)
        lse_ref[0, g:g + 1, :] = jnp.transpose(m_scr[g] + jnp.log2(l))[0:1, :]


def attention_fwd(me, q_fin, kv_blocks, kv_heads):
    heads, seq, _ = q_fin.shape
    n_cp = len(kv_blocks)
    groups = heads // kv_heads
    rows = seq // 2
    grid_spec = pltpu.PrefetchScalarGridSpec(
        num_scalar_prefetch=1,
        grid=(kv_heads, 2),
        in_specs=[pl.BlockSpec((groups, rows, HD), lambda h, i, *_: (h, i, 0))] + anywhere(n_cp),
        out_specs=[
            pl.BlockSpec((1, rows, groups * HD), lambda h, i, *_: (i, 0, h)),
            pl.BlockSpec((1, 8, rows), lambda h, i, *_: (h, 0, i)),
        ],
        scratch_shapes=[
            pltpu.VMEM((kv_heads, n_cp, seq, HD), BF16),
            pltpu.VMEM((kv_heads, n_cp, seq, HD), BF16),
            pltpu.VMEM((groups, rows, HD), F32),
            pltpu.VMEM((groups, rows, 2 * HD), F32),
            pltpu.SemaphoreType.DMA((n_cp, kv_heads, 2)),
        ],
    )
    pairs = heads * rows * rows * (2 * n_cp + 1)
    return pl.pallas_call(
        functools.partial(fwd_kernel, n_cp),
        name="fwd",
        grid_spec=grid_spec,
        out_shape=[
            like((2, rows, heads * HD), BF16),
            like((kv_heads, 8, seq), F32),
        ],
        compiler_params=params(2),
        cost_estimate=cost(2 * pairs * HD, 4 * seq * heads * HD, pairs),
    )(me, q_fin, *kv_blocks)


def bwd_kernel(n_cp, half, me_ref, q_ref, do_ref, o_ref, lse_ref, qraw_ref, cos_ref, sin_ref, qn_ref, *rest):
    kv_refs, rest = rest[:n_cp], rest[n_cp:]
    if half:
        dq_ref, keep_ref, send_ref, low_ref, gain_ref = rest[:5]
    else:
        low_ref, dq_ref, keep_ref, send_ref, gain_ref = rest[:5]
    k_buf, v_buf, dq_scr, dkv_scr, sems = rest[5:]
    h = pl.program_id(0)
    groups, rows, _ = q_ref.shape
    two = n_cp // 2

    @pl.when(h == 0)
    def _():
        load_kv(kv_refs, k_buf, v_buf, sems, range(k_buf.shape[0]))
        gain_ref[:] = jnp.zeros(gain_ref.shape, F32)

    if half:
        dkv_scr[:] = jnp.zeros(dkv_scr.shape, F32)
    else:
        dkv_scr[:] = low_ref[:, :, 0]

    me = me_ref[0]
    piece = 2 * n_cp - 1 - me if half else me
    scale = HD ** -0.5
    delta = []
    for g in range(groups):
        prod = do_ref[g].astype(F32) * o_ref[0, :, g * HD:(g + 1) * HD].astype(F32)
        column = jnp.broadcast_to(row_sum(prod), (rows, HD))
        delta.append(jnp.transpose(column)[0:1, :])
    dq_scr[:] = jnp.zeros(dq_scr.shape, F32)

    def block(j, masked):
        slot, upper = piece_place(j, me, n_cp)
        span = pl.ds(pl.multiple_of(upper * rows, rows), rows)
        k = k_buf[h, slot, span, :]
        v = v_buf[h, slot, span, :]
        probs, d_scores = [], []
        for g in range(groups):
            s = dot(k, q_ref[g], NT)
            p = jnp.exp2(s * (scale * LOG2E) - lse_ref[0, g:g + 1, :])
            if masked:
                k_pos = lax.broadcasted_iota(jnp.int32, s.shape, 0)
                q_pos = lax.broadcasted_iota(jnp.int32, s.shape, 1)
                p = jnp.where(k_pos <= q_pos, p, 0.0)
            probs.append(p.astype(BF16))
            d_scores.append((p * (dot(v, do_ref[g], NT) - delta[g])).astype(BF16))
        for g in range(groups):
            dq_scr[g] += dot(d_scores[g], k, TN)
        index = (slot % 2) * two + slot // 2
        into = span if half else pl.ds(0, rows)
        d_all = jnp.concatenate(d_scores, axis=1)
        p_all = jnp.concatenate(probs, axis=1)
        dkv_scr[index, 0, into, :] += dot(d_all, q_ref[:].reshape(groups * rows, HD)) * scale
        dkv_scr[index, 1, into, :] += dot(p_all, do_ref[:].reshape(groups * rows, HD))

    def full(j, carry):
        block(j, False)
        return carry

    lax.fori_loop(0, piece, full, 0)
    block(piece, True)
    for g in range(groups):
        d_raw, d_gain = norm_rope_back(dq_scr[g] * scale, qraw_ref[g], qn_ref[:], cos_ref[:], sin_ref[:])
        dq_ref[:, g * HD:(g + 1) * HD] = d_raw
        gain_ref[0:1, :] += d_gain
    for i in range(two):
        own = slice(rows, 2 * rows) if half else slice(0, rows)
        keep_ref[i, :, 0] = dkv_scr[i, :, own]
        send_ref[i, :, 0] = dkv_scr[two + i, :, own]
    if half:
        low_ref[:, :, 0] = dkv_scr[:, :, :rows]


def attention_bwd(half, me, q_fin, d_out, out, lse, q_raw, cos_t, sin_t, q_norm, kv_blocks, kv_heads, low=None):
    heads, seq, _ = q_fin.shape
    n_cp = len(kv_blocks)
    groups = heads // kv_heads
    rows = seq // 2
    by_head = pl.BlockSpec((groups, rows, HD), lambda h, *_: (h, half, 0))
    table = rows_of(rows, HD, lambda h: half)
    by_owner = lambda n: pl.BlockSpec((n, 2, 1, rows, HD), lambda h, *_: (0, 0, h, 0, 0))
    grads = lambda n: like((n, 2, kv_heads, rows, HD), F32)
    extra = () if low is None else (low,)
    carried = [n_cp] if half else []
    grid_spec = pltpu.PrefetchScalarGridSpec(
        num_scalar_prefetch=1,
        grid=(kv_heads,),
        in_specs=[
            by_head,
            pl.BlockSpec((groups, rows, HD), lambda h, *_: (h, 0, 0)),
            pl.BlockSpec((1, rows, groups * HD), lambda h, *_: (half, 0, h)),
            pl.BlockSpec((1, 8, rows), lambda h, *_: (h, 0, half)),
            by_head,
            table,
            table,
            whole((1, HD)),
        ]
        + anywhere(n_cp)
        + [by_owner(n_cp)] * len(extra),
        out_specs=[
            pl.BlockSpec((rows, groups * HD), lambda h, *_: (0, h)),
            by_owner(n_cp // 2),
            by_owner(n_cp // 2),
            *map(by_owner, carried),
            whole((8, HD)),
        ],
        scratch_shapes=[
            pltpu.VMEM((kv_heads, n_cp, seq, HD), BF16),
            pltpu.VMEM((kv_heads, n_cp, seq, HD), BF16),
            pltpu.VMEM((groups, rows, HD), F32),
            pltpu.VMEM((n_cp, 2, seq if half else rows, HD), F32),
            pltpu.SemaphoreType.DMA((n_cp, kv_heads, 2)),
        ],
    )
    pairs = heads * rows * rows * (n_cp + 1)
    return pl.pallas_call(
        functools.partial(bwd_kernel, n_cp, half),
        grid_spec=grid_spec,
        out_shape=[
            like((rows, heads * HD), BF16),
            grads(n_cp // 2),
            grads(n_cp // 2),
            *map(grads, carried),
            like((8, HD), F32),
        ],
        compiler_params=params(1),
        cost_estimate=cost(5 * pairs * HD, 8 * seq * heads * HD, pairs),
    )(me, q_fin, d_out, out, lse, q_raw, cos_t, sin_t, q_norm, *kv_blocks, *extra)


def post_kernel(n_w, at_ref, o_ref, wmine_ref, *rest):
    w_refs = rest[:n_w]
    x_ref, dy_ref, wpost_ref = rest[n_w:n_w + 3]
    y_ref, dattn_ref, do_ref, dpost_ref, o_buf, m_buf, w_buf, attn_scr, o_sem, m_sem, w_sem = rest[-11:]
    i = pl.program_id(0)
    n_tp, _, width = o_ref.shape
    rows, dim = x_ref.shape
    cols = attn_scr.shape[2]
    steps = n_w // 2
    mine = pltpu.make_async_copy(wmine_ref, m_buf, m_sem.at[0])

    def weight_copies(pair, par):
        to = [w_buf.at[par, :, pl.ds(j * cols, cols)] for j in range(2)]
        return [pltpu.make_async_copy(w_refs[2 * pair + j], to[j], w_sem.at[par, j]) for j in range(2)]

    @pl.when(i == 0)
    def _():
        copies = [
            pltpu.make_async_copy(o_ref.at[t], o_buf.at[:, pl.ds(t * width, width)], o_sem.at[t]) for t in range(n_tp)
        ]
        for copy in copies + weight_copies(0, 0):
            copy.start()
        for copy in copies:
            copy.wait()

    for pair in range(1, steps):

        @pl.when(i == pair - 1)
        def _():
            for copy in weight_copies(pair, pair % 2):
                copy.start()

    @pl.when(i == steps - 1)
    def _():
        mine.start()

    @pl.when(i < steps)
    def _():
        par = i % 2
        for copy in weight_copies(0, par):
            copy.wait()
        both = dot(o_buf[:], w_buf[par])
        for j in range(2):
            attn_scr[jnp.bitwise_xor(at_ref[0], 2 * i + j)] = both[:, j * cols:(j + 1) * cols]

    @pl.when(i == steps)
    def _():
        dpost_ref[:] = jnp.zeros(dpost_ref.shape, F32)
        mine.wait()

    @pl.when(i >= steps)
    def _():
        tiles = [(s, t * HD, slice(s * cols + t * HD, s * cols + (t + 1) * HD)) for s in range(n_w) for t in range(cols // HD)]
        sub = few(rows)

        def some_rows(r, carry):
            here = pl.ds(pl.multiple_of(r * sub, sub), sub)
            there = pl.ds(pl.multiple_of((i - steps) * rows + r * sub, sub), sub)
            square = jnp.zeros((sub, HD), F32)
            cross = jnp.zeros((sub, HD), F32)
            for s, t, at in tiles:
                attn = attn_scr[s, there, t:t + HD]
                square += attn * attn
                cross += attn * (dy_ref[here, at].astype(F32) * (1.0 + wpost_ref[:, at]))
            inv = inv_rms(square, dim)
            shrink = inv * inv * inv * row_mean(cross, dim)
            for s, t, at in tiles:
                attn = attn_scr[s, there, t:t + HD]
                gain = 1.0 + wpost_ref[:, at]
                dy = dy_ref[here, at].astype(F32)
                unit = attn * inv
                y_ref[here, at] = (x_ref[here, at].astype(F32) + unit * gain).astype(BF16)
                dpost_ref[:, at] += fold(dy * unit)
                dattn_ref[here, at] = (inv * (dy * gain) - attn * shrink).astype(BF16)
            return carry

        lax.fori_loop(0, rows // sub, some_rows, 0)
        d_out = dot(dattn_ref[:], m_buf[:], NT)
        for h in range(do_ref.shape[0]):
            do_ref[h] = d_out[:, h * HD:(h + 1) * HD].astype(BF16)


def post(half, at, out_all, w_all, w_mine, x, dy, w_post, y=None):
    n_tp, chunk, width = out_all.shape
    seq, dim = x.shape
    rows = min(2 * HD, chunk)
    heads = width // HD
    n_w = len(w_all)
    n = chunk // rows
    steps = n_w // 2
    block = lambda i: jnp.maximum(i - steps, 0)
    row = rows_of(rows, dim, lambda i: half * n + block(i))
    extra = () if y is None else (y,)
    grid_spec = pltpu.PrefetchScalarGridSpec(
        num_scalar_prefetch=1,
        grid=(steps + n,),
        in_specs=anywhere(2 + n_w) + [row, row, whole((1, dim))] + anywhere(len(extra)),
        out_specs=[
            row,
            rows_of(rows, dim, block),
            pl.BlockSpec((heads, rows, HD), lambda i, *_: (0, block(i), 0)),
            whole((8, dim)),
        ],
        scratch_shapes=[
            pltpu.VMEM((chunk, n_tp * width), BF16),
            pltpu.VMEM(w_mine.shape, BF16),
            pltpu.VMEM((2, n_tp * width, dim // steps), BF16),
            pltpu.VMEM((n_w, chunk, dim // n_w), F32),
            pltpu.SemaphoreType.DMA((n_tp,)),
            pltpu.SemaphoreType.DMA((1,)),
            pltpu.SemaphoreType.DMA((2, 2)),
        ],
    )
    return pl.pallas_call(
        functools.partial(post_kernel, n_w),
        grid_spec=grid_spec,
        out_shape=[like((seq, dim), BF16), like((chunk, dim), BF16), like((heads, chunk, HD), BF16), like((8, dim), F32)],
        input_output_aliases={n_w + 6: 0} if extra else {},
        compiler_params=params(1),
        cost_estimate=cost(chunk * dim * width * (n_tp + 1), dim * (4 * chunk + width * n_tp)),
    )(at, out_all, w_mine, *w_all, x, dy, w_post, *extra)


def dwo_kernel(core_ref, o_ref, *refs):
    d_refs, (give_ref, keep_ref) = refs[:2], refs[2:]
    half = give_ref.shape[0]
    for ref, core in ((give_ref, 1 - core_ref[0]), (keep_ref, core_ref[0])):
        span = pl.ds(pl.multiple_of(core * half, HD), half)
        ref[:] = sum(dot(o_ref[j, :, span], d_refs[j][:], TN) for j in range(2))


def out_weight_grad(core, out, d_attn, cols=512):
    _, chunk, width = out.shape
    dim = d_attn[0].shape[1]
    tile = lambda n: pl.BlockSpec((n, cols), lambda i, *_: (0, i))
    sums = like((width // 2, dim), F32)
    grid_spec = pltpu.PrefetchScalarGridSpec(
        num_scalar_prefetch=1,
        grid=(dim // cols,),
        in_specs=[fixed(out.shape), tile(chunk), tile(chunk)],
        out_specs=[tile(width // 2), tile(width // 2)],
    )
    return pl.pallas_call(
        dwo_kernel,
        name="dwo",
        grid_spec=grid_spec,
        out_shape=[sums, sums],
        compiler_params=params(1),
        cost_estimate=cost(2 * chunk * dim * width, 2 * dim * (width + chunk)),
    )(core, out, *d_attn)


def kback_kernel(own_ref, near_ref, far_ref, kraw_ref, cos_ref, sin_ref, kn_ref, out_ref, gain_ref):
    @pl.when(pl.program_id(0) == 0)
    def _():
        gain_ref[:] = jnp.zeros(gain_ref.shape, F32)

    kv_heads = own_ref.shape[2]
    for h in range(kv_heads):
        cols = slice(h * HD, (h + 1) * HD)
        d_k, d_v = (own_ref[0, t, h] + near_ref[0, t, h] + far_ref[t, h] for t in range(2))
        d_raw, d_gain = norm_rope_back(d_k, kraw_ref[:, cols], kn_ref[:], cos_ref[:], sin_ref[:])
        out_ref[:, cols] = d_raw
        gain_ref[0:1, :] += d_gain
        out_ref[:, (kv_heads + h) * HD:(kv_heads + h + 1) * HD] = d_v.astype(BF16)


def key_back(half, own, near, far, k_raw, cos_t, sin_t, k_norm):
    _, _, kv_heads, chunk, _ = own.shape
    rows = min(2 * HD, chunk)
    n = chunk // rows
    two = pl.BlockSpec((1, 2, kv_heads, rows, HD), lambda i: (0, 0, 0, i, 0))
    row = lambda cols: rows_of(rows, cols, lambda i: half * n + i)
    return pl.pallas_call(
        kback_kernel,
        grid=(n,),
        in_specs=[
            two,
            two,
            pl.BlockSpec((2, kv_heads, rows, HD), lambda i: (0, 0, i, 0)),
            row(kv_heads * HD),
            row(HD),
            row(HD),
            whole((1, HD)),
        ],
        out_specs=[rows_of(rows, 2 * kv_heads * HD), whole((8, HD))],
        out_shape=[
            like((chunk, 2 * kv_heads * HD), BF16),
            like((8, HD), F32),
        ],
        compiler_params=params(1),
        cost_estimate=cost(32 * chunk * kv_heads * HD, 8 * chunk * kv_heads * HD),
    )(own, near, far, k_raw, cos_t, sin_t, k_norm)


def dx_kernel(n_tp, n_w, at_ref, *refs):
    g_refs, refs = refs[:n_tp], refs[n_tp:]
    w_refs, refs = (refs[:n_w[0]], refs[n_w[0]:sum(n_w)]), refs[sum(n_w):]
    x_ref, dy_ref, wpre_ref, dx_ref, dpre_ref, g_scr, *bufs, acc, sem = refs
    i = pl.program_id(0)
    rows = g_refs[0].shape[0]
    cols = acc.shape[2]
    split = bufs[0].shape[4]

    per_step = (n_w[0] // n_w[1], 1)

    def weight_copies(step, par):
        return [
            pltpu.make_async_copy(w_refs[kind][step * per_step[kind] + j], bufs[kind].at[par, j], sem.at[par, kind, j])
            for kind in range(2)
            for j in range(per_step[kind])
        ]

    @pl.when(i == 0)
    def _():
        for copy in weight_copies(0, 0):
            copy.start()
        for s in range(n_tp):
            g_scr[lax.rem(at_ref[2] + n_tp - s, n_tp)] = g_refs[s][:]
        acc[:] = jnp.zeros(acc.shape, F32)

    for step in range(1, n_w[1]):

        @pl.when(i == step - 1)
        def _():
            for copy in weight_copies(step, step % 2):
                copy.start()

    par = i % 2
    for copy in weight_copies(0, par):
        copy.wait()
    for kind in range(2):
        for j in range(per_step[kind]):
            slot = i * per_step[kind] + j
            part = slice(split, None) if kind else slice(split)
            total = sum(dot(bufs[kind][par, j, t], g_scr[t, :, part], NT) for t in range(n_tp))
            total = jnp.transpose(total)
            share = jnp.bitwise_xor(at_ref[kind], slot)
            for k in range(total.shape[1] // cols):
                acc[share * (total.shape[1] // cols) + k] += total[:, k * cols:(k + 1) * cols]

    @pl.when(i == pl.num_programs(0) - 1)
    def _():
        dpre_ref[:] = jnp.zeros(dpre_ref.shape, F32)
        n = acc.shape[0]
        tiles = [(s, t, slice(s * cols + t, s * cols + t + HD)) for s in range(n) for t in range(0, cols, HD)]
        dim = n * cols
        sub = few(rows)

        def some_rows(r, carry):
            here = pl.ds(pl.multiple_of(r * sub, sub), sub)
            square = jnp.zeros((sub, HD), F32)
            cross = jnp.zeros((sub, HD), F32)
            for s, t, at in tiles:
                x = x_ref[here, at].astype(F32)
                square += x * x
                cross += x * (acc[s, here, t:t + HD] * (1.0 + wpre_ref[:, at]))
            inv = inv_rms(square, dim)
            shrink = inv * inv * inv * row_mean(cross, dim)
            for s, t, at in tiles:
                x = x_ref[here, at].astype(F32)
                d_normed = acc[s, here, t:t + HD]
                dpre_ref[:, at] += fold(d_normed * (x * inv))
                d_x = inv * (d_normed * (1.0 + wpre_ref[:, at])) - x * shrink
                dx_ref[here, at] = (dy_ref[here, at].astype(F32) + d_x).astype(BF16)
            return carry

        lax.fori_loop(0, rows // sub, some_rows, 0)


def input_grad(half, at, grads, w_all, x, dy, w_pre):
    n_tp = len(grads)
    n_w = tuple(map(len, w_all))
    rows, width = grads[0].shape
    dim = x.shape[1]
    here = pl.BlockSpec((rows, dim), lambda i, t: (half * n_tp + t[2], 0))
    grid_spec = pltpu.PrefetchScalarGridSpec(
        num_scalar_prefetch=1,
        grid=(n_w[1],),
        in_specs=[whole((rows, width))] * n_tp + anywhere(sum(n_w)) + [here, here, whole((1, dim))],
        out_specs=[whole((rows, dim)), whole((8, dim))],
        scratch_shapes=[
            pltpu.VMEM((n_tp, rows, width), BF16),
            *(pltpu.VMEM((2, len(w) // n_w[1], *w[0].shape), BF16) for w in w_all),
            pltpu.VMEM((n_w[0], rows, dim // n_w[0]), F32),
            pltpu.SemaphoreType.DMA((2, 2, 2)),
        ],
    )
    return pl.pallas_call(
        functools.partial(dx_kernel, n_tp, n_w),
        grid_spec=grid_spec,
        out_shape=[like((rows, dim), BF16), like((8, dim), F32)],
        compiler_params=params(1),
        cost_estimate=cost(n_tp * rows * width * dim, n_tp * width * dim),
    )(at, *grads, *w_all[0], *w_all[1], x, dy, w_pre)


def place_kernel(rows_ref, *rest):
    rest[-1][:] = rows_ref[:]


def place(half, rows, total=None):
    chunk, dim = rows.shape
    block = min(HD, chunk)
    n = chunk // block
    extra = () if total is None else (total,)
    return pl.pallas_call(
        place_kernel,
        name="place",
        grid=(n,),
        in_specs=[rows_of(block, dim)] + anywhere(len(extra)),
        out_specs=rows_of(block, dim, lambda i: half * n + i),
        out_shape=like((2 * chunk, dim), BF16),
        input_output_aliases={1: 0} if extra else {},
        compiler_params=params(1),
        cost_estimate=cost(chunk * dim, 2 * chunk * dim),
    )(rows, *extra)


def dw_kernel(n_cp, me_ref, *refs):
    g_refs, n_refs = refs[:2 * n_cp], refs[2 * n_cp:-7]
    dwq_ref, dwk_ref, dwv_ref, n_buf, g_buf, n_sem, g_sem = refs[-7:]
    i = pl.program_id(0)
    cols = n_buf.shape[3]
    chunk, width = g_refs[0].shape
    me = me_ref[0]

    def place(refs_in, buf, sem):
        copies = []
        for j, (ref, shape) in enumerate(refs_in):
            start = sum(r[1] for r in refs_in[:j - j % n_cp:n_cp])
            to = buf.at[jnp.bitwise_xor(me, j % n_cp), pl.ds(start, shape)]
            copies.append(pltpu.make_async_copy(ref, to, sem.at[j]))
        return copies

    def fetch(step, par):
        span = pl.ds(pl.multiple_of(step * cols, cols), cols)
        return place([(r.at[:, span], r.shape[0]) for r in n_refs], n_buf.at[par], n_sem.at[par])

    @pl.when(i == 0)
    def _():
        grads = place([(r, chunk) for r in g_refs], g_buf, g_sem)
        for copy in fetch(0, 0) + grads:
            copy.start()
        for copy in grads:
            copy.wait()

    @pl.when(i + 1 < pl.num_programs(0))
    def _():
        for copy in fetch(i + 1, (i + 1) % 2):
            copy.start()

    for copy in fetch(i, i % 2):
        copy.wait()
    seq = 2 * chunk
    grad = dot(n_buf[i % 2].reshape(n_cp * seq, cols), g_buf[:].reshape(n_cp * seq, width), TN)
    q_width, kv_width = dwq_ref.shape[1], dwk_ref.shape[1]
    dwq_ref[:] = grad[:, :q_width]
    dwk_ref[:] = grad[:, q_width:q_width + kv_width]
    dwv_ref[:] = grad[:, q_width + kv_width:]


def weight_grads(me, normed, grads, q_width, cols=256):
    n_cp = len(grads) // 2
    chunk, width = grads[0].shape
    dim = normed[0].shape[1]
    kv_width = (width - q_width) // 2
    tile = lambda n: rows_of(cols, n)
    grid_spec = pltpu.PrefetchScalarGridSpec(
        num_scalar_prefetch=1,
        grid=(dim // cols,),
        in_specs=anywhere(len(grads) + len(normed)),
        out_specs=[tile(q_width), tile(kv_width), tile(kv_width)],
        scratch_shapes=[
            pltpu.VMEM((2, n_cp, 2 * chunk, cols), BF16),
            pltpu.VMEM((n_cp, 2 * chunk, width), BF16),
            pltpu.SemaphoreType.DMA((2, len(normed))),
            pltpu.SemaphoreType.DMA((len(grads),)),
        ],
    )
    return pl.pallas_call(
        functools.partial(dw_kernel, n_cp),
        name="dw",
        grid_spec=grid_spec,
        out_shape=[like((dim, n), F32) for n in (q_width, kv_width, kv_width)],
        compiler_params=params(1),
        cost_estimate=cost(2 * n_cp * chunk * dim * width, 2 * n_cp * chunk * (dim + width)),
    )(me, *grads, *normed)


def join_kernel(core_ref, keep_ref, other_ref, *rest):
    half = pl.program_id(0)

    @pl.when(half == core_ref[0])
    def _():
        rest[-1][:] = keep_ref[:]

    @pl.when(half != core_ref[0])
    def _():
        rest[-1][:] = other_ref[:]


def join_halves(core, keep, other, start, half, total=None):
    block, width = HD, keep.shape[1]
    n = keep.shape[0] // block
    extra = () if total is None else (total,)
    part = pl.BlockSpec((block, width), lambda i, j, c: (j, 0))
    grid_spec = pltpu.PrefetchScalarGridSpec(
        num_scalar_prefetch=1,
        grid=(2, n),
        in_specs=[part, part] + anywhere(len(extra)),
        out_specs=pl.BlockSpec((block, width), lambda i, j, c: (i * (half // block) + start // block + j, 0)),
    )
    return pl.pallas_call(
        join_kernel,
        name="join",
        grid_spec=grid_spec,
        out_shape=like((2 * half, width), F32),
        input_output_aliases={3: 0} if extra else {},
        compiler_params=params(2),
        cost_estimate=cost(n * block * width, 8 * n * block * width),
    )(core, keep, other, *extra)


def solution(mesh):
    n_cp, n_tp, n_dp = mesh.shape["cp"], mesh.shape["tp"], mesh.shape["dp"]
    near = [(i, i ^ 1) for i in range(n_cp)]
    across = [(i, i ^ 2) for i in range(n_cp)]
    beside = [(i, i ^ 1) for i in range(n_dp)]

    def from_cp(value):
        far = lax.ppermute(value, "cp", across)
        return [value, lax.ppermute(value, "cp", near), far, lax.ppermute(far, "cp", near)]

    def per_device(hidden, cotangent, pos_loc, w_q, w_k, w_v, w_o, w_pre, w_post, q_norm, k_norm):
        _, seq, dim = hidden.shape
        x, dy = hidden[0], cotangent[0]
        kv_heads = w_k.shape[1] // HD
        cp, tp, dp = (lax.axis_index(a).astype(jnp.int32) for a in ("cp", "tp", "dp"))
        core = cp % 2
        me, one_core = cp.reshape(1), core.reshape(1)

        share = dp * n_cp + cp
        shares = n_dp * n_cp
        cols = dim // shares

        def over_tp(part):
            return lax.all_gather(part, "tp", axis=0, tiled=True)

        def spread(own):
            blocks = from_cp(own)
            if n_dp == 2:
                for value in (own, blocks[2]):
                    other = lax.ppermute(value, "dp", beside)
                    blocks += [other, lax.ppermute(other, "cp", near)]
            return blocks

        w_o_all = spread(over_tp(lax.dynamic_slice_in_dim(w_o, share * cols, cols, 1)))
        w_a = lax.dynamic_slice_in_dim(w_q, share * cols, cols, 0)
        share_b = dp * 2 + core
        cols_b = dim // (2 * n_dp)
        w_b = jnp.concatenate([lax.dynamic_slice_in_dim(w, share_b * cols_b, cols_b, 0) for w in (w_k, w_v)], axis=1)
        w_a_all = spread(over_tp(w_a).reshape(n_tp, cols, w_a.shape[1]))

        cos_t, sin_t = rope_tables(pos_loc)
        qn, kn = q_norm.reshape(1, HD), k_norm.reshape(1, HD)
        wpre, wpost = w_pre.reshape(1, dim), w_post.reshape(1, dim)
        rows = seq // 8
        x_far = lax.ppermute(x[:rows], "cp", across)
        *normed, kv_own, k_raw = project_kv(x, wpre, w_k, w_v, kn, cos_t, sin_t, rows, (1, 3, 4))
        kv_blocks = from_cp(kv_own)
        q_fin, q_raw = project_q(normed, w_q, qn, cos_t, sin_t, rows)
        far = norm_rows(x_far, wpre)
        normed_all = [normed[0], lax.ppermute(normed[0], "cp", near), far, lax.ppermute(far, "cp", near)]
        normed_all += from_cp(normed[1]) + from_cp(normed[2])
        out, lse = attention_fwd(me, q_fin, kv_blocks, kv_heads)

        out_all = {}
        for half in (1, 0):
            out_all[half] = lax.all_gather(out[half], "tp", axis=0, tiled=False)
        w_b = over_tp(w_b).reshape(n_tp, cols_b, w_b.shape[1])
        w_b_all = [w_b, lax.ppermute(w_b, "cp", near)]
        if n_dp == 2:
            w_b = lax.ppermute(w_b, "dp", beside)
            w_b_all += [w_b, lax.ppermute(w_b, "cp", near)]
        at = jnp.stack([share, core])

        low, dq, d_attn, d_post, gains, carried, y = [], {}, {}, [], [], {}, None
        for half in (1, 0):
            y, d_attn[half], d_out, part = post(half, at, out_all[half], w_o_all, w_o, x, dy, wpost, y)
            d_post.append(part)
            dq[half], kept, sent, *low, gain = attention_bwd(
                half, me, q_fin, d_out, out, lse, q_raw, cos_t, sin_t, qn, kv_blocks, kv_heads, *low
            )
            gains.append(gain[0])
            got = lax.ppermute(sent, "cp", near)
            carried[half] = (kept, got, lax.ppermute(kept[1] + got[1], "cp", across))

        give, keep = out_weight_grad(one_core, out, (d_attn[0], d_attn[1]))
        got = lax.ppermute(give, "cp", near)
        rows = keep.shape[0]
        d_wo = None
        for start, stop in ((0, rows - HD), (rows - HD, rows)):
            mine_part = keep[start:stop] + got[start:stop]
            mine_part = mine_part + lax.ppermute(mine_part, "cp", across)
            other = lax.ppermute(mine_part, "cp", near)
            d_wo = join_halves(one_core, mine_part, other, start, rows, d_wo)

        rows = seq // 2 // n_tp
        at_tp = jnp.stack([share, share_b, tp])
        grads, d_hidden, d_pre = {}, None, []
        for half in (1, 0):
            d_kv, gain = key_back(half, *carried[half], k_raw, cos_t, sin_t, kn)
            gains.append(gain[0])
            g = grads[half] = jnp.concatenate([dq[half], d_kv], axis=1)
            pieces = [lax.dynamic_slice_in_dim(g, tp * rows, rows, 0)]
            for s in range(1, n_tp):
                part = lax.dynamic_slice_in_dim(g, ((tp + s) % n_tp) * rows, rows, 0)
                pieces.append(lax.ppermute(part, "tp", [(i, (i + s) % n_tp) for i in range(n_tp)]))
            dx_rows, part = input_grad(half, at_tp, pieces, (w_a_all, w_b_all), x, dy, wpre)
            d_pre.append(part)
            dx_rows = lax.all_gather(dx_rows, "tp", axis=0, tiled=True)
            d_hidden = place(half, dx_rows, d_hidden)

        grads_all = from_cp(grads[0]) + from_cp(grads[1])
        d_wq, d_wk, d_wv = weight_grads(me, normed_all, grads_all, w_q.shape[1])

        d_post, d_pre = jnp.sum(sum(d_post), axis=0), jnp.sum(sum(d_pre), axis=0)
        small = jnp.concatenate([jnp.where(tp == 0, d_post, 0.0), d_pre, sum(gains[:2]), sum(gains[2:])])
        small = small + lax.ppermute(small, "cp", near)
        small = small + lax.ppermute(small, "cp", across)
        small = small + lax.ppermute(small, "tp", [(i, i ^ 1) for i in range(n_tp)])
        small = small + lax.ppermute(small, "tp", [(i, i ^ 2) for i in range(n_tp)])
        d_post, d_pre, d_qn, d_kn = jnp.split(small, np.cumsum([dim, dim, HD]))
        return y[None], d_hidden[None], d_wq, d_wk, d_wv, d_wo, d_pre, d_post, d_qn, d_kn

    rows, cols, all_of = P('dp', 'cp'), P(None, 'tp'), P()
    specs_in = (rows, rows, P(('dp', 'cp')), cols, cols, cols, P('tp'), all_of, all_of, all_of, all_of)
    grid, by_dp = P('dp', 'tp'), P('dp')
    specs_out = (rows, rows, grid, grid, grid, P(('dp', 'tp')), by_dp, by_dp, by_dp, by_dp)
    return jax.shard_map(per_device, mesh=mesh, in_specs=specs_in, out_specs=specs_out, check_vma=False)
```
